32 devices in a mesh: seq: 8 (over z, y), ch: 4 (over x, core).
Axes of the slice: x: 2, y: 2, z: 4, core: 2. Of those that a mesh axis runs over, the one named last changes fastest.
Arguments:
- query_input: bfloat16 [1024, 2048], P('seq', 'ch'), may hold values from -6 to 6
- key_input: bfloat16 [1024, 2048], P('seq', 'ch'), may hold values from -6 to 6
- value_input: bfloat16 [1024, 2048], P('seq', 'ch'), may hold values from -6 to 6
- cotangent: bfloat16 [1024, 2048], P('seq', 'ch'), may hold values from -6 to 6
- filter_taps: float32 [1024, 2048], P('seq', 'ch'), may hold values from -0.1875 to 0.1875
- skip_gain: float32 [2048], P('ch'), may hold values from -2 to 2
Outputs:
- output: bfloat16 [1024, 2048], P('seq', 'ch')
- query_grad: bfloat16 [1024, 2048], P('seq', 'ch')
- key_grad: bfloat16 [1024, 2048], P('seq', 'ch')
- value_grad: bfloat16 [1024, 2048], P('seq', 'ch')
- filter_grad: float32 [1024, 2048], P('seq', 'ch')
- skip_grad: float32 [2048], P('ch')
- grad_rms: float32 [], replicated
The draws below stay inside these ranges and needn't reach their ends.
All inputs are finite; a program needn't handle non-finite values.
Results may differ from the reference program's by a relative error of at most 0.0014.
Values sent between devices are 32-bit elements; how exact they have to be, the bound alone decides.
A program may use at most 64 MiB of HBM per device.

```python
import math
import jax
import jax.numpy as jnp
from jax import lax

CH_DEV = 512
TOKENS = 1024
CHANNELS = 2048
N_CH = 4


def level_of(own_key, dims, cuts, least, top_value):
    loudness = 1.0
    for dim, parts in cuts:
        heights = jax.random.uniform(jax.random.fold_in(jax.random.fold_in(own_key, 6), dim), (parts,), jnp.float32, least / len(cuts), top_value / len(cuts))
        loudness = loudness * jnp.repeat(jnp.exp(heights), dims[dim] // parts).reshape((-1,) + (1,) * (len(dims) - 1 - dim))
    return loudness


def gaussian(key, dims, deviation, reach, pieces=(), held_as=jnp.bfloat16):
    entries = deviation * jax.random.normal(key, dims, jnp.float32)
    if pieces:
        entries = entries * level_of(key, dims, pieces, -0.22, 0.18)
    return jnp.clip(entries, -reach, reach).astype(held_as)


def setup_inputs(seed: int = 0) -> dict:
    splits = jax.random.split(jax.random.key(seed), 7)
    return {
        "query_input": gaussian(splits[0], (TOKENS, CHANNELS), 1.0, 6.0, ((0, 8), (1, 4))),
        "key_input": gaussian(splits[1], (TOKENS, CHANNELS), 1.0, 6.0, ((0, 8), (1, 4))),
        "value_input": gaussian(splits[2], (TOKENS, CHANNELS), 1.0, 6.0, ((0, 8), (1, 4))),
        "cotangent": gaussian(splits[3], (TOKENS, CHANNELS), 1.0, 6.0, ((0, 8), (1, 4))),
        "filter_taps": gaussian(splits[4], (TOKENS, CHANNELS), TOKENS ** -0.5, 0.1875, ((0, 8), (1, 4)), jnp.float32),
        "skip_gain": gaussian(splits[5], (CHANNELS,), 0.5, 2.0, ((0, 4),), jnp.float32),
    }


def one_group(operands):
    query_input, key_input, value_input, cotangent, filter_taps, skip_gain = operands
    query_val = query_input.astype(jnp.float32)
    key_val = key_input.astype(jnp.float32)
    value_val = value_input.astype(jnp.float32)
    cot_val = cotangent.astype(jnp.float32)
    mixed_in = key_val * value_val
    gated_cot = query_val * cot_val
    length = 2 * TOKENS
    mixed_spec = jnp.fft.rfft(mixed_in, n=length, axis=0)
    gated_spec = jnp.fft.rfft(gated_cot, n=length, axis=0)
    taps_spec = jnp.fft.rfft(filter_taps, n=length, axis=0)
    conv_out = jnp.fft.irfft(mixed_spec * taps_spec, n=length, axis=0)[:TOKENS]
    back_conv = jnp.fft.irfft(gated_spec * jnp.conj(taps_spec), n=length, axis=0)[:TOKENS]
    kernel_grad = jnp.fft.irfft(gated_spec * jnp.conj(mixed_spec), n=length, axis=0)[:TOKENS]
    inner_sum = conv_out + skip_gain[None, :] * mixed_in
    mixed_grad = back_conv + skip_gain[None, :] * gated_cot
    grad_scale = 1.0 / math.sqrt(TOKENS)
    return ((query_val * inner_sum).astype(jnp.bfloat16), (cot_val * inner_sum).astype(jnp.bfloat16), (mixed_grad * value_val).astype(jnp.bfloat16), (mixed_grad * key_val).astype(jnp.bfloat16), kernel_grad * grad_scale, lax.optimization_barrier(jnp.sum(gated_cot * mixed_in, axis=0)) * grad_scale)

def split_rows(array):
    return jnp.moveaxis(array.reshape(array.shape[0], N_CH, CH_DEV), 1, 0)

def join_rows(array):
    return jnp.moveaxis(array, 0, 1).reshape(array.shape[1], N_CH * CH_DEV)

def reference(query_input, key_input, value_input, cotangent, filter_taps, skip_gain):
    operands = (split_rows(query_input), split_rows(key_input), split_rows(value_input), split_rows(cotangent), split_rows(filter_taps), skip_gain.reshape(N_CH, CH_DEV))
    results = lax.map(one_group, operands)
    output = join_rows(results[0])
    query_grad = join_rows(results[1])
    key_grad = join_rows(results[2])
    value_grad = join_rows(results[3])
    filter_grad = join_rows(results[4])
    skip_grad = results[5].reshape(CHANNELS)
    squares = jnp.sum(filter_grad * filter_grad) + jnp.sum(skip_grad * skip_grad)
    grad_rms = jnp.sqrt(squares / (CHANNELS * (TOKENS + 1)))
    return (output, query_grad, key_grad, value_grad, filter_grad, skip_grad, grad_rms)
```

```python
import functools
import math

import jax
import jax.numpy as jnp
import numpy as np
from jax import lax
from jax.experimental import pallas as pl
from jax.experimental.pallas import tpu as pltpu
from jax.sharding import PartitionSpec as P

LANES = 128
MESH = pl.DeviceIdType.MESH


def complex_mul(left_op, right_op):
    return jnp.stack(
        [
            left_op[0] * right_op[0] - left_op[1] * right_op[1],
            left_op[0] * right_op[1] + left_op[1] * right_op[0],
        ]
    )


def conj_of(stacked):
    return jnp.stack([stacked[0], -stacked[1]])


def dft_table(length, direction):
    counter = jnp.arange(length)
    angles = (
        2.0 * math.pi / length * (counter[:, None] * counter[None, :] % length).astype(jnp.float32)
    )
    return (jnp.cos(angles), direction * jnp.sin(angles))


def dft_along(stacked, length, direction, pattern):
    table_re, table_im = dft_table(length, direction)

    def contract(table, part_in):
        return jnp.einsum(pattern, table, part_in, precision=lax.Precision.HIGHEST)

    real_out = contract(table_re, stacked[0]) - contract(table_im, stacked[1])
    imag_out = contract(table_re, stacked[1]) + contract(table_im, stacked[0])
    return jnp.stack([real_out, imag_out])


def grid_twiddle(devices, block, direction):
    seq_length = devices * block
    counter = jnp.arange(devices)[:, None] * jnp.arange(block)[None, :] % seq_length
    angles = direction * 2.0 * math.pi / seq_length * counter.astype(jnp.float32)
    return jnp.stack([jnp.cos(angles), jnp.sin(angles)])[:, None, None]


def local_forward(stacked, devices, block):
    array_shape = stacked.shape
    stacked = stacked.reshape(array_shape[0], array_shape[1], array_shape[2], devices, block)
    stacked = dft_along(stacked, devices, -1.0, "kj,scjp->sckp")
    stacked = complex_mul(stacked, grid_twiddle(devices, block, -1.0))
    return dft_along(stacked, block, -1.0, "kp,scjp->scjk")


def local_inverse(stacked, devices, block):
    stacked = dft_along(stacked, block, 1.0, "kp,scjp->scjk")
    stacked = complex_mul(stacked, grid_twiddle(devices, block, 1.0))
    stacked = dft_along(stacked, devices, 1.0, "kj,scjp->sckp")
    array_shape = stacked.shape
    return stacked.reshape(array_shape[0], array_shape[1], array_shape[2], devices * block) / (
        devices * block
    )


def modulated(signals, cosine, sine_part):
    zero_part = jnp.zeros_like(signals)
    return jnp.stack(
        [
            jnp.concatenate([signals, signals * cosine]),
            jnp.concatenate([zero_part, -signals * sine_part]),
        ]
    )


def spectral_products(spectrum):
    mixed_spec = spectrum[:, 0::3]
    gated_spec = spectrum[:, 1::3]
    taps_spec = spectrum[:, 2::3]
    out_spec = complex_mul(mixed_spec, taps_spec)
    back_spec = complex_mul(gated_spec, conj_of(taps_spec))
    grad_spec = complex_mul(gated_spec, conj_of(mixed_spec))
    return jnp.stack(
        [
            out_spec[:, 0],
            back_spec[:, 0],
            grad_spec[:, 0],
            out_spec[:, 1],
            back_spec[:, 1],
            grad_spec[:, 1],
        ],
        axis=1,
    )


def unfold(series, cosine, sine_part):
    return tuple(
        (
            0.5
            * (
                series[0, signal_index]
                + cosine * series[0, signal_index + 3]
                - sine_part * series[1, signal_index + 3]
            )
            for signal_index in range(3)
        )
    )


def channel_local(mixed_in, gated_cot, filter_taps, devices):
    pieces = (
        lax.all_to_all(mixed_in, "seq", split_axis=1, concat_axis=0, tiled=True),
        lax.all_to_all(gated_cot, "seq", split_axis=1, concat_axis=0, tiled=True),
        lax.all_to_all(filter_taps, "seq", split_axis=1, concat_axis=0, tiled=True),
    )
    laid = jnp.transpose(jnp.stack(pieces), (0, 2, 1))
    seq_length = laid.shape[2]
    block = seq_length // devices
    angles = math.pi / seq_length * jnp.arange(seq_length).astype(jnp.float32)
    cosine = jnp.cos(angles)
    sine_row = jnp.sin(angles)
    spectrum = local_forward(modulated(laid, cosine, sine_row), devices, block)
    series = local_inverse(spectral_products(spectrum), devices, block)
    results = unfold(series, cosine, sine_row)
    return (
        lax.all_to_all(results[0].T, "seq", split_axis=0, concat_axis=1, tiled=True),
        lax.all_to_all(results[1].T, "seq", split_axis=0, concat_axis=1, tiled=True),
        lax.all_to_all(results[2].T, "seq", split_axis=0, concat_axis=1, tiled=True),
    )


def body(query_input, key_input, value_input, cotangent, filter_taps, skip_gain):
    devices = lax.axis_size("seq")
    row_count, channels = query_input.shape
    seq_length = row_count * devices
    query_val = query_input.astype(jnp.float32)
    key_val = key_input.astype(jnp.float32)
    value_val = value_input.astype(jnp.float32)
    cot_val = cotangent.astype(jnp.float32)
    mixed_in = key_val * value_val
    gated_cot = query_val * cot_val
    conv_out, back_conv, kernel_grad = channel_local(mixed_in, gated_cot, filter_taps, devices)
    inner_sum = conv_out + skip_gain[None, :] * mixed_in
    mixed_grad = back_conv + skip_gain[None, :] * gated_cot
    output = (query_val * inner_sum).astype(jnp.bfloat16)
    query_grad = (cot_val * inner_sum).astype(jnp.bfloat16)
    key_grad = (mixed_grad * value_val).astype(jnp.bfloat16)
    value_grad = (mixed_grad * key_val).astype(jnp.bfloat16)
    time_scale = 1.0 / math.sqrt(seq_length)
    filter_grad = kernel_grad * time_scale
    filter_sq = jnp.sum(filter_grad * filter_grad)
    skip_part = jnp.sum(gated_cot * mixed_in, axis=0) * time_scale
    skip_grad = lax.psum(skip_part, "seq")
    total_sq = lax.psum(filter_sq + jnp.sum(skip_grad * skip_grad) / devices, ("seq", "ch"))
    grad_rms = jnp.sqrt(total_sq / (channels * lax.axis_size("ch") * (seq_length + 1)))
    return (output, query_grad, key_grad, value_grad, filter_grad, skip_grad, grad_rms)


def split_high_low(array):
    high = array.astype(jnp.bfloat16)
    return high, (array - high.astype(jnp.float32)).astype(jnp.bfloat16)


def half_tables(points):
    odd = 2 * np.arange(points, dtype=np.int64) + 1
    angles = math.pi / (4 * points) * (odd[:, None] * odd[None, :] % (8 * points))
    parts = []
    for table in (np.cos(angles), np.sin(angles)):
        table = table.astype(np.float32)
        high = table.astype(jnp.bfloat16)
        parts += [high, (table - high.astype(np.float32)).astype(jnp.bfloat16)]
    shift = math.pi / (4 * points) * odd[:, None] * np.ones((1, LANES))
    return np.stack(parts), np.stack([np.cos(shift), np.sin(shift)]).astype(np.float32)


def kernel(
    devices, groups, count,
    q_hbm, k_hbm, v_hbm, c_hbm, h_hbm, skip_hbm, table_hbm, twist_hbm,
    out_ref, dq_ref, dk_ref, dv_ref, dh_ref, dskip_ref, rms_ref,
    q_ref, k_ref, v_ref, c_ref, skip_ref, x_buf, g_buf, wide, flat, send, recv, spec, prod, back, home, tail, tail_home, sq_send, sq_recv,
    table, twist, send_sem, recv_sem, own_sem, tail_send, tail_recv, sq_ssem, sq_rsem, load_sem, in_sem,
):
    me = lax.axis_index("seq")
    mine = lax.axis_index("ch")
    rows, channels = q_hbm.shape
    half = rows // 2
    points = half * devices
    low = LANES // 2
    time_scale = 1.0 / math.sqrt(2 * points)

    barrier = pltpu.get_barrier_semaphore()
    for k in range(1, devices):
        pl.semaphore_signal(
            barrier, inc=1, device_id={"seq": lax.rem(me + k, devices)}, device_id_type=MESH
        )
    for k in range(1, groups):
        pl.semaphore_signal(
            barrier, inc=1, device_id={"ch": lax.rem(mine + k, groups)}, device_id_type=MESH
        )
    blocks = channels // LANES

    def columns_of(j):
        return pl.ds(j * LANES, LANES)

    inputs = tuple(
        pltpu.make_async_copy(source, target, in_sem.at[index])
        for index, (source, target) in enumerate(
            [(k_hbm, k_ref), (v_hbm, v_ref), (q_hbm, q_ref), (c_hbm, c_ref), (skip_hbm, skip_ref)]
            + [(h_hbm.at[:, columns_of(j)], wide.at[j]) for j in range(blocks)]
        )
    )
    for load in inputs:
        load.start()
    loads = (
        pltpu.make_async_copy(table_hbm, table, load_sem.at[0]),
        pltpu.make_async_copy(twist_hbm, twist, load_sem.at[1]),
    )
    for load in loads:
        load.start()

    def remote(source, target, slot, k):
        peer = lax.rem(me + k, devices)
        return pltpu.make_async_remote_copy(
            src_ref=source.at[peer],
            dst_ref=target.at[me],
            send_sem=send_sem.at[slot, k],
            recv_sem=recv_sem.at[slot, k],
            device_id={"seq": peer},
            device_id_type=MESH,
        )

    def own(source, target, slot):
        return pltpu.make_async_copy(source.at[me], target.at[me], own_sem.at[slot])

    def tail_copy(k):
        peer = lax.rem(me + k, devices)
        return pltpu.make_async_remote_copy(
            src_ref=tail,
            dst_ref=tail_home.at[me],
            send_sem=tail_send.at[k],
            recv_sem=tail_recv.at[k],
            device_id={"seq": peer},
            device_id_type=MESH,
        )

    def square_copy(k):
        peer = lax.rem(mine + k, groups)
        return pltpu.make_async_remote_copy(
            src_ref=sq_send,
            dst_ref=sq_recv.at[mine],
            send_sem=sq_ssem.at[k],
            recv_sem=sq_rsem.at[k],
            device_id={"ch": peer},
            device_id_type=MESH,
        )

    def start_all(source, target, slot):
        for k in range(1, devices):
            remote(source, target, slot, k).start()
        own(source, target, slot).start()

    def wait_arrivals(source, target, slot):
        for k in range(1, devices):
            remote(source, target, slot, k).wait_recv()
        own(source, target, slot).wait()

    first = lax.broadcasted_iota(jnp.int32, (half, LANES), 1) < low

    def pack(source, signal):
        for j in range(channels // LANES):
            even = source[j, pl.ds(0, half, stride=2), :]
            odd = source[j, pl.ds(1, half, stride=2), :]
            send[signal, 2 * j] = jnp.where(first, even, pltpu.roll(odd, low, 1))
            send[signal, 2 * j + 1] = jnp.where(first, pltpu.roll(even, low, 1), odd)

    def unpack(signal):
        for j in range(channels // LANES):
            left = home[signal, 2 * j]
            right = home[signal, 2 * j + 1]
            flat[signal, j, pl.ds(0, half, stride=2), :] = jnp.where(
                first, left, pltpu.roll(right, low, 1)
            )
            flat[signal, j, pl.ds(1, half, stride=2), :] = jnp.where(
                first, pltpu.roll(left, low, 1), right
            )

    inputs[0].wait()
    inputs[1].wait()
    for j in range(blocks):
        at = columns_of(j)
        x_buf[j] = k_ref[:, at].astype(jnp.float32) * v_ref[:, at].astype(jnp.float32)
    pack(x_buf, 0)
    pl.semaphore_wait(barrier, devices + groups - 2)
    start_all(send.at[0], recv.at[0], 0)
    inputs[2].wait()
    inputs[3].wait()
    for j in range(blocks):
        at = columns_of(j)
        g_buf[j] = q_ref[:, at].astype(jnp.float32) * c_ref[:, at].astype(jnp.float32)
    pack(g_buf, 1)
    start_all(send.at[1], recv.at[1], 1)
    for load in inputs[4:]:
        load.wait()
    pack(wide, 2)
    start_all(send.at[2], recv.at[2], 2)
    for load in loads:
        load.wait()

    def times(which, high, rest):
        both = jnp.concatenate([high, rest], axis=1)
        main = jnp.dot(table[2 * which], both, preferred_element_type=jnp.float32)
        small = jnp.dot(table[2 * which + 1], high, preferred_element_type=jnp.float32)
        return main[:, :LANES] + (main[:, LANES:] + small)

    def forward(signal):
        high, rest = split_high_low(recv[signal].reshape(points, LANES))
        spec[signal, 0] = times(0, high, rest)
        spec[signal, 1] = -times(1, high, rest)

    def inverse(slot, scale):
        real_high, real_rest = split_high_low(prod[0])
        imag_high, imag_rest = split_high_low(prod[1])
        series = times(0, real_high, real_rest) - times(1, imag_high, imag_rest)
        series = series * (scale / points)
        back[slot] = series.reshape(devices, half, LANES)
        return series

    step = 32

    def halves(ref_row, part, at):
        value = spec[ref_row, part, at, :]
        turned = pltpu.roll(value, low, 1)
        left = lax.broadcasted_iota(jnp.int32, (step, LANES), 1) < low
        return value, turned, jnp.where(left, value, turned), jnp.where(left, turned, value)

    def products(signal, other, conjugate):
        sign = jnp.where(lax.broadcasted_iota(jnp.int32, (step, LANES), 1) < low, 1.0, -1.0)

        @pl.loop(0, points // step)
        def _(index):
            at = pl.ds(pl.multiple_of(index * step, step), step)
            cosine = twist[0, at, :]
            sine = twist[1, at, :]
            signed = sine * sign
            _, _, even_re, odd_re = halves(other, 0, at)
            _, _, even_im, odd_im = halves(other, 1, at)
            a_re, as_re, _, _ = halves(signal, 0, at)
            a_im, as_im, _, _ = halves(signal, 1, at)
            p_re = even_re * cosine - even_im * sine
            p_im = even_im * cosine + even_re * sine
            if conjugate:
                r_re = odd_re * cosine - odd_im * signed
                r_im = odd_im * cosine + odd_re * signed
                prod[0, at, :] = a_re * p_re + a_im * p_im + (as_re * r_re + as_im * r_im)
                prod[1, at, :] = a_im * p_re - a_re * p_im + (as_im * r_re - as_re * r_im)
            else:
                r_re = odd_re * cosine + odd_im * signed
                r_im = odd_im * cosine - odd_re * signed
                prod[0, at, :] = a_re * p_re - a_im * p_im + (as_re * r_re - as_im * r_im)
                prod[1, at, :] = a_im * p_re + a_re * p_im + (as_im * r_re + as_re * r_im)

    wait_arrivals(send.at[0], recv.at[0], 0)
    forward(0)
    wait_arrivals(send.at[1], recv.at[1], 1)
    forward(1)
    products(1, 0, True)
    series = inverse(0, time_scale)
    start_all(back.at[0], home.at[0], 3)
    direct = jnp.sum(
        (recv[0] * recv[1]).reshape(points // 8, 8, LANES), axis=0
    )
    direct = jnp.sum(direct, axis=0, keepdims=True)
    direct = jnp.broadcast_to(direct, (8, LANES)) * time_scale
    direct = direct + pltpu.roll(direct, low, 1)
    squares = jnp.sum((series * series).reshape(points // 8, 8, LANES), axis=0)
    squares = squares + direct * direct * (1.0 / 16.0)
    sq_send[...] = squares
    for k in range(1, groups):
        square_copy(k).start()
    sq_own = pltpu.make_async_copy(sq_send, sq_recv.at[mine], load_sem.at[2])
    sq_own.start()

    wait_arrivals(send.at[2], recv.at[2], 2)
    forward(2)
    products(0, 2, False)
    inverse(1, 1.0)
    start_all(back.at[1], home.at[1], 4)
    for k in range(1, groups):
        square_copy(k).wait_recv()
    sq_own.wait()
    total = sq_recv[0]
    for k in range(1, groups):
        total = total + sq_recv[k]
    tail[0] = direct
    tail[1] = total
    for k in range(1, devices):
        tail_copy(k).start()
    tail_own = pltpu.make_async_copy(tail, tail_home.at[me], load_sem.at[3])
    tail_own.start()
    products(1, 2, True)
    inverse(2, 1.0)
    start_all(back.at[2], home.at[2], 5)

    wait_arrivals(back.at[0], home.at[0], 3)
    unpack(0)
    for j in range(blocks):
        dh_ref[:, columns_of(j)] = flat[0, j]

    wait_arrivals(back.at[1], home.at[1], 4)
    unpack(1)
    for j in range(blocks):
        at = columns_of(j)
        inner = flat[1, j] + skip_ref[:, at] * x_buf[j]
        out_ref[:, at] = (q_ref[:, at].astype(jnp.float32) * inner).astype(jnp.bfloat16)
        dq_ref[:, at] = (c_ref[:, at].astype(jnp.float32) * inner).astype(jnp.bfloat16)

    for k in range(1, devices):
        tail_copy(k).wait_recv()
    tail_own.wait()
    total = tail_home[0, 1]
    for k in range(1, devices):
        total = total + tail_home[k, 1]
    total = jnp.sum(jnp.sum(total, axis=0, keepdims=True), axis=1, keepdims=True)
    rms_ref[...] = jnp.sqrt(total / count)
    for j in range(blocks):
        left = lax.broadcasted_iota(jnp.int32, (8, LANES), 1) < low
        both = jnp.where(left, tail_home[2 * j, 0], tail_home[2 * j + 1, 0])
        dskip_ref[:, columns_of(j)] = both[0:1]

    wait_arrivals(back.at[2], home.at[2], 5)
    unpack(2)
    for j in range(blocks):
        at = columns_of(j)
        grad = flat[2, j] + skip_ref[:, at] * g_buf[j]
        dk_ref[:, at] = (grad * v_ref[:, at].astype(jnp.float32)).astype(jnp.bfloat16)
        dv_ref[:, at] = (grad * k_ref[:, at].astype(jnp.float32)).astype(jnp.bfloat16)

    for k in range(1, devices):
        for slot in range(3):
            remote(send.at[slot], recv.at[slot], slot, k).wait_send()
            remote(back.at[slot], home.at[slot], slot + 3, k).wait_send()
        tail_copy(k).wait_send()
    for k in range(1, groups):
        square_copy(k).wait_send()


def emit(*refs):
    sources, targets, sem = refs[:7], refs[7:14], refs[14]
    copies = [
        pltpu.make_async_copy(source, target, sem.at[index])
        for index, (source, target) in enumerate(zip(sources, targets))
    ]
    for copy in copies:
        copy.start()
    for copy in copies:
        copy.wait()


def fused_body(query_input, key_input, value_input, cotangent, filter_taps, skip_gain):
    devices = lax.axis_size("seq")
    groups = lax.axis_size("ch")
    rows, channels = query_input.shape
    half = rows // 2
    points = half * devices
    tables, twists = half_tables(points)
    count = float(channels * groups * (rows * devices + 1))
    vmem = pl.BlockSpec(memory_space=pltpu.VMEM)
    hbm = pl.BlockSpec(memory_space=pltpu.HBM)
    moved = (3, devices, half, LANES)
    blocks = channels // LANES
    shapes = [((rows, channels), jnp.bfloat16)] * 4 + [
        ((rows, channels), jnp.float32),
        ((1, channels), jnp.float32),
        ((1, 1), jnp.float32),
    ]
    held = pl.pallas_call(
        functools.partial(kernel, devices, groups, count),
        out_shape=tuple(pltpu.VMEM(*shape) for shape in shapes),
        in_specs=[hbm] * 8,
        out_specs=(vmem,) * 7,
        scratch_shapes=[
            pltpu.VMEM((rows, channels), jnp.bfloat16),
            pltpu.VMEM((rows, channels), jnp.bfloat16),
            pltpu.VMEM((rows, channels), jnp.bfloat16),
            pltpu.VMEM((rows, channels), jnp.bfloat16),
            pltpu.VMEM((1, channels), jnp.float32),
            pltpu.VMEM((blocks, rows, LANES), jnp.float32),
            pltpu.VMEM((blocks, rows, LANES), jnp.float32),
            pltpu.VMEM((blocks, rows, LANES), jnp.float32),
            pltpu.VMEM((3, blocks, rows, LANES), jnp.float32),
            pltpu.VMEM(moved, jnp.float32),
            pltpu.VMEM(moved, jnp.float32),
            pltpu.VMEM((3, 2, points, LANES), jnp.float32),
            pltpu.VMEM((2, points, LANES), jnp.float32),
            pltpu.VMEM(moved, jnp.float32),
            pltpu.VMEM(moved, jnp.float32),
            pltpu.VMEM((2, 8, LANES), jnp.float32),
            pltpu.VMEM((devices, 2, 8, LANES), jnp.float32),
            pltpu.VMEM((8, LANES), jnp.float32),
            pltpu.VMEM((groups, 8, LANES), jnp.float32),
            pltpu.VMEM(tables.shape, jnp.bfloat16),
            pltpu.VMEM(twists.shape, jnp.float32),
            pltpu.SemaphoreType.DMA((6, devices)),
            pltpu.SemaphoreType.DMA((6, devices)),
            pltpu.SemaphoreType.DMA((6,)),
            pltpu.SemaphoreType.DMA((devices,)),
            pltpu.SemaphoreType.DMA((devices,)),
            pltpu.SemaphoreType.DMA((groups,)),
            pltpu.SemaphoreType.DMA((groups,)),
            pltpu.SemaphoreType.DMA((4,)),
            pltpu.SemaphoreType.DMA((5 + blocks,)),
        ],
        compiler_params=pltpu.CompilerParams(
            collective_id=0, has_side_effects=True, vmem_limit_bytes=(64 << 20) - (960 << 10)
        ),
    )(
        query_input, key_input, value_input, cotangent, filter_taps,
        skip_gain.reshape(1, channels), jnp.asarray(tables), jnp.asarray(twists),
    )
    results = pl.pallas_call(
        emit,
        out_shape=tuple(jax.ShapeDtypeStruct(*shape) for shape in shapes),
        in_specs=[vmem] * 7,
        out_specs=(hbm,) * 7,
        scratch_shapes=[pltpu.SemaphoreType.DMA((7,))],
        compiler_params=pltpu.CompilerParams(vmem_limit_bytes=4 << 20),
    )(*held)
    return (*results[:5], results[5].reshape(channels), results[6].reshape(()))


def pick_body(query_input, *others):
    devices = lax.axis_size("seq")
    rows, channels = query_input.shape
    fits = 2 * channels == LANES * devices and channels % LANES == 0 and rows % 16 == 0
    chosen = fused_body if fits and rows * devices <= 2048 else body
    return chosen(query_input, *others)


def solution(mesh):
    return jax.shard_map(
        pick_body,
        mesh=mesh,
        in_specs=(
            P("seq", "ch"),
            P("seq", "ch"),
            P("seq", "ch"),
            P("seq", "ch"),
            P("seq", "ch"),
            P("ch"),
        ),
        out_specs=(
            P("seq", "ch"),
            P("seq", "ch"),
            P("seq", "ch"),
            P("seq", "ch"),
            P("seq", "ch"),
            P("ch"),
            P(),
        ),
        check_vma=False,
    )
```

```python
import functools
import math

import jax
import jax.numpy as jnp
import numpy as np
from jax import lax
from jax.experimental import pallas as pl
from jax.experimental.pallas import tpu as pltpu
from jax.sharding import PartitionSpec as P

LANES = 128
MESH = pl.DeviceIdType.MESH


def complex_mul(left_op, right_op):
    return jnp.stack(
        [
            left_op[0] * right_op[0] - left_op[1] * right_op[1],
            left_op[0] * right_op[1] + left_op[1] * right_op[0],
        ]
    )


def conj_of(stacked):
    return jnp.stack([stacked[0], -stacked[1]])


def dft_table(length, direction):
    counter = jnp.arange(length)
    angles = (
        2.0 * math.pi / length * (counter[:, None] * counter[None, :] % length).astype(jnp.float32)
    )
    return (jnp.cos(angles), direction * jnp.sin(angles))


def dft_along(stacked, length, direction, pattern):
    table_re, table_im = dft_table(length, direction)

    def contract(table, part_in):
        return jnp.einsum(pattern, table, part_in, precision=lax.Precision.HIGHEST)

    real_out = contract(table_re, stacked[0]) - contract(table_im, stacked[1])
    imag_out = contract(table_re, stacked[1]) + contract(table_im, stacked[0])
    return jnp.stack([real_out, imag_out])


def grid_twiddle(devices, block, direction):
    seq_length = devices * block
    counter = jnp.arange(devices)[:, None] * jnp.arange(block)[None, :] % seq_length
    angles = direction * 2.0 * math.pi / seq_length * counter.astype(jnp.float32)
    return jnp.stack([jnp.cos(angles), jnp.sin(angles)])[:, None, None]


def local_forward(stacked, devices, block):
    array_shape = stacked.shape
    stacked = stacked.reshape(array_shape[0], array_shape[1], array_shape[2], devices, block)
    stacked = dft_along(stacked, devices, -1.0, "kj,scjp->sckp")
    stacked = complex_mul(stacked, grid_twiddle(devices, block, -1.0))
    return dft_along(stacked, block, -1.0, "kp,scjp->scjk")


def local_inverse(stacked, devices, block):
    stacked = dft_along(stacked, block, 1.0, "kp,scjp->scjk")
    stacked = complex_mul(stacked, grid_twiddle(devices, block, 1.0))
    stacked = dft_along(stacked, devices, 1.0, "kj,scjp->sckp")
    array_shape = stacked.shape
    return stacked.reshape(array_shape[0], array_shape[1], array_shape[2], devices * block) / (
        devices * block
    )


def modulated(signals, cosine, sine_part):
    zero_part = jnp.zeros_like(signals)
    return jnp.stack(
        [
            jnp.concatenate([signals, signals * cosine]),
            jnp.concatenate([zero_part, -signals * sine_part]),
        ]
    )


def spectral_products(spectrum):
    mixed_spec = spectrum[:, 0::3]
    gated_spec = spectrum[:, 1::3]
    taps_spec = spectrum[:, 2::3]
    out_spec = complex_mul(mixed_spec, taps_spec)
    back_spec = complex_mul(gated_spec, conj_of(taps_spec))
    grad_spec = complex_mul(gated_spec, conj_of(mixed_spec))
    return jnp.stack(
        [
            out_spec[:, 0],
            back_spec[:, 0],
            grad_spec[:, 0],
            out_spec[:, 1],
            back_spec[:, 1],
            grad_spec[:, 1],
        ],
        axis=1,
    )


def unfold(series, cosine, sine_part):
    return tuple(
        (
            0.5
            * (
                series[0, signal_index]
                + cosine * series[0, signal_index + 3]
                - sine_part * series[1, signal_index + 3]
            )
            for signal_index in range(3)
        )
    )


def channel_local(mixed_in, gated_cot, filter_taps, devices):
    pieces = (
        lax.all_to_all(mixed_in, "seq", split_axis=1, concat_axis=0, tiled=True),
        lax.all_to_all(gated_cot, "seq", split_axis=1, concat_axis=0, tiled=True),
        lax.all_to_all(filter_taps, "seq", split_axis=1, concat_axis=0, tiled=True),
    )
    laid = jnp.transpose(jnp.stack(pieces), (0, 2, 1))
    seq_length = laid.shape[2]
    block = seq_length // devices
    angles = math.pi / seq_length * jnp.arange(seq_length).astype(jnp.float32)
    cosine = jnp.cos(angles)
    sine_row = jnp.sin(angles)
    spectrum = local_forward(modulated(laid, cosine, sine_row), devices, block)
    series = local_inverse(spectral_products(spectrum), devices, block)
    results = unfold(series, cosine, sine_row)
    return (
        lax.all_to_all(results[0].T, "seq", split_axis=0, concat_axis=1, tiled=True),
        lax.all_to_all(results[1].T, "seq", split_axis=0, concat_axis=1, tiled=True),
        lax.all_to_all(results[2].T, "seq", split_axis=0, concat_axis=1, tiled=True),
    )


def body(query_input, key_input, value_input, cotangent, filter_taps, skip_gain):
    devices = lax.axis_size("seq")
    row_count, channels = query_input.shape
    seq_length = row_count * devices
    query_val = query_input.astype(jnp.float32)
    key_val = key_input.astype(jnp.float32)
    value_val = value_input.astype(jnp.float32)
    cot_val = cotangent.astype(jnp.float32)
    mixed_in = key_val * value_val
    gated_cot = query_val * cot_val
    conv_out, back_conv, kernel_grad = channel_local(mixed_in, gated_cot, filter_taps, devices)
    inner_sum = conv_out + skip_gain[None, :] * mixed_in
    mixed_grad = back_conv + skip_gain[None, :] * gated_cot
    output = (query_val * inner_sum).astype(jnp.bfloat16)
    query_grad = (cot_val * inner_sum).astype(jnp.bfloat16)
    key_grad = (mixed_grad * value_val).astype(jnp.bfloat16)
    value_grad = (mixed_grad * key_val).astype(jnp.bfloat16)
    time_scale = 1.0 / math.sqrt(seq_length)
    filter_grad = kernel_grad * time_scale
    filter_sq = jnp.sum(filter_grad * filter_grad)
    skip_part = jnp.sum(gated_cot * mixed_in, axis=0) * time_scale
    skip_grad = lax.psum(skip_part, "seq")
    total_sq = lax.psum(filter_sq + jnp.sum(skip_grad * skip_grad) / devices, ("seq", "ch"))
    grad_rms = jnp.sqrt(total_sq / (channels * lax.axis_size("ch") * (seq_length + 1)))
    return (output, query_grad, key_grad, value_grad, filter_grad, skip_grad, grad_rms)


def split_high_low(array):
    high = array.astype(jnp.bfloat16)
    return high, (array - high.astype(jnp.float32)).astype(jnp.bfloat16)


def half_tables(points):
    odd = 2 * np.arange(points, dtype=np.int64) + 1
    angles = math.pi / (4 * points) * (odd[:, None] * odd[None, :] % (8 * points))
    parts = []
    for table in (np.cos(angles), np.sin(angles)):
        table = table.astype(np.float32)
        high = table.astype(jnp.bfloat16)
        parts += [high, (table - high.astype(np.float32)).astype(jnp.bfloat16)]
    shift = math.pi / (4 * points) * odd[:, None] * np.ones((1, LANES))
    return np.stack(parts), np.stack([np.cos(shift), np.sin(shift)]).astype(np.float32)


def kernel(
    devices, groups, count,
    q_hbm, k_hbm, v_hbm, c_hbm, h_hbm, skip_hbm, table_hbm, twist_hbm,
    out_ref, dq_ref, dk_ref, dv_ref, dh_ref, dskip_ref, rms_ref,
    q_ref, k_ref, v_ref, c_ref, skip_ref, x_buf, g_buf, wide, flat,
    send, recv, spec, prod, back, home, extra, part_send, part_home, sq_send, sq_recv, sq_home,
    table, twist, in_send, in_recv, out_send, home_recv, extra_recv,
    part_ssem, part_rsem, sq_ssem, sq_rsem, tot_ssem, tot_rsem, load_sem, in_sem,
):
    me = lax.axis_index("seq")
    mine = lax.axis_index("ch")
    rows, channels = q_hbm.shape
    half = rows // 2
    points = half * devices
    low = LANES // 2
    time_scale = 1.0 / math.sqrt(2 * points)
    blocks = channels // LANES
    side = devices // 2
    pair = devices // 4
    split = 3 * pair
    base = me // side * side
    other = side - base
    early = me < side
    late = me >= side
    whole_here = (me >= pair) & (me < side)
    far_second = (me >= side) & (me < split)
    has_second = me < split

    barrier = pltpu.get_barrier_semaphore()
    for k in range(1, devices):
        pl.semaphore_signal(
            barrier, inc=1, device_id={"seq": lax.rem(me + k, devices)}, device_id_type=MESH
        )
    for k in range(1, groups):
        pl.semaphore_signal(
            barrier, inc=1, device_id={"ch": lax.rem(mine + k, groups)}, device_id_type=MESH
        )

    def columns_of(j):
        return pl.ds(j * LANES, LANES)

    inputs = tuple(
        pltpu.make_async_copy(source, target, in_sem.at[index])
        for index, (source, target) in enumerate(
            [(k_hbm, k_ref), (v_hbm, v_ref), (q_hbm, q_ref), (c_hbm, c_ref), (skip_hbm, skip_ref)]
            + [(h_hbm.at[:, columns_of(j)], wide.at[j]) for j in range(blocks)]
        )
    )
    for load in inputs:
        load.start()
    loads = (
        pltpu.make_async_copy(table_hbm, table, load_sem.at[0]),
        pltpu.make_async_copy(twist_hbm, twist, load_sem.at[1]),
    )
    for load in loads:
        load.start()

    def near_owner(c):
        return (c, 0) if c < pair else (c, 1) if c < side else (c - side, 1)

    def far_owner(c):
        return (side + c, 0) if c < side else (c, 1)

    def whole_owner(c):
        return (c - side, 0)

    beyond = (me // pair + 3) // 4
    my_chunk = (lax.rem(me + side * beyond, devices), me + side * (1 - beyond))

    def to_owner(signal, c, owner, lane):
        device, slot = owner
        return pltpu.make_async_remote_copy(
            src_ref=send.at[signal, c],
            dst_ref=recv.at[slot, signal, me],
            send_sem=in_send.at[signal, c, lane],
            recv_sem=in_recv.at[slot, signal, me],
            device_id={"seq": jnp.int32(device)},
            device_id_type=MESH,
        )

    def give(signal, c, owner, lane, can_be_me):
        device, slot = owner
        if not can_be_me:
            to_owner(signal, c, owner, lane).start()
            return

        @pl.when(me != device)
        def _():
            to_owner(signal, c, owner, lane).start()

        @pl.when(me == device)
        def _():
            pltpu.make_async_copy(
                send.at[signal, c], recv.at[slot, signal, me], in_recv.at[slot, signal, me]
            ).start()

    def given(signal, c, owner, lane, can_be_me):
        if not can_be_me:
            to_owner(signal, c, owner, lane).wait_send()
            return

        @pl.when(me != owner[0])
        def _():
            to_owner(signal, c, owner, lane).wait_send()

    def early_far(signal, act):
        for c in range(split):
            act(signal, c, far_owner(c), 0, False)

    def early_whole(signal, act):
        for c in range(split, devices):
            act(signal, c, whole_owner(c), 0, True)

    def early_near(signal, act):
        for c in range(split):
            act(signal, c, near_owner(c), 1, True)

    def late_all(signal, act):
        for c in range(split, devices):
            act(signal, c, whole_owner(c), 0, False)
        for c in range(split):
            act(signal, c, far_owner(c), 0, True)

    def await_input(slot, signal):
        def wait_from(start):
            for k in range(side):
                there = start + k
                pltpu.make_async_copy(
                    send.at[signal, 0], recv.at[slot, signal, there], in_recv.at[slot, signal, there]
                ).wait()

        wait_from(base)
        if slot == 0:
            crosses = whole_here if signal == 1 else me >= pair
        elif signal == 1:
            return
        else:
            crosses = far_second

        @pl.when(crosses)
        def _():
            wait_from(other)

    def to_home(slot, kind, dest):
        c = my_chunk[slot]
        return pltpu.make_async_remote_copy(
            src_ref=back.at[slot, kind, dest],
            dst_ref=home.at[kind, c],
            send_sem=out_send.at[slot, kind, dest],
            recv_sem=home_recv.at[kind, c],
            device_id={"seq": dest},
            device_id_type=MESH,
        )

    def to_extra(slot, kind, dest):
        c = my_chunk[slot]
        return pltpu.make_async_remote_copy(
            src_ref=back.at[slot, kind, dest],
            dst_ref=extra.at[kind, c],
            send_sem=out_send.at[slot, kind, dest],
            recv_sem=extra_recv.at[kind, c],
            device_id={"seq": dest},
            device_id_type=MESH,
        )

    def outward(slot, kind, act):
        if slot == 0:
            @pl.when(whole_here)
            def _():
                for k in range(side):
                    act(to_home(slot, kind, other + k))

        if kind < 2:
            @pl.when(late if slot == 0 else far_second)
            def _():
                for k in range(side):
                    act(to_extra(slot, kind, other + k))

        for k in range(1, side):
            act(to_home(slot, kind, base + lax.rem(me - base + k, side)))

    def give_back(slot, kind):
        outward(slot, kind, lambda copy: copy.start())
        c = my_chunk[slot]
        pltpu.make_async_copy(back.at[slot, kind, me], home.at[kind, c], home_recv.at[kind, c]).start()

    def given_back(slot, kind):
        outward(slot, kind, lambda copy: copy.wait_send())

    def part_copy(k):
        peer = lax.rem(me + k, devices)
        return pltpu.make_async_remote_copy(
            src_ref=part_send,
            dst_ref=part_home.at[me],
            send_sem=part_ssem.at[k],
            recv_sem=part_rsem.at[k],
            device_id={"seq": peer},
            device_id_type=MESH,
        )

    def square_copy(k):
        peer = lax.rem(mine + k, groups)
        return pltpu.make_async_remote_copy(
            src_ref=sq_send.at[0],
            dst_ref=sq_recv.at[mine],
            send_sem=sq_ssem.at[k],
            recv_sem=sq_rsem.at[k],
            device_id={"ch": peer},
            device_id_type=MESH,
        )

    def total_copy(k):
        peer = lax.rem(me + k, devices)
        return pltpu.make_async_remote_copy(
            src_ref=sq_send.at[1],
            dst_ref=sq_home.at[me],
            send_sem=tot_ssem.at[k],
            recv_sem=tot_rsem.at[k],
            device_id={"seq": peer},
            device_id_type=MESH,
        )

    first = lax.broadcasted_iota(jnp.int32, (half, LANES), 1) < low

    def pack(source, signal):
        for j in range(blocks):
            even = source[j, pl.ds(0, half, stride=2), :]
            odd = source[j, pl.ds(1, half, stride=2), :]
            send[signal, 2 * j] = jnp.where(first, even, pltpu.roll(odd, low, 1))
            send[signal, 2 * j + 1] = jnp.where(first, pltpu.roll(even, low, 1), odd)

    inputs[0].wait()
    inputs[1].wait()
    for j in range(blocks):
        at = columns_of(j)
        x_buf[j] = k_ref[:, at].astype(jnp.float32) * v_ref[:, at].astype(jnp.float32)
    pack(x_buf, 0)
    pl.semaphore_wait(barrier, devices + groups - 2)

    @pl.when(early)
    def _():
        early_far(0, give)
        early_whole(0, give)

    @pl.when(late)
    def _():
        late_all(0, give)

    inputs[2].wait()
    inputs[3].wait()
    for j in range(blocks):
        at = columns_of(j)
        g_buf[j] = q_ref[:, at].astype(jnp.float32) * c_ref[:, at].astype(jnp.float32)
    pack(g_buf, 1)

    @pl.when(early)
    def _():
        early_whole(1, give)

    @pl.when(late)
    def _():
        late_all(1, give)

    for load in inputs[4:]:
        load.wait()
    pack(wide, 2)

    @pl.when(early)
    def _():
        early_far(2, give)
        early_whole(2, give)
        for signal in range(3):
            early_near(signal, give)

    @pl.when(late)
    def _():
        late_all(2, give)

    part_send[...] = jnp.zeros((8, LANES), jnp.float32)
    for j in range(blocks):
        part_send[pl.ds(j, 1), :] = jnp.sum(x_buf[j] * g_buf[j], axis=0, keepdims=True) * time_scale
    part_home[me] = part_send[...]
    for k in range(1, devices):
        part_copy(k).start()

    nothing = jnp.zeros((side, half, LANES), jnp.float32)

    @pl.when(me < pair)
    def _():
        for signal in range(3):
            recv[0, signal, pl.ds(side, side)] = nothing

    @pl.when(early)
    def _():
        for signal in range(3):
            recv[1, signal, pl.ds(side, side)] = nothing

    @pl.when(late)
    def _():
        recv[0, 1, pl.ds(0, side)] = nothing
        recv[1, 1, pl.ds(0, side)] = nothing
        extra[...] = jnp.zeros(extra.shape, jnp.float32)

    for load in loads:
        load.wait()

    def times(which, high, rest):
        both = jnp.concatenate([high, rest], axis=1)
        main = jnp.dot(table[2 * which], both, preferred_element_type=jnp.float32)
        small = jnp.dot(table[2 * which + 1], high, preferred_element_type=jnp.float32)
        return main[:, :LANES] + (main[:, LANES:] + small)

    def forward(slot, signal):
        high, rest = split_high_low(recv[slot, signal].reshape(points, LANES))
        spec[slot, signal, 0] = times(0, high, rest)
        spec[slot, signal, 1] = -times(1, high, rest)

    def inverse(slot, kind, scale):
        real_high, real_rest = split_high_low(prod[0])
        imag_high, imag_rest = split_high_low(prod[1])
        series = times(0, real_high, real_rest) - times(1, imag_high, imag_rest)
        back[slot, kind] = (series * (scale / points)).reshape(devices, half, LANES)

    step = 128

    def halves(slot, ref_row, part, at):
        value = spec[slot, ref_row, part, at, :]
        turned = pltpu.roll(value, low, 1)
        left = lax.broadcasted_iota(jnp.int32, (step, LANES), 1) < low
        return value, turned, jnp.where(left, value, turned), jnp.where(left, turned, value)

    def products(slot, signal, other_signal, conjugate):
        sign = jnp.where(lax.broadcasted_iota(jnp.int32, (step, LANES), 1) < low, 1.0, -1.0)

        @pl.loop(0, points // step)
        def _(index):
            at = pl.ds(pl.multiple_of(index * step, step), step)
            cosine = twist[0, at, :]
            sine = twist[1, at, :]
            signed = sine * sign
            _, _, even_re, odd_re = halves(slot, other_signal, 0, at)
            _, _, even_im, odd_im = halves(slot, other_signal, 1, at)
            a_re, as_re, _, _ = halves(slot, signal, 0, at)
            a_im, as_im, _, _ = halves(slot, signal, 1, at)
            p_re = even_re * cosine - even_im * sine
            p_im = even_im * cosine + even_re * sine
            if conjugate:
                r_re = odd_re * cosine - odd_im * signed
                r_im = odd_im * cosine + odd_re * signed
                prod[0, at, :] = a_re * p_re + a_im * p_im + (as_re * r_re + as_im * r_im)
                prod[1, at, :] = a_im * p_re - a_re * p_im + (as_im * r_re - as_re * r_im)
            else:
                r_re = odd_re * cosine + odd_im * signed
                r_im = odd_im * cosine - odd_re * signed
                prod[0, at, :] = a_re * p_re - a_im * p_im + (as_re * r_re - as_im * r_im)
                prod[1, at, :] = a_im * p_re + a_re * p_im + (as_im * r_re + as_re * r_im)

    def begin(slot):
        await_input(slot, 0)
        forward(slot, 0)
        await_input(slot, 1)
        forward(slot, 1)
        products(slot, 1, 0, True)
        inverse(slot, 0, time_scale)
        give_back(slot, 0)

    def finish(slot):
        await_input(slot, 2)
        forward(slot, 2)
        products(slot, 1, 2, True)
        inverse(slot, 1, 1.0)
        give_back(slot, 1)
        products(slot, 0, 2, False)
        inverse(slot, 2, 1.0)
        give_back(slot, 2)

    begin(0)

    @pl.when(has_second)
    def _():
        begin(1)

    finish(0)

    @pl.when(has_second)
    def _():
        finish(1)

    def await_home(kind, c):
        pltpu.make_async_copy(back.at[0, 0, 0], home.at[kind, c], home_recv.at[kind, c]).wait()

    def await_extra(kind, c):
        pltpu.make_async_copy(back.at[0, 0, 0], extra.at[kind, c], extra_recv.at[kind, c]).wait()

    def unpack(kind, j):
        pieces = []
        for c in (2 * j, 2 * j + 1):
            await_home(kind, c)
        if kind < 2 and 2 * j < split:
            @pl.when(early)
            def _():
                for c in (2 * j, 2 * j + 1):
                    await_extra(kind, c)

            pieces = [home[kind, c] + extra[kind, c] for c in (2 * j, 2 * j + 1)]
        else:
            pieces = [home[kind, c] for c in (2 * j, 2 * j + 1)]
        left, right = pieces
        flat[j, pl.ds(0, half, stride=2), :] = jnp.where(first, left, pltpu.roll(right, low, 1))
        flat[j, pl.ds(1, half, stride=2), :] = jnp.where(first, pltpu.roll(left, low, 1), right)
        return flat[j]

    for k in range(1, devices):
        part_copy(k).wait_recv()
    direct = part_home[0]
    for k in range(1, devices):
        direct = direct + part_home[k]
    for j in range(blocks):
        dskip_ref[:, columns_of(j)] = direct[j : j + 1]

    squares = direct * direct * (1.0 / devices)
    for j in reversed(range(blocks)):
        value = unpack(0, j)
        dh_ref[:, columns_of(j)] = value
        squares = squares + jnp.sum((value * value).reshape(rows // 8, 8, LANES), axis=0)
    sq_send[0] = squares
    sq_recv[mine] = squares
    for k in range(1, groups):
        square_copy(k).start()

    @pl.when(early)
    def _():
        early_far(0, given)
        early_far(2, given)
        for signal in range(3):
            early_whole(signal, given)
            early_near(signal, given)

    @pl.when(late)
    def _():
        for signal in range(3):
            late_all(signal, given)

    for k in range(1, devices):
        part_copy(k).wait_send()

    given_back(0, 0)

    @pl.when(has_second)
    def _():
        given_back(1, 0)

    for k in range(1, groups):
        square_copy(k).wait_recv()
    total = sq_recv[0]
    for k in range(1, groups):
        total = total + sq_recv[k]
    sq_send[1] = total
    sq_home[me] = total
    for k in range(1, devices):
        total_copy(k).start()

    for j in reversed(range(blocks)):
        at = columns_of(j)
        inner = unpack(2, j) + skip_ref[:, at] * x_buf[j]
        out_ref[:, at] = (q_ref[:, at].astype(jnp.float32) * inner).astype(jnp.bfloat16)
        dq_ref[:, at] = (c_ref[:, at].astype(jnp.float32) * inner).astype(jnp.bfloat16)

    for k in range(1, devices):
        total_copy(k).wait_recv()
    total = sq_home[0]
    for k in range(1, devices):
        total = total + sq_home[k]
    total = jnp.sum(jnp.sum(total, axis=0, keepdims=True), axis=1, keepdims=True)
    rms_ref[...] = jnp.sqrt(total / count)
    for k in range(1, groups):
        square_copy(k).wait_send()
    for k in range(1, devices):
        total_copy(k).wait_send()

    for j in reversed(range(blocks)):
        at = columns_of(j)
        grad = unpack(1, j) + skip_ref[:, at] * g_buf[j]
        dk_ref[:, at] = (grad * v_ref[:, at].astype(jnp.float32)).astype(jnp.bfloat16)
        dv_ref[:, at] = (grad * k_ref[:, at].astype(jnp.float32)).astype(jnp.bfloat16)

    for kind in (1, 2):
        given_back(0, kind)

    @pl.when(has_second)
    def _():
        for kind in (1, 2):
            given_back(1, kind)


def emit(*refs):
    sources, targets, sem = refs[:7], refs[7:14], refs[14]
    copies = [
        pltpu.make_async_copy(source, target, sem.at[index])
        for index, (source, target) in enumerate(zip(sources, targets))
    ]
    for copy in copies:
        copy.start()
    for copy in copies:
        copy.wait()


def fused_body(query_input, key_input, value_input, cotangent, filter_taps, skip_gain):
    devices = lax.axis_size("seq")
    groups = lax.axis_size("ch")
    rows, channels = query_input.shape
    half = rows // 2
    points = half * devices
    tables, twists = half_tables(points)
    count = float(channels * groups * (rows * devices + 1))
    vmem = pl.BlockSpec(memory_space=pltpu.VMEM)
    hbm = pl.BlockSpec(memory_space=pltpu.HBM)
    chunks = 2 * channels // LANES
    blocks = channels // LANES
    shapes = [((rows, channels), jnp.bfloat16)] * 4 + [
        ((rows, channels), jnp.float32),
        ((1, channels), jnp.float32),
        ((1, 1), jnp.float32),
    ]
    held = pl.pallas_call(
        functools.partial(kernel, devices, groups, count),
        out_shape=tuple(pltpu.VMEM(*shape) for shape in shapes),
        in_specs=[hbm] * 8,
        out_specs=(vmem,) * 7,
        scratch_shapes=[
            pltpu.VMEM((rows, channels), jnp.bfloat16),
            pltpu.VMEM((rows, channels), jnp.bfloat16),
            pltpu.VMEM((rows, channels), jnp.bfloat16),
            pltpu.VMEM((rows, channels), jnp.bfloat16),
            pltpu.VMEM((1, channels), jnp.float32),
            pltpu.VMEM((blocks, rows, LANES), jnp.float32),
            pltpu.VMEM((blocks, rows, LANES), jnp.float32),
            pltpu.VMEM((blocks, rows, LANES), jnp.float32),
            pltpu.VMEM((blocks, rows, LANES), jnp.float32),
            pltpu.VMEM((3, chunks, half, LANES), jnp.float32),
            pltpu.VMEM((2, 3, devices, half, LANES), jnp.float32),
            pltpu.VMEM((2, 3, 2, points, LANES), jnp.float32),
            pltpu.VMEM((2, points, LANES), jnp.float32),
            pltpu.VMEM((2, 3, devices, half, LANES), jnp.float32),
            pltpu.VMEM((3, chunks, half, LANES), jnp.float32),
            pltpu.VMEM((2, 3 * (devices // 4), half, LANES), jnp.float32),
            pltpu.VMEM((8, LANES), jnp.float32),
            pltpu.VMEM((devices, 8, LANES), jnp.float32),
            pltpu.VMEM((2, 8, LANES), jnp.float32),
            pltpu.VMEM((groups, 8, LANES), jnp.float32),
            pltpu.VMEM((devices, 8, LANES), jnp.float32),
            pltpu.VMEM(tables.shape, jnp.bfloat16),
            pltpu.VMEM(twists.shape, jnp.float32),
            pltpu.SemaphoreType.DMA((3, chunks, 2)),
            pltpu.SemaphoreType.DMA((2, 3, devices)),
            pltpu.SemaphoreType.DMA((2, 3, devices)),
            pltpu.SemaphoreType.DMA((3, chunks)),
            pltpu.SemaphoreType.DMA((2, 3 * (devices // 4))),
            pltpu.SemaphoreType.DMA((devices,)),
            pltpu.SemaphoreType.DMA((devices,)),
            pltpu.SemaphoreType.DMA((groups,)),
            pltpu.SemaphoreType.DMA((groups,)),
            pltpu.SemaphoreType.DMA((devices,)),
            pltpu.SemaphoreType.DMA((devices,)),
            pltpu.SemaphoreType.DMA((2,)),
            pltpu.SemaphoreType.DMA((5 + blocks,)),
        ],
        compiler_params=pltpu.CompilerParams(
            collective_id=0, has_side_effects=True, vmem_limit_bytes=(64 << 20) - (960 << 10)
        ),
    )(
        query_input, key_input, value_input, cotangent, filter_taps,
        skip_gain.reshape(1, channels), jnp.asarray(tables), jnp.asarray(twists),
    )
    results = pl.pallas_call(
        emit,
        out_shape=tuple(jax.ShapeDtypeStruct(*shape) for shape in shapes),
        in_specs=[vmem] * 7,
        out_specs=(hbm,) * 7,
        scratch_shapes=[pltpu.SemaphoreType.DMA((7,))],
        compiler_params=pltpu.CompilerParams(vmem_limit_bytes=4 << 20),
    )(*held)
    return (*results[:5], results[5].reshape(channels), results[6].reshape(()))


def pick_body(query_input, *others):
    devices = lax.axis_size("seq")
    rows, channels = query_input.shape
    fits = devices == 8 and 2 * channels == LANES * devices and rows % 16 == 0
    chosen = fused_body if fits and rows * devices <= 2048 else body
    return chosen(query_input, *others)


def solution(mesh):
    return jax.shard_map(
        pick_body,
        mesh=mesh,
        in_specs=(
            P("seq", "ch"),
            P("seq", "ch"),
            P("seq", "ch"),
            P("seq", "ch"),
            P("seq", "ch"),
            P("ch"),
        ),
        out_specs=(
            P("seq", "ch"),
            P("seq", "ch"),
            P("seq", "ch"),
            P("seq", "ch"),
            P("seq", "ch"),
            P("ch"),
            P(),
        ),
        check_vma=False,
    )
```

```python
import functools
import math

import jax
import jax.numpy as jnp
import numpy as np
from jax import lax
from jax.experimental import pallas as pl
from jax.experimental.pallas import tpu as pltpu
from jax.sharding import PartitionSpec as P

LANES = 128
MESH = pl.DeviceIdType.MESH


def complex_mul(left_op, right_op):
    return jnp.stack(
        [
            left_op[0] * right_op[0] - left_op[1] * right_op[1],
            left_op[0] * right_op[1] + left_op[1] * right_op[0],
        ]
    )


def conj_of(stacked):
    return jnp.stack([stacked[0], -stacked[1]])


def dft_table(length, direction):
    counter = jnp.arange(length)
    angles = (
        2.0 * math.pi / length * (counter[:, None] * counter[None, :] % length).astype(jnp.float32)
    )
    return (jnp.cos(angles), direction * jnp.sin(angles))


def dft_along(stacked, length, direction, pattern):
    table_re, table_im = dft_table(length, direction)

    def contract(table, part_in):
        return jnp.einsum(pattern, table, part_in, precision=lax.Precision.HIGHEST)

    real_out = contract(table_re, stacked[0]) - contract(table_im, stacked[1])
    imag_out = contract(table_re, stacked[1]) + contract(table_im, stacked[0])
    return jnp.stack([real_out, imag_out])


def grid_twiddle(devices, block, direction):
    seq_length = devices * block
    counter = jnp.arange(devices)[:, None] * jnp.arange(block)[None, :] % seq_length
    angles = direction * 2.0 * math.pi / seq_length * counter.astype(jnp.float32)
    return jnp.stack([jnp.cos(angles), jnp.sin(angles)])[:, None, None]


def local_forward(stacked, devices, block):
    array_shape = stacked.shape
    stacked = stacked.reshape(array_shape[0], array_shape[1], array_shape[2], devices, block)
    stacked = dft_along(stacked, devices, -1.0, "kj,scjp->sckp")
    stacked = complex_mul(stacked, grid_twiddle(devices, block, -1.0))
    return dft_along(stacked, block, -1.0, "kp,scjp->scjk")


def local_inverse(stacked, devices, block):
    stacked = dft_along(stacked, block, 1.0, "kp,scjp->scjk")
    stacked = complex_mul(stacked, grid_twiddle(devices, block, 1.0))
    stacked = dft_along(stacked, devices, 1.0, "kj,scjp->sckp")
    array_shape = stacked.shape
    return stacked.reshape(array_shape[0], array_shape[1], array_shape[2], devices * block) / (
        devices * block
    )


def modulated(signals, cosine, sine_part):
    zero_part = jnp.zeros_like(signals)
    return jnp.stack(
        [
            jnp.concatenate([signals, signals * cosine]),
            jnp.concatenate([zero_part, -signals * sine_part]),
        ]
    )


def spectral_products(spectrum):
    mixed_spec = spectrum[:, 0::3]
    gated_spec = spectrum[:, 1::3]
    taps_spec = spectrum[:, 2::3]
    out_spec = complex_mul(mixed_spec, taps_spec)
    back_spec = complex_mul(gated_spec, conj_of(taps_spec))
    grad_spec = complex_mul(gated_spec, conj_of(mixed_spec))
    return jnp.stack(
        [
            out_spec[:, 0],
            back_spec[:, 0],
            grad_spec[:, 0],
            out_spec[:, 1],
            back_spec[:, 1],
            grad_spec[:, 1],
        ],
        axis=1,
    )


def unfold(series, cosine, sine_part):
    return tuple(
        (
            0.5
            * (
                series[0, signal_index]
                + cosine * series[0, signal_index + 3]
                - sine_part * series[1, signal_index + 3]
            )
            for signal_index in range(3)
        )
    )


def channel_local(mixed_in, gated_cot, filter_taps, devices):
    pieces = (
        lax.all_to_all(mixed_in, "seq", split_axis=1, concat_axis=0, tiled=True),
        lax.all_to_all(gated_cot, "seq", split_axis=1, concat_axis=0, tiled=True),
        lax.all_to_all(filter_taps, "seq", split_axis=1, concat_axis=0, tiled=True),
    )
    laid = jnp.transpose(jnp.stack(pieces), (0, 2, 1))
    seq_length = laid.shape[2]
    block = seq_length // devices
    angles = math.pi / seq_length * jnp.arange(seq_length).astype(jnp.float32)
    cosine = jnp.cos(angles)
    sine_row = jnp.sin(angles)
    spectrum = local_forward(modulated(laid, cosine, sine_row), devices, block)
    series = local_inverse(spectral_products(spectrum), devices, block)
    results = unfold(series, cosine, sine_row)
    return (
        lax.all_to_all(results[0].T, "seq", split_axis=0, concat_axis=1, tiled=True),
        lax.all_to_all(results[1].T, "seq", split_axis=0, concat_axis=1, tiled=True),
        lax.all_to_all(results[2].T, "seq", split_axis=0, concat_axis=1, tiled=True),
    )


def body(query_input, key_input, value_input, cotangent, filter_taps, skip_gain):
    devices = lax.axis_size("seq")
    row_count, channels = query_input.shape
    seq_length = row_count * devices
    query_val = query_input.astype(jnp.float32)
    key_val = key_input.astype(jnp.float32)
    value_val = value_input.astype(jnp.float32)
    cot_val = cotangent.astype(jnp.float32)
    mixed_in = key_val * value_val
    gated_cot = query_val * cot_val
    conv_out, back_conv, kernel_grad = channel_local(mixed_in, gated_cot, filter_taps, devices)
    inner_sum = conv_out + skip_gain[None, :] * mixed_in
    mixed_grad = back_conv + skip_gain[None, :] * gated_cot
    output = (query_val * inner_sum).astype(jnp.bfloat16)
    query_grad = (cot_val * inner_sum).astype(jnp.bfloat16)
    key_grad = (mixed_grad * value_val).astype(jnp.bfloat16)
    value_grad = (mixed_grad * key_val).astype(jnp.bfloat16)
    time_scale = 1.0 / math.sqrt(seq_length)
    filter_grad = kernel_grad * time_scale
    filter_sq = jnp.sum(filter_grad * filter_grad)
    skip_part = jnp.sum(gated_cot * mixed_in, axis=0) * time_scale
    skip_grad = lax.psum(skip_part, "seq")
    total_sq = lax.psum(filter_sq + jnp.sum(skip_grad * skip_grad) / devices, ("seq", "ch"))
    grad_rms = jnp.sqrt(total_sq / (channels * lax.axis_size("ch") * (seq_length + 1)))
    return (output, query_grad, key_grad, value_grad, filter_grad, skip_grad, grad_rms)


def split_high_low(array):
    high = array.astype(jnp.bfloat16)
    return high, (array - high.astype(jnp.float32)).astype(jnp.bfloat16)


def half_tables(points):
    odd = 2 * np.arange(points, dtype=np.int64) + 1
    angles = math.pi / (4 * points) * (odd[:, None] * odd[None, :] % (8 * points))
    parts = []
    for table in (np.cos(angles), np.sin(angles)):
        table = table.astype(np.float32)
        high = table.astype(jnp.bfloat16)
        parts += [high, (table - high.astype(np.float32)).astype(jnp.bfloat16)]
    shift = math.pi / (4 * points) * odd[:, None] * np.ones((1, LANES))
    return np.stack(parts), np.stack([np.cos(shift), np.sin(shift)]).astype(np.float32)


def kernel(
    devices, groups, count,
    k_hbm, v_hbm, q_hbm, c_hbm, h_hbm, skip_hbm, table_hbm, twist_hbm,
    out_ref, dq_ref, dk_ref, dv_ref, dh_ref, dskip_ref, rms_ref,
    gates, skip_ref, x_buf, g_buf, wide, flat,
    send, recv, spec, prod, back, home, extra,
    part_send, part_home, sq_acc, sq_send, sq_recv, sq_home, table, twist,
    load_sem, in_send, in_recv, out_send, home_recv, extra_recv, small_send, small_recv,
):
    me = lax.axis_index("seq")
    mine = lax.axis_index("ch")
    rows, channels = q_hbm.shape
    half = rows // 2
    points = half * devices
    low = LANES // 2
    time_scale = 1.0 / math.sqrt(2 * points)
    blocks = channels // LANES
    side = devices // 2
    pair = devices // 4
    split = 3 * pair
    base = me // side * side
    other = side - base
    early = me < side
    late = me >= side
    near_here = me < pair
    whole_here = (me >= pair) & (me < side)
    far_two = (me >= side) & (me < split)
    far_one = me >= split

    barrier = pltpu.get_barrier_semaphore()
    for k in range(1, devices):
        pl.semaphore_signal(
            barrier, inc=1, device_id={"seq": lax.rem(me + k, devices)}, device_id_type=MESH
        )
    for k in range(1, groups):
        pl.semaphore_signal(
            barrier, inc=1, device_id={"ch": lax.rem(mine + k, groups)}, device_id_type=MESH
        )

    def columns_of(j):
        return pl.ds(j * LANES, LANES)

    for index, source in enumerate((k_hbm, v_hbm, q_hbm, c_hbm)):
        pltpu.make_async_copy(source, gates.at[index], load_sem.at[index // 2]).start()
    for j in range(blocks):
        pltpu.make_async_copy(h_hbm.at[:, columns_of(j)], wide.at[j], load_sem.at[2]).start()
    loads = (
        pltpu.make_async_copy(skip_hbm, skip_ref, load_sem.at[3]),
        pltpu.make_async_copy(table_hbm, table, load_sem.at[4]),
        pltpu.make_async_copy(twist_hbm, twist, load_sem.at[5]),
    )
    for load in loads:
        load.start()

    def gate(index, j):
        return gates[index, :, columns_of(j)].astype(jnp.float32)

    def wait_bytes(ref, sem):
        pltpu.make_async_copy(ref, ref, sem).wait()

    def near_owner(c):
        return (c % pair, c // pair)

    def far_owner(c):
        return (side + c, 0) if c < side else (c, 1)

    def whole_owner(c):
        return (c - side, 0)

    def give(signal, c, owner, can_be_me):
        device, slot = owner
        target = recv.at[(slot * 3 + signal) * devices + me]
        sem = in_recv.at[slot * 3 + signal]

        def remote():
            pltpu.make_async_remote_copy(
                src_ref=send.at[signal, c],
                dst_ref=target,
                send_sem=in_send.at[0],
                recv_sem=sem,
                device_id={"seq": jnp.int32(device)},
                device_id_type=MESH,
            ).start()

        if not can_be_me:
            remote()
            return

        pl.when(me != device)(remote)

        @pl.when(me == device)
        def _():
            pltpu.make_async_copy(send.at[signal, c], target, sem).start()

    def give_far(signal, chunks, can_be_me=False):
        for c in chunks:
            give(signal, c, far_owner(c), can_be_me)

    def give_whole(signal, can_be_me=False):
        for c in range(split, devices):
            give(signal, c, whole_owner(c), can_be_me)

    def give_near(signal, slot, can_be_me=False):
        for c in range(slot * pair, (slot + 1) * pair):
            give(signal, c, near_owner(c), can_be_me)

    def await_input(slot, signal, start, sources):
        first_one = (slot * 3 + signal) * devices + start
        wait_bytes(recv.at[pl.ds(first_one, sources)], in_recv.at[slot * 3 + signal])

    def to_home(slot, kind, c, dest):
        pltpu.make_async_remote_copy(
            src_ref=back.at[slot, kind, dest],
            dst_ref=home.at[kind, c],
            send_sem=out_send.at[0],
            recv_sem=home_recv.at[kind],
            device_id={"seq": dest},
            device_id_type=MESH,
        ).start()

    def to_extra(slot, kind, c, dest):
        pltpu.make_async_remote_copy(
            src_ref=back.at[slot, kind, dest],
            dst_ref=extra.at[kind, c],
            send_sem=out_send.at[0],
            recv_sem=extra_recv.at[kind],
            device_id={"seq": dest},
            device_id_type=MESH,
        ).start()

    def inward(slot, kind, c):
        for k in range(1, side):
            to_home(slot, kind, c, base + lax.rem(me - base + k, side))
        pltpu.make_async_copy(back.at[slot, kind, me], home.at[kind, c], home_recv.at[kind]).start()

    def small_copy(source, target, index, device_id):
        return pltpu.make_async_remote_copy(
            src_ref=source,
            dst_ref=target,
            send_sem=small_send.at[index],
            recv_sem=small_recv.at[index],
            device_id=device_id,
            device_id_type=MESH,
        )

    def to_peers(source, target, index):
        for k in range(1, devices):
            peer = lax.rem(me + k, devices)
            small_copy(source, target.at[me], index, {"seq": peer}).start()

    def share_squares(squares):
        sq_send[0] = squares
        sq_recv[mine] = squares
        for k in range(1, groups):
            peer = lax.rem(mine + k, groups)
            small_copy(sq_send.at[0], sq_recv.at[mine], 1, {"ch": peer}).start()

    def share_totals():
        wait_bytes(sq_recv.at[pl.ds(0, groups - 1)], small_recv.at[1])
        total = sq_recv[0]
        for k in range(1, groups):
            total = total + sq_recv[k]
        sq_send[1] = total
        sq_home[me] = total
        to_peers(sq_send.at[1], sq_home, 2)

    first = lax.broadcasted_iota(jnp.int32, (half, LANES), 1) < low

    def pack(source, signal):
        for j in range(blocks):
            even = source[j, pl.ds(0, half, stride=2), :]
            odd = source[j, pl.ds(1, half, stride=2), :]
            send[signal, 2 * j] = jnp.where(first, even, pltpu.roll(odd, low, 1))
            send[signal, 2 * j + 1] = jnp.where(first, pltpu.roll(even, low, 1), odd)

    wait_bytes(gates.at[pl.ds(0, 2)], load_sem.at[0])
    for j in range(blocks):
        x_buf[j] = gate(0, j) * gate(1, j)
    pack(x_buf, 0)
    pl.semaphore_wait(barrier, devices + groups - 2)

    @pl.when(early)
    def _():
        give_far(0, range(split))

    @pl.when(near_here)
    def _():
        give_whole(0)

    @pl.when(whole_here)
    def _():
        give_near(0, 0)
        give_whole(0, True)

    @pl.when(late)
    def _():
        give_whole(0)
        give_far(0, range(side), True)

    wait_bytes(gates.at[pl.ds(2, 2)], load_sem.at[1])
    for j in range(blocks):
        g_buf[j] = gate(2, j) * gate(3, j)
    pack(g_buf, 1)

    @pl.when(near_here)
    def _():
        give_whole(1)

    @pl.when(whole_here)
    def _():
        give_near(1, 0)
        give_whole(1, True)
        for slot in (1, 2):
            for signal in (0, 1):
                give_near(signal, slot)

    @pl.when(late)
    def _():
        give_whole(1)
        give_far(1, range(side), True)
        for signal in (0, 1):
            give_far(signal, range(side, split), True)

    wait_bytes(wide, load_sem.at[2])
    pack(wide, 2)

    @pl.when(near_here)
    def _():
        give_far(2, range(split))
        give_whole(2)
        for signal in range(3):
            for slot in range(3):
                give_near(signal, slot, True)

    @pl.when(whole_here)
    def _():
        give_whole(2, True)
        for slot in range(3):
            give_near(2, slot)

    @pl.when(late)
    def _():
        give_whole(2)
        give_far(2, range(split), True)
        extra[...] = jnp.zeros(extra.shape, jnp.float32)

    part_send[...] = jnp.zeros((8, LANES), jnp.float32)
    for j in range(blocks):
        part_send[pl.ds(j, 1), :] = jnp.sum(x_buf[j] * g_buf[j], axis=0, keepdims=True) * time_scale
    part_home[me] = part_send[...]
    to_peers(part_send, part_home, 0)
    sq_acc[...] = jnp.zeros((8, LANES), jnp.float32)
    for load in loads:
        load.wait()

    def times(which, pieces, at_row, at_column):
        high, rest = pieces
        both = jnp.concatenate([high, rest], axis=1)
        main = jnp.dot(
            table[2 * which, at_row, at_column], both, preferred_element_type=jnp.float32
        )
        small = jnp.dot(
            table[2 * which + 1, at_row, at_column], high, preferred_element_type=jnp.float32
        )
        return main[:, :LANES] + (main[:, LANES:] + small)

    full = slice(0, points)
    early_part = slice(0, points // 2)
    late_part = slice(points // 2, points)

    def forward(slot, signal, part):
        start = (slot * 3 + signal) * devices + part.start // half
        sources = (part.stop - part.start) // half
        data = recv[pl.ds(start, sources)].reshape(sources * half, LANES)
        pieces = split_high_low(data)
        spec[slot, signal, 0] = times(0, pieces, full, part)
        spec[slot, signal, 1] = -times(1, pieces, full, part)

    def inverse(slot, kind, part, scale):
        series = times(0, split_high_low(prod[0]), part, full)
        series = series - times(1, split_high_low(prod[1]), part, full)
        series = series * (scale / points)
        start = part.start // half
        sources = (part.stop - part.start) // half
        back[slot, kind, start : start + sources] = series.reshape(sources, half, LANES)
        return series

    def square_sum(series):
        sq_acc[...] += jnp.sum((series * series).reshape(side * half // 8, 8, LANES), axis=0)

    step = 128

    def halves(slot, ref_row, part, at):
        value = spec[slot, ref_row, part, at, :]
        turned = pltpu.roll(value, low, 1)
        left = lax.broadcasted_iota(jnp.int32, (step, LANES), 1) < low
        return value, turned, jnp.where(left, value, turned), jnp.where(left, turned, value)

    def products(slot, signal, other_signal, conjugate):
        sign = jnp.where(lax.broadcasted_iota(jnp.int32, (step, LANES), 1) < low, 1.0, -1.0)

        @pl.loop(0, points // step)
        def _(index):
            at = pl.ds(pl.multiple_of(index * step, step), step)
            cosine = twist[0, at, :]
            sine = twist[1, at, :]
            signed = sine * sign
            _, _, even_re, odd_re = halves(slot, other_signal, 0, at)
            _, _, even_im, odd_im = halves(slot, other_signal, 1, at)
            a_re, as_re, _, _ = halves(slot, signal, 0, at)
            a_im, as_im, _, _ = halves(slot, signal, 1, at)
            p_re = even_re * cosine - even_im * sine
            p_im = even_im * cosine + even_re * sine
            if conjugate:
                r_re = odd_re * cosine - odd_im * signed
                r_im = odd_im * cosine + odd_re * signed
                prod[0, at, :] = a_re * p_re + a_im * p_im + (as_re * r_re + as_im * r_im)
                prod[1, at, :] = a_im * p_re - a_re * p_im + (as_im * r_re - as_re * r_im)
            else:
                r_re = odd_re * cosine + odd_im * signed
                r_im = odd_im * cosine - odd_re * signed
                prod[0, at, :] = a_re * p_re - a_im * p_im + (as_re * r_re - as_im * r_im)
                prod[1, at, :] = a_im * p_re + a_re * p_im + (as_im * r_re + as_re * r_im)

    @pl.when(near_here)
    def _():
        @pl.loop(0, 3)
        def _(slot):
            c = slot * pair + me
            for signal in (0, 1):
                await_input(slot, signal, 0, side)
                forward(slot, signal, early_part)
            products(slot, 1, 0, True)
            inverse(slot, 0, early_part, time_scale)
            inward(slot, 0, c)

        @pl.loop(0, 3)
        def _(slot):
            c = slot * pair + me
            await_input(slot, 2, 0, side)
            forward(slot, 2, early_part)
            products(slot, 1, 2, True)
            inverse(slot, 1, early_part, 1.0)
            inward(slot, 1, c)
            products(slot, 0, 2, False)
            inverse(slot, 2, early_part, 1.0)
            inward(slot, 2, c)

    def outward(slot, kind, c):
        @pl.when(whole_here)
        def _():
            for k in range(side):
                to_home(slot, kind, c, other + k)

        if kind < 2:
            @pl.when(late)
            def _():
                for k in range(side):
                    to_extra(slot, kind, c, other + k)

        inward(slot, kind, c)

    @pl.when(me >= pair)
    def _():
        zone = me // pair
        slots = 2 - lax.rem(zone, 2)

        @pl.when(late)
        def _():
            await_input(0, 1, side, side)

        @pl.loop(0, slots)
        def _(slot):
            c = lax.rem(me + side + side * slot, devices)

            @pl.when(late & (slot > 0))
            def _():
                await_input(slot, 1, side, side)

            @pl.when(late)
            def _():
                forward(slot, 1, late_part)

            await_input(slot, 0, 0, devices)

            @pl.when(whole_here)
            def _():
                give_far(2, range(split))
                await_input(slot, 1, 0, devices)
                forward(slot, 1, full)

            forward(slot, 0, full)
            products(slot, 1, 0, True)
            series = inverse(slot, 0, full, time_scale)
            outward(slot, 0, c)
            square_sum(series[points // 2 :])

        @pl.when(late)
        def _():
            share_squares(sq_acc[...])

        await_input(0, 2, 0, devices)

        @pl.when(late)
        def _():
            share_totals()

        @pl.loop(0, slots)
        def _(slot):
            c = lax.rem(me + side + side * slot, devices)

            @pl.when(slot > 0)
            def _():
                await_input(slot, 2, 0, devices)

            forward(slot, 2, full)
            products(slot, 1, 2, True)
            inverse(slot, 1, full, 1.0)
            outward(slot, 1, c)
            products(slot, 0, 2, False)
            inverse(slot, 2, full, 1.0)
            outward(slot, 2, c)

    def await_home(kind):
        wait_bytes(home.at[kind], home_recv.at[kind])
        if kind < 2:
            @pl.when(early)
            def _():
                wait_bytes(extra.at[kind], extra_recv.at[kind])

    def unpack(kind, j):
        pieces = []
        for c in (2 * j, 2 * j + 1):
            value = home[kind, c]
            pieces.append(value + extra[kind, c] if kind < 2 and c < split else value)
        left, right = pieces
        flat[j, pl.ds(0, half, stride=2), :] = jnp.where(first, left, pltpu.roll(right, low, 1))
        flat[j, pl.ds(1, half, stride=2), :] = jnp.where(first, pltpu.roll(left, low, 1), right)
        return flat[j]

    wait_bytes(part_home.at[pl.ds(0, devices - 1)], small_recv.at[0])
    direct = part_home[0]
    for k in range(1, devices):
        direct = direct + part_home[k]
    for j in range(blocks):
        dskip_ref[:, columns_of(j)] = direct[j : j + 1]

    await_home(0)
    squares = sq_acc[...] + direct * direct * (1.0 / side)
    for j in range(blocks):
        value = unpack(0, j)
        dh_ref[:, columns_of(j)] = value
        squares = squares + jnp.sum((value * value).reshape(rows // 8, 8, LANES), axis=0)

    @pl.when(early)
    def _():
        share_squares(squares)

    def assemble_inner():
        await_home(2)
        for j in range(blocks):
            at = columns_of(j)
            inner = unpack(2, j) + skip_ref[:, at] * x_buf[j]
            out_ref[:, at] = (gate(2, j) * inner).astype(jnp.bfloat16)
            dq_ref[:, at] = (gate(3, j) * inner).astype(jnp.bfloat16)

    def assemble_grad():
        await_home(1)
        for j in range(blocks):
            at = columns_of(j)
            grad = unpack(1, j) + skip_ref[:, at] * g_buf[j]
            dk_ref[:, at] = (grad * gate(1, j)).astype(jnp.bfloat16)
            dv_ref[:, at] = (grad * gate(0, j)).astype(jnp.bfloat16)

    @pl.when(near_here)
    def _():
        assemble_inner()

    @pl.when(early)
    def _():
        share_totals()

    @pl.when(me >= pair)
    def _():
        assemble_inner()

    assemble_grad()

    wait_bytes(sq_home.at[pl.ds(0, devices - 1)], small_recv.at[2])
    total = sq_home[0]
    for k in range(1, devices):
        total = total + sq_home[k]
    total = jnp.sum(jnp.sum(total, axis=0, keepdims=True), axis=1, keepdims=True)
    rms_ref[...] = jnp.sqrt(total / count)

    for condition, sent, returned in (
        (near_here, 3 * (split - 3) + 2 * split + 3 * pair, 9 * (side - 1)),
        (whole_here, 5 * split + 3 * (pair - 1), 3 * (devices - 1)),
        (far_two, 3 * (split - 2) + 3 * pair, 2 * (2 * side + 3 * (side - 1))),
        (far_one, 3 * (split - 1) + 3 * pair, 2 * side + 3 * (side - 1)),
    ):
        @pl.when(condition)
        def _():
            wait_bytes(recv.at[pl.ds(0, sent)], in_send.at[0])
            wait_bytes(recv.at[pl.ds(0, returned)], out_send.at[0])

    wait_bytes(part_home.at[pl.ds(0, devices - 1)], small_send.at[0])
    wait_bytes(sq_recv.at[pl.ds(0, groups - 1)], small_send.at[1])
    wait_bytes(sq_home.at[pl.ds(0, devices - 1)], small_send.at[2])


def emit(*refs):
    sources, targets, sem = refs[:7], refs[7:14], refs[14]
    copies = [
        pltpu.make_async_copy(source, target, sem.at[index])
        for index, (source, target) in enumerate(zip(sources, targets))
    ]
    for copy in copies:
        copy.start()
    for copy in copies:
        copy.wait()


def fused_body(query_input, key_input, value_input, cotangent, filter_taps, skip_gain):
    devices = lax.axis_size("seq")
    groups = lax.axis_size("ch")
    rows, channels = query_input.shape
    half = rows // 2
    points = half * devices
    tables, twists = half_tables(points)
    count = float(channels * groups * (rows * devices + 1))
    vmem = pl.BlockSpec(memory_space=pltpu.VMEM)
    hbm = pl.BlockSpec(memory_space=pltpu.HBM)
    chunks = 2 * channels // LANES
    blocks = channels // LANES
    shapes = [((rows, channels), jnp.bfloat16)] * 4 + [
        ((rows, channels), jnp.float32),
        ((1, channels), jnp.float32),
        ((1, 1), jnp.float32),
    ]
    held = pl.pallas_call(
        functools.partial(kernel, devices, groups, count),
        out_shape=tuple(pltpu.VMEM(*shape) for shape in shapes),
        in_specs=[hbm] * 8,
        out_specs=(vmem,) * 7,
        scratch_shapes=[
            pltpu.VMEM((4, rows, channels), jnp.bfloat16),
            pltpu.VMEM((1, channels), jnp.float32),
            pltpu.VMEM((blocks, rows, LANES), jnp.float32),
            pltpu.VMEM((blocks, rows, LANES), jnp.float32),
            pltpu.VMEM((blocks, rows, LANES), jnp.float32),
            pltpu.VMEM((blocks, rows, LANES), jnp.float32),
            pltpu.VMEM((3, chunks, half, LANES), jnp.float32),
            pltpu.VMEM((9 * devices, half, LANES), jnp.float32),
            pltpu.VMEM((3, 3, 2, points, LANES), jnp.float32),
            pltpu.VMEM((2, points, LANES), jnp.float32),
            pltpu.VMEM((3, 3, devices, half, LANES), jnp.float32),
            pltpu.VMEM((3, chunks, half, LANES), jnp.float32),
            pltpu.VMEM((2, 3 * (devices // 4), half, LANES), jnp.float32),
            pltpu.VMEM((8, LANES), jnp.float32),
            pltpu.VMEM((devices, 8, LANES), jnp.float32),
            pltpu.VMEM((8, LANES), jnp.float32),
            pltpu.VMEM((2, 8, LANES), jnp.float32),
            pltpu.VMEM((groups, 8, LANES), jnp.float32),
            pltpu.VMEM((devices, 8, LANES), jnp.float32),
            pltpu.VMEM(tables.shape, jnp.bfloat16),
            pltpu.VMEM(twists.shape, jnp.float32),
            pltpu.SemaphoreType.DMA((6,)),
            pltpu.SemaphoreType.DMA((1,)),
            pltpu.SemaphoreType.DMA((9,)),
            pltpu.SemaphoreType.DMA((1,)),
            pltpu.SemaphoreType.DMA((3,)),
            pltpu.SemaphoreType.DMA((2,)),
            pltpu.SemaphoreType.DMA((3,)),
            pltpu.SemaphoreType.DMA((3,)),
        ],
        compiler_params=pltpu.CompilerParams(
            collective_id=0, has_side_effects=True, vmem_limit_bytes=(64 << 20) - (960 << 10)
        ),
    )(
        key_input, value_input, query_input, cotangent, filter_taps,
        skip_gain.reshape(1, channels), jnp.asarray(tables), jnp.asarray(twists),
    )
    results = pl.pallas_call(
        emit,
        out_shape=tuple(jax.ShapeDtypeStruct(*shape) for shape in shapes),
        in_specs=[vmem] * 7,
        out_specs=(hbm,) * 7,
        scratch_shapes=[pltpu.SemaphoreType.DMA((7,))],
        compiler_params=pltpu.CompilerParams(vmem_limit_bytes=4 << 20),
    )(*held)
    return (*results[:5], results[5].reshape(channels), results[6].reshape(()))


def pick_body(query_input, *others):
    devices = lax.axis_size("seq")
    rows, channels = query_input.shape
    fits = devices == 8 and 2 * channels == LANES * devices and rows % 16 == 0
    chosen = fused_body if fits and rows * devices <= 2048 else body
    return chosen(query_input, *others)


def solution(mesh):
    return jax.shard_map(
        pick_body,
        mesh=mesh,
        in_specs=(
            P("seq", "ch"),
            P("seq", "ch"),
            P("seq", "ch"),
            P("seq", "ch"),
            P("seq", "ch"),
            P("ch"),
        ),
        out_specs=(
            P("seq", "ch"),
            P("seq", "ch"),
            P("seq", "ch"),
            P("seq", "ch"),
            P("seq", "ch"),
            P("ch"),
            P(),
        ),
        check_vma=False,
    )
```

```python
import functools
import math

import jax
import jax.numpy as jnp
import numpy as np
from jax import lax
from jax.experimental import pallas as pl
from jax.experimental.pallas import tpu as pltpu
from jax.sharding import PartitionSpec as P

LANES = 128
MESH = pl.DeviceIdType.MESH


def complex_mul(left_op, right_op):
    return jnp.stack(
        [
            left_op[0] * right_op[0] - left_op[1] * right_op[1],
            left_op[0] * right_op[1] + left_op[1] * right_op[0],
        ]
    )


def conj_of(stacked):
    return jnp.stack([stacked[0], -stacked[1]])


def dft_table(length, direction):
    counter = jnp.arange(length)
    angles = (
        2.0 * math.pi / length * (counter[:, None] * counter[None, :] % length).astype(jnp.float32)
    )
    return (jnp.cos(angles), direction * jnp.sin(angles))


def dft_along(stacked, length, direction, pattern):
    table_re, table_im = dft_table(length, direction)

    def contract(table, part_in):
        return jnp.einsum(pattern, table, part_in, precision=lax.Precision.HIGHEST)

    real_out = contract(table_re, stacked[0]) - contract(table_im, stacked[1])
    imag_out = contract(table_re, stacked[1]) + contract(table_im, stacked[0])
    return jnp.stack([real_out, imag_out])


def grid_twiddle(devices, block, direction):
    seq_length = devices * block
    counter = jnp.arange(devices)[:, None] * jnp.arange(block)[None, :] % seq_length
    angles = direction * 2.0 * math.pi / seq_length * counter.astype(jnp.float32)
    return jnp.stack([jnp.cos(angles), jnp.sin(angles)])[:, None, None]


def local_forward(stacked, devices, block):
    array_shape = stacked.shape
    stacked = stacked.reshape(array_shape[0], array_shape[1], array_shape[2], devices, block)
    stacked = dft_along(stacked, devices, -1.0, "kj,scjp->sckp")
    stacked = complex_mul(stacked, grid_twiddle(devices, block, -1.0))
    return dft_along(stacked, block, -1.0, "kp,scjp->scjk")


def local_inverse(stacked, devices, block):
    stacked = dft_along(stacked, block, 1.0, "kp,scjp->scjk")
    stacked = complex_mul(stacked, grid_twiddle(devices, block, 1.0))
    stacked = dft_along(stacked, devices, 1.0, "kj,scjp->sckp")
    array_shape = stacked.shape
    return stacked.reshape(array_shape[0], array_shape[1], array_shape[2], devices * block) / (
        devices * block
    )


def modulated(signals, cosine, sine_part):
    zero_part = jnp.zeros_like(signals)
    return jnp.stack(
        [
            jnp.concatenate([signals, signals * cosine]),
            jnp.concatenate([zero_part, -signals * sine_part]),
        ]
    )


def spectral_products(spectrum):
    mixed_spec = spectrum[:, 0::3]
    gated_spec = spectrum[:, 1::3]
    taps_spec = spectrum[:, 2::3]
    out_spec = complex_mul(mixed_spec, taps_spec)
    back_spec = complex_mul(gated_spec, conj_of(taps_spec))
    grad_spec = complex_mul(gated_spec, conj_of(mixed_spec))
    return jnp.stack(
        [
            out_spec[:, 0],
            back_spec[:, 0],
            grad_spec[:, 0],
            out_spec[:, 1],
            back_spec[:, 1],
            grad_spec[:, 1],
        ],
        axis=1,
    )


def unfold(series, cosine, sine_part):
    return tuple(
        (
            0.5
            * (
                series[0, signal_index]
                + cosine * series[0, signal_index + 3]
                - sine_part * series[1, signal_index + 3]
            )
            for signal_index in range(3)
        )
    )


def channel_local(mixed_in, gated_cot, filter_taps, devices):
    pieces = (
        lax.all_to_all(mixed_in, "seq", split_axis=1, concat_axis=0, tiled=True),
        lax.all_to_all(gated_cot, "seq", split_axis=1, concat_axis=0, tiled=True),
        lax.all_to_all(filter_taps, "seq", split_axis=1, concat_axis=0, tiled=True),
    )
    laid = jnp.transpose(jnp.stack(pieces), (0, 2, 1))
    seq_length = laid.shape[2]
    block = seq_length // devices
    angles = math.pi / seq_length * jnp.arange(seq_length).astype(jnp.float32)
    cosine = jnp.cos(angles)
    sine_row = jnp.sin(angles)
    spectrum = local_forward(modulated(laid, cosine, sine_row), devices, block)
    series = local_inverse(spectral_products(spectrum), devices, block)
    results = unfold(series, cosine, sine_row)
    return (
        lax.all_to_all(results[0].T, "seq", split_axis=0, concat_axis=1, tiled=True),
        lax.all_to_all(results[1].T, "seq", split_axis=0, concat_axis=1, tiled=True),
        lax.all_to_all(results[2].T, "seq", split_axis=0, concat_axis=1, tiled=True),
    )


def body(query_input, key_input, value_input, cotangent, filter_taps, skip_gain):
    devices = lax.axis_size("seq")
    row_count, channels = query_input.shape
    seq_length = row_count * devices
    query_val = query_input.astype(jnp.float32)
    key_val = key_input.astype(jnp.float32)
    value_val = value_input.astype(jnp.float32)
    cot_val = cotangent.astype(jnp.float32)
    mixed_in = key_val * value_val
    gated_cot = query_val * cot_val
    conv_out, back_conv, kernel_grad = channel_local(mixed_in, gated_cot, filter_taps, devices)
    inner_sum = conv_out + skip_gain[None, :] * mixed_in
    mixed_grad = back_conv + skip_gain[None, :] * gated_cot
    output = (query_val * inner_sum).astype(jnp.bfloat16)
    query_grad = (cot_val * inner_sum).astype(jnp.bfloat16)
    key_grad = (mixed_grad * value_val).astype(jnp.bfloat16)
    value_grad = (mixed_grad * key_val).astype(jnp.bfloat16)
    time_scale = 1.0 / math.sqrt(seq_length)
    filter_grad = kernel_grad * time_scale
    filter_sq = jnp.sum(filter_grad * filter_grad)
    skip_part = jnp.sum(gated_cot * mixed_in, axis=0) * time_scale
    skip_grad = lax.psum(skip_part, "seq")
    total_sq = lax.psum(filter_sq + jnp.sum(skip_grad * skip_grad) / devices, ("seq", "ch"))
    grad_rms = jnp.sqrt(total_sq / (channels * lax.axis_size("ch") * (seq_length + 1)))
    return (output, query_grad, key_grad, value_grad, filter_grad, skip_grad, grad_rms)


def split_high_low(array):
    high = array.astype(jnp.bfloat16)
    return high, (array - high.astype(jnp.float32)).astype(jnp.bfloat16)


def half_tables(points):
    odd = 2 * np.arange(points, dtype=np.int64) + 1
    angles = math.pi / (4 * points) * (odd[:, None] * odd[None, :] % (8 * points))
    parts = []
    for table in (np.cos(angles), np.sin(angles)):
        table = table.astype(np.float32)
        high = table.astype(jnp.bfloat16)
        parts += [high, (table - high.astype(np.float32)).astype(jnp.bfloat16)]
    shift = math.pi / (4 * points) * odd[:, None] * np.ones((1, LANES))
    return np.stack(parts), np.stack([np.cos(shift), np.sin(shift)]).astype(np.float32)


def kernel(
    devices, groups, count,
    k_hbm, v_hbm, q_hbm, c_hbm, h_hbm, skip_hbm, table_hbm, twist_hbm,
    out_ref, dq_ref, dk_ref, dv_ref, dh_ref, dskip_ref, rms_ref,
    gates, skip_ref, x_buf, g_buf, wide, flat,
    send, recv, spec, prod, back, home, extra,
    part_send, part_home, sq_acc, sq_send, sq_all, table, twist,
    load_sem, in_send, in_recv, out_send, home_recv, extra_recv, small_send, small_recv, ready,
):
    me = lax.axis_index("seq")
    mine = lax.axis_index("ch")
    rows, channels = q_hbm.shape
    half = rows // 2
    points = half * devices
    low = LANES // 2
    time_scale = 1.0 / math.sqrt(2 * points)
    blocks = channels // LANES
    side = devices // 2
    pair = devices // 4
    split = 3 * pair
    base = me // side * side
    other = side - base
    early = me < side
    late = me >= side
    near_here = me < pair
    whole_here = (me >= pair) & (me < side)
    far_two = (me >= side) & (me < split)
    far_one = me >= split

    barrier = pltpu.get_barrier_semaphore()
    for k in range(1, groups):
        pl.semaphore_signal(
            barrier, inc=1, device_id={"ch": lax.rem(mine + k, groups)}, device_id_type=MESH
        )

    @pl.when(me < split)
    def _():
        for k in range(1, devices):
            pl.semaphore_signal(
                barrier, inc=1, device_id={"seq": lax.rem(me + k, devices)}, device_id_type=MESH
            )

    @pl.when(far_one)
    def _():
        for k in range(1, pair):
            peer = split + lax.rem(me - split + k, pair)
            pl.semaphore_signal(barrier, inc=1, device_id={"seq": peer}, device_id_type=MESH)

    def columns_of(j):
        return pl.ds(j * LANES, LANES)

    for index, source in enumerate((k_hbm, v_hbm, q_hbm, c_hbm)):
        pltpu.make_async_copy(source, gates.at[index], load_sem.at[index // 2]).start()
    for j in range(blocks):
        pltpu.make_async_copy(h_hbm.at[:, columns_of(j)], wide.at[j], load_sem.at[2]).start()
    loads = (
        pltpu.make_async_copy(skip_hbm, skip_ref, load_sem.at[3]),
        pltpu.make_async_copy(table_hbm, table, load_sem.at[4]),
        pltpu.make_async_copy(twist_hbm, twist, load_sem.at[5]),
    )
    for load in loads:
        load.start()

    @pl.when(far_one)
    def _():
        pl.semaphore_wait(barrier, devices + groups - 2)
        for device in range(split):
            pl.semaphore_signal(
                ready, inc=1, device_id={"seq": jnp.int32(device)}, device_id_type=MESH
            )

    def gate(index, j):
        return gates[index, :, columns_of(j)].astype(jnp.float32)

    def wait_bytes(ref, sem):
        pltpu.make_async_copy(ref, ref, sem).wait()

    def near_owner(c):
        return (c % pair, c // pair)

    def far_owner(c):
        return (side + c, 0) if c < side else (c, 1)

    def whole_owner(c):
        return (c - side, 0)

    def give(signal, c, owner, can_be_me):
        device, slot = owner
        target = recv.at[(slot * 3 + signal) * devices + me]
        sem = in_recv.at[slot * 3 + signal]

        def remote():
            pltpu.make_async_remote_copy(
                src_ref=send.at[signal, c],
                dst_ref=target,
                send_sem=in_send.at[0],
                recv_sem=sem,
                device_id={"seq": jnp.int32(device)},
                device_id_type=MESH,
            ).start()

        if not can_be_me:
            remote()
            return

        pl.when(me != device)(remote)

        @pl.when(me == device)
        def _():
            pltpu.make_async_copy(send.at[signal, c], target, sem).start()

    def give_far(signal, chunks, can_be_me=False):
        for c in chunks:
            give(signal, c, far_owner(c), can_be_me)

    def give_whole(signal, can_be_me=False):
        for c in range(split, devices):
            give(signal, c, whole_owner(c), can_be_me)

    def give_near(signal, slot, can_be_me=False):
        for c in range(slot * pair, (slot + 1) * pair):
            give(signal, c, near_owner(c), can_be_me)

    def await_input(slot, signal, start, sources):
        first_one = (slot * 3 + signal) * devices + start
        wait_bytes(recv.at[pl.ds(first_one, sources)], in_recv.at[slot * 3 + signal])

    def to_home(slot, kind, c, dest):
        pltpu.make_async_remote_copy(
            src_ref=back.at[slot, kind, dest],
            dst_ref=home.at[kind, c],
            send_sem=out_send.at[0],
            recv_sem=home_recv.at[kind],
            device_id={"seq": dest},
            device_id_type=MESH,
        ).start()

    def to_extra(slot, kind, c, dest):
        pltpu.make_async_remote_copy(
            src_ref=back.at[slot, kind, dest],
            dst_ref=extra.at[kind, c],
            send_sem=out_send.at[0],
            recv_sem=extra_recv.at[kind],
            device_id={"seq": dest},
            device_id_type=MESH,
        ).start()

    def inward(slot, kind, c):
        for k in range(1, side):
            to_home(slot, kind, c, base + lax.rem(me - base + k, side))
        pltpu.make_async_copy(back.at[slot, kind, me], home.at[kind, c], home_recv.at[kind]).start()

    def small_copy(source, target, index, device_id):
        return pltpu.make_async_remote_copy(
            src_ref=source,
            dst_ref=target,
            send_sem=small_send.at[index],
            recv_sem=small_recv.at[index],
            device_id=device_id,
            device_id_type=MESH,
        )

    def to_peers(source, target, index):
        for k in range(1, devices):
            peer = lax.rem(me + k, devices)
            small_copy(source, target.at[me], index, {"seq": peer}).start()

    def share_squares(squares):
        row = jnp.sum(squares, axis=0, keepdims=True)
        sq_send[0] = row
        sq_all[me * groups + mine] = row
        for k in range(devices):
            for n in range(groups):
                if k or n:
                    peer = {"seq": lax.rem(me + k, devices), "ch": lax.rem(mine + n, groups)}
                    small_copy(sq_send.at[0], sq_all.at[me * groups + mine], 1, peer).start()

    first = lax.broadcasted_iota(jnp.int32, (half, LANES), 1) < low

    def pack(source, signal):
        for j in range(blocks):
            even = source[j, pl.ds(0, half, stride=2), :]
            odd = source[j, pl.ds(1, half, stride=2), :]
            send[signal, 2 * j] = jnp.where(first, even, pltpu.roll(odd, low, 1))
            send[signal, 2 * j + 1] = jnp.where(first, pltpu.roll(even, low, 1), odd)

    wait_bytes(gates.at[pl.ds(0, 2)], load_sem.at[0])
    for j in range(blocks):
        x_buf[j] = gate(0, j) * gate(1, j)
    pack(x_buf, 0)
    @pl.when(me < split)
    def _():
        pl.semaphore_wait(barrier, split + groups - 2)

    to_two = (*range(pair), *range(side, split))
    to_one = range(pair, side)

    @pl.when(early)
    def _():
        give_far(0, to_two)

    @pl.when(near_here)
    def _():
        give_whole(0)

    @pl.when(whole_here)
    def _():
        give_near(0, 0)
        give_whole(0, True)

    @pl.when(far_two)
    def _():
        give_whole(0)
        give_far(0, range(pair), True)

    @pl.when(far_one)
    def _():
        give_far(0, range(pair))

    wait_bytes(gates.at[pl.ds(2, 2)], load_sem.at[1])
    for j in range(blocks):
        g_buf[j] = gate(2, j) * gate(3, j)
    pack(g_buf, 1)

    @pl.when(near_here)
    def _():
        give_whole(1)

    @pl.when(whole_here)
    def _():
        give_near(1, 0)
        give_whole(1, True)

    @pl.when(far_two)
    def _():
        give_whole(1)
        give_far(1, range(pair), True)
        for signal in (0, 1):
            give_far(signal, range(side, split), True)

    @pl.when(far_one)
    def _():
        give_far(1, range(pair))
        give_whole(0)
        give_whole(1)
        for signal in (0, 1):
            give_far(signal, to_one, True)
        for signal in (0, 1):
            give_far(signal, range(side, split))

    wait_bytes(wide, load_sem.at[2])
    pack(wide, 2)

    @pl.when(whole_here)
    def _():
        give_whole(2, True)

    @pl.when(far_two)
    def _():
        give_whole(2)

    @pl.when(me < split)
    def _():
        pl.semaphore_wait(ready, pair)

    @pl.when(early)
    def _():
        give_far(0, to_one)

    @pl.when(near_here)
    def _():
        give_far(2, (*to_two, *to_one))
        give_whole(2)
        for signal in range(3):
            for slot in range(3):
                give_near(signal, slot, True)

    @pl.when(whole_here)
    def _():
        for slot in (1, 2):
            for signal in (0, 1):
                give_near(signal, slot)
        for slot in range(3):
            give_near(2, slot)

    @pl.when(far_two)
    def _():
        for signal in (0, 1):
            give_far(signal, to_one)
        give_far(2, to_two, True)
        give_far(2, to_one)

    @pl.when(far_one)
    def _():
        give_whole(2)
        give_far(2, to_two)
        give_far(2, to_one, True)

    @pl.when(late)
    def _():
        extra[...] = jnp.zeros(extra.shape, jnp.float32)

    for j in range(blocks):
        part_send[pl.ds(j, 1), :] = jnp.sum(x_buf[j] * g_buf[j], axis=0, keepdims=True) * time_scale
    part_home[me] = part_send[...]
    to_peers(part_send, part_home, 0)
    sq_acc[...] = jnp.zeros((8, LANES), jnp.float32)
    for load in loads:
        load.wait()

    def times(which, pieces, at_row, at_column):
        high, rest = pieces
        both = jnp.concatenate([high, rest], axis=1)
        main = jnp.dot(
            table[2 * which, at_row, at_column], both, preferred_element_type=jnp.float32
        )
        small = jnp.dot(
            table[2 * which + 1, at_row, at_column], high, preferred_element_type=jnp.float32
        )
        return main[:, :LANES] + (main[:, LANES:] + small)

    full = slice(0, points)
    early_part = slice(0, points // 2)
    late_part = slice(points // 2, points)

    def forward(slot, signal, part):
        start = (slot * 3 + signal) * devices + part.start // half
        sources = (part.stop - part.start) // half
        data = recv[pl.ds(start, sources)].reshape(sources * half, LANES)
        pieces = split_high_low(data)
        spec[slot, signal, 0] = times(0, pieces, full, part)
        spec[slot, signal, 1] = -times(1, pieces, full, part)

    def inverse(slot, kind, part, scale):
        series = times(0, split_high_low(prod[0]), part, full)
        series = series - times(1, split_high_low(prod[1]), part, full)
        series = series * (scale / points)
        start = part.start // half
        sources = (part.stop - part.start) // half
        back[slot, kind, start : start + sources] = series.reshape(sources, half, LANES)
        return series

    def square_sum(series):
        sq_acc[...] += jnp.sum((series * series).reshape(side * half // 8, 8, LANES), axis=0)

    step = 128

    def halves(slot, ref_row, part, at):
        value = spec[slot, ref_row, part, at, :]
        turned = pltpu.roll(value, low, 1)
        left = lax.broadcasted_iota(jnp.int32, (step, LANES), 1) < low
        return value, turned, jnp.where(left, value, turned), jnp.where(left, turned, value)

    def products(slot, signal, other_signal, conjugate):
        sign = jnp.where(lax.broadcasted_iota(jnp.int32, (step, LANES), 1) < low, 1.0, -1.0)

        @pl.loop(0, points // step)
        def _(index):
            at = pl.ds(pl.multiple_of(index * step, step), step)
            cosine = twist[0, at, :]
            sine = twist[1, at, :]
            signed = sine * sign
            _, _, even_re, odd_re = halves(slot, other_signal, 0, at)
            _, _, even_im, odd_im = halves(slot, other_signal, 1, at)
            a_re, as_re, _, _ = halves(slot, signal, 0, at)
            a_im, as_im, _, _ = halves(slot, signal, 1, at)
            p_re = even_re * cosine - even_im * sine
            p_im = even_im * cosine + even_re * sine
            if conjugate:
                r_re = odd_re * cosine - odd_im * signed
                r_im = odd_im * cosine + odd_re * signed
                prod[0, at, :] = a_re * p_re + a_im * p_im + (as_re * r_re + as_im * r_im)
                prod[1, at, :] = a_im * p_re - a_re * p_im + (as_im * r_re - as_re * r_im)
            else:
                r_re = odd_re * cosine + odd_im * signed
                r_im = odd_im * cosine - odd_re * signed
                prod[0, at, :] = a_re * p_re - a_im * p_im + (as_re * r_re - as_im * r_im)
                prod[1, at, :] = a_im * p_re + a_re * p_im + (as_im * r_re + as_re * r_im)

    @pl.when(near_here)
    def _():
        @pl.loop(0, 3)
        def _(slot):
            c = slot * pair + me
            for signal in (0, 1):
                await_input(slot, signal, 0, side)
                forward(slot, signal, early_part)
            products(slot, 1, 0, True)
            inverse(slot, 0, early_part, time_scale)
            inward(slot, 0, c)

        @pl.loop(0, 3)
        def _(slot):
            c = slot * pair + me
            await_input(slot, 2, 0, side)
            forward(slot, 2, early_part)
            products(slot, 1, 2, True)
            inverse(slot, 1, early_part, 1.0)
            inward(slot, 1, c)
            products(slot, 0, 2, False)
            inverse(slot, 2, early_part, 1.0)
            inward(slot, 2, c)

    def outward(slot, kind, c):
        @pl.when(whole_here)
        def _():
            for k in range(side):
                to_home(slot, kind, c, other + k)

        if kind < 2:
            @pl.when(late)
            def _():
                for k in range(side):
                    to_extra(slot, kind, c, other + k)

        inward(slot, kind, c)

    @pl.when(me >= pair)
    def _():
        zone = me // pair
        slots = 2 - lax.rem(zone, 2)

        @pl.when(late)
        def _():
            await_input(0, 1, side, side)

        @pl.loop(0, slots)
        def _(slot):
            c = lax.rem(me + side + side * slot, devices)

            @pl.when(late & (slot > 0))
            def _():
                await_input(slot, 1, side, side)

            @pl.when(late)
            def _():
                forward(slot, 1, late_part)

            await_input(slot, 0, 0, devices)

            forward(slot, 0, full)

            @pl.when(whole_here)
            def _():
                await_input(slot, 1, 0, devices)
                forward(slot, 1, full)
                give_far(2, (*to_two, *to_one))

            products(slot, 1, 0, True)
            series = inverse(slot, 0, full, time_scale)
            outward(slot, 0, c)
            square_sum(series[points // 2 :])

        @pl.when(late)
        def _():
            share_squares(sq_acc[...])

        @pl.loop(0, slots)
        def _(slot):
            c = lax.rem(me + side + side * slot, devices)
            await_input(slot, 2, 0, devices)
            forward(slot, 2, full)
            products(slot, 1, 2, True)
            inverse(slot, 1, full, 1.0)
            outward(slot, 1, c)
            products(slot, 0, 2, False)
            inverse(slot, 2, full, 1.0)
            outward(slot, 2, c)

    def await_home(kind):
        wait_bytes(home.at[kind], home_recv.at[kind])
        if kind < 2:
            @pl.when(early)
            def _():
                wait_bytes(extra.at[kind], extra_recv.at[kind])

    def unpack(kind, j):
        pieces = []
        for c in (2 * j, 2 * j + 1):
            value = home[kind, c]
            pieces.append(value + extra[kind, c] if kind < 2 and c < split else value)
        left, right = pieces
        flat[j, pl.ds(0, half, stride=2), :] = jnp.where(first, left, pltpu.roll(right, low, 1))
        flat[j, pl.ds(1, half, stride=2), :] = jnp.where(first, pltpu.roll(left, low, 1), right)
        return flat[j]

    wait_bytes(part_home.at[pl.ds(0, devices - 1)], small_recv.at[0])
    direct = part_home[0]
    for k in range(1, devices):
        direct = direct + part_home[k]
    for j in range(blocks):
        dskip_ref[:, columns_of(j)] = direct[j : j + 1]

    await_home(0)
    squares = sq_acc[...]
    for j in range(blocks):
        squares = squares + direct[j : j + 1] * direct[j : j + 1] * (1.0 / (8 * side))
    for j in range(blocks):
        value = unpack(0, j)
        dh_ref[:, columns_of(j)] = value
        squares = squares + jnp.sum((value * value).reshape(rows // 8, 8, LANES), axis=0)

    @pl.when(early)
    def _():
        share_squares(squares)

    def assemble_inner():
        await_home(2)
        for j in range(blocks):
            at = columns_of(j)
            inner = unpack(2, j) + skip_ref[:, at] * x_buf[j]
            out_ref[:, at] = (gate(2, j) * inner).astype(jnp.bfloat16)
            dq_ref[:, at] = (gate(3, j) * inner).astype(jnp.bfloat16)

    def assemble_grad():
        await_home(1)
        for j in range(blocks):
            at = columns_of(j)
            grad = unpack(1, j) + skip_ref[:, at] * g_buf[j]
            dk_ref[:, at] = (grad * gate(1, j)).astype(jnp.bfloat16)
            dv_ref[:, at] = (grad * gate(0, j)).astype(jnp.bfloat16)

    assemble_inner()
    assemble_grad()

    everyone = devices * groups
    wait_bytes(sq_all.at[pl.ds(0, everyone - 1)], small_recv.at[1])
    total = sq_all[0]
    for k in range(1, everyone):
        total = total + sq_all[k]
    total = jnp.sum(total, axis=1, keepdims=True)
    rms_ref[...] = jnp.sqrt(total / count)

    for condition, sent, returned in (
        (near_here, 3 * (split - 3) + 2 * split + 3 * pair, 9 * (side - 1)),
        (whole_here, 5 * split + 3 * (pair - 1), 3 * (devices - 1)),
        (far_two, 3 * (split - 2) + 3 * pair, 2 * (2 * side + 3 * (side - 1))),
        (far_one, 3 * (split - 1) + 3 * pair, 2 * side + 3 * (side - 1)),
    ):
        @pl.when(condition)
        def _():
            wait_bytes(recv.at[pl.ds(0, sent)], in_send.at[0])
            wait_bytes(recv.at[pl.ds(0, returned)], out_send.at[0])

    wait_bytes(part_home.at[pl.ds(0, devices - 1)], small_send.at[0])
    wait_bytes(sq_all.at[pl.ds(0, everyone - 1)], small_send.at[1])


def emit(*refs):
    sources, targets, sem = refs[:7], refs[7:14], refs[14]
    copies = [
        pltpu.make_async_copy(source, target, sem.at[index])
        for index, (source, target) in enumerate(zip(sources, targets))
    ]
    for copy in copies:
        copy.start()
    for copy in copies:
        copy.wait()


def fused_body(query_input, key_input, value_input, cotangent, filter_taps, skip_gain):
    devices = lax.axis_size("seq")
    groups = lax.axis_size("ch")
    rows, channels = query_input.shape
    half = rows // 2
    points = half * devices
    tables, twists = half_tables(points)
    count = float(channels * groups * (rows * devices + 1))
    vmem = pl.BlockSpec(memory_space=pltpu.VMEM)
    hbm = pl.BlockSpec(memory_space=pltpu.HBM)
    chunks = 2 * channels // LANES
    blocks = channels // LANES
    shapes = [((rows, channels), jnp.bfloat16)] * 4 + [
        ((rows, channels), jnp.float32),
        ((1, channels), jnp.float32),
        ((1, 1), jnp.float32),
    ]
    held = pl.pallas_call(
        functools.partial(kernel, devices, groups, count),
        out_shape=tuple(pltpu.VMEM(*shape) for shape in shapes),
        in_specs=[hbm] * 8,
        out_specs=(vmem,) * 7,
        scratch_shapes=[
            pltpu.VMEM((4, rows, channels), jnp.bfloat16),
            pltpu.VMEM((1, channels), jnp.float32),
            pltpu.VMEM((blocks, rows, LANES), jnp.float32),
            pltpu.VMEM((blocks, rows, LANES), jnp.float32),
            pltpu.VMEM((blocks, rows, LANES), jnp.float32),
            pltpu.VMEM((blocks, rows, LANES), jnp.float32),
            pltpu.VMEM((3, chunks, half, LANES), jnp.float32),
            pltpu.VMEM((9 * devices, half, LANES), jnp.float32),
            pltpu.VMEM((3, 3, 2, points, LANES), jnp.float32),
            pltpu.VMEM((2, points, LANES), jnp.float32),
            pltpu.VMEM((3, 3, devices, half, LANES), jnp.float32),
            pltpu.VMEM((3, chunks, half, LANES), jnp.float32),
            pltpu.VMEM((2, 3 * (devices // 4), half, LANES), jnp.float32),
            pltpu.VMEM((blocks, LANES), jnp.float32),
            pltpu.VMEM((devices, blocks, LANES), jnp.float32),
            pltpu.VMEM((8, LANES), jnp.float32),
            pltpu.VMEM((1, 1, LANES), jnp.float32),
            pltpu.VMEM((devices * groups, 1, LANES), jnp.float32),
            pltpu.VMEM(tables.shape, jnp.bfloat16),
            pltpu.VMEM(twists.shape, jnp.float32),
            pltpu.SemaphoreType.DMA((6,)),
            pltpu.SemaphoreType.DMA((1,)),
            pltpu.SemaphoreType.DMA((9,)),
            pltpu.SemaphoreType.DMA((1,)),
            pltpu.SemaphoreType.DMA((3,)),
            pltpu.SemaphoreType.DMA((2,)),
            pltpu.SemaphoreType.DMA((2,)),
            pltpu.SemaphoreType.DMA((2,)),
            pltpu.SemaphoreType.REGULAR,
        ],
        compiler_params=pltpu.CompilerParams(
            collective_id=0, has_side_effects=True, vmem_limit_bytes=(64 << 20) - (960 << 10)
        ),
    )(
        key_input, value_input, query_input, cotangent, filter_taps,
        skip_gain.reshape(1, channels), jnp.asarray(tables), jnp.asarray(twists),
    )
    results = pl.pallas_call(
        emit,
        out_shape=tuple(jax.ShapeDtypeStruct(*shape) for shape in shapes),
        in_specs=[vmem] * 7,
        out_specs=(hbm,) * 7,
        scratch_shapes=[pltpu.SemaphoreType.DMA((7,))],
        compiler_params=pltpu.CompilerParams(vmem_limit_bytes=4 << 20),
    )(*held)
    return (*results[:5], results[5].reshape(channels), results[6].reshape(()))


def pick_body(query_input, *others):
    devices = lax.axis_size("seq")
    rows, channels = query_input.shape
    fits = devices == 8 and 2 * channels == LANES * devices and rows % 16 == 0
    chosen = fused_body if fits and rows * devices <= 2048 else body
    return chosen(query_input, *others)


def solution(mesh):
    return jax.shard_map(
        pick_body,
        mesh=mesh,
        in_specs=(
            P("seq", "ch"),
            P("seq", "ch"),
            P("seq", "ch"),
            P("seq", "ch"),
            P("seq", "ch"),
            P("ch"),
        ),
        out_specs=(
            P("seq", "ch"),
            P("seq", "ch"),
            P("seq", "ch"),
            P("seq", "ch"),
            P("seq", "ch"),
            P("ch"),
            P(),
        ),
        check_vma=False,
    )
```

```python
import functools
import math

import jax
import jax.numpy as jnp
import numpy as np
from jax import lax
from jax.experimental import pallas as pl
from jax.experimental.pallas import tpu as pltpu
from jax.sharding import PartitionSpec as P

LANES = 128
MESH = pl.DeviceIdType.MESH


def complex_mul(left_op, right_op):
    return jnp.stack(
        [
            left_op[0] * right_op[0] - left_op[1] * right_op[1],
            left_op[0] * right_op[1] + left_op[1] * right_op[0],
        ]
    )


def conj_of(stacked):
    return jnp.stack([stacked[0], -stacked[1]])


def dft_table(length, direction):
    counter = jnp.arange(length)
    angles = (
        2.0 * math.pi / length * (counter[:, None] * counter[None, :] % length).astype(jnp.float32)
    )
    return (jnp.cos(angles), direction * jnp.sin(angles))


def dft_along(stacked, length, direction, pattern):
    table_re, table_im = dft_table(length, direction)

    def contract(table, part_in):
        return jnp.einsum(pattern, table, part_in, precision=lax.Precision.HIGHEST)

    real_out = contract(table_re, stacked[0]) - contract(table_im, stacked[1])
    imag_out = contract(table_re, stacked[1]) + contract(table_im, stacked[0])
    return jnp.stack([real_out, imag_out])


def grid_twiddle(devices, block, direction):
    seq_length = devices * block
    counter = jnp.arange(devices)[:, None] * jnp.arange(block)[None, :] % seq_length
    angles = direction * 2.0 * math.pi / seq_length * counter.astype(jnp.float32)
    return jnp.stack([jnp.cos(angles), jnp.sin(angles)])[:, None, None]


def local_forward(stacked, devices, block):
    array_shape = stacked.shape
    stacked = stacked.reshape(array_shape[0], array_shape[1], array_shape[2], devices, block)
    stacked = dft_along(stacked, devices, -1.0, "kj,scjp->sckp")
    stacked = complex_mul(stacked, grid_twiddle(devices, block, -1.0))
    return dft_along(stacked, block, -1.0, "kp,scjp->scjk")


def local_inverse(stacked, devices, block):
    stacked = dft_along(stacked, block, 1.0, "kp,scjp->scjk")
    stacked = complex_mul(stacked, grid_twiddle(devices, block, 1.0))
    stacked = dft_along(stacked, devices, 1.0, "kj,scjp->sckp")
    array_shape = stacked.shape
    return stacked.reshape(array_shape[0], array_shape[1], array_shape[2], devices * block) / (
        devices * block
    )


def modulated(signals, cosine, sine_part):
    zero_part = jnp.zeros_like(signals)
    return jnp.stack(
        [
            jnp.concatenate([signals, signals * cosine]),
            jnp.concatenate([zero_part, -signals * sine_part]),
        ]
    )


def spectral_products(spectrum):
    mixed_spec = spectrum[:, 0::3]
    gated_spec = spectrum[:, 1::3]
    taps_spec = spectrum[:, 2::3]
    out_spec = complex_mul(mixed_spec, taps_spec)
    back_spec = complex_mul(gated_spec, conj_of(taps_spec))
    grad_spec = complex_mul(gated_spec, conj_of(mixed_spec))
    return jnp.stack(
        [
            out_spec[:, 0],
            back_spec[:, 0],
            grad_spec[:, 0],
            out_spec[:, 1],
            back_spec[:, 1],
            grad_spec[:, 1],
        ],
        axis=1,
    )


def unfold(series, cosine, sine_part):
    return tuple(
        (
            0.5
            * (
                series[0, signal_index]
                + cosine * series[0, signal_index + 3]
                - sine_part * series[1, signal_index + 3]
            )
            for signal_index in range(3)
        )
    )


def channel_local(mixed_in, gated_cot, filter_taps, devices):
    pieces = (
        lax.all_to_all(mixed_in, "seq", split_axis=1, concat_axis=0, tiled=True),
        lax.all_to_all(gated_cot, "seq", split_axis=1, concat_axis=0, tiled=True),
        lax.all_to_all(filter_taps, "seq", split_axis=1, concat_axis=0, tiled=True),
    )
    laid = jnp.transpose(jnp.stack(pieces), (0, 2, 1))
    seq_length = laid.shape[2]
    block = seq_length // devices
    angles = math.pi / seq_length * jnp.arange(seq_length).astype(jnp.float32)
    cosine = jnp.cos(angles)
    sine_row = jnp.sin(angles)
    spectrum = local_forward(modulated(laid, cosine, sine_row), devices, block)
    series = local_inverse(spectral_products(spectrum), devices, block)
    results = unfold(series, cosine, sine_row)
    return (
        lax.all_to_all(results[0].T, "seq", split_axis=0, concat_axis=1, tiled=True),
        lax.all_to_all(results[1].T, "seq", split_axis=0, concat_axis=1, tiled=True),
        lax.all_to_all(results[2].T, "seq", split_axis=0, concat_axis=1, tiled=True),
    )


def body(query_input, key_input, value_input, cotangent, filter_taps, skip_gain):
    devices = lax.axis_size("seq")
    row_count, channels = query_input.shape
    seq_length = row_count * devices
    query_val = query_input.astype(jnp.float32)
    key_val = key_input.astype(jnp.float32)
    value_val = value_input.astype(jnp.float32)
    cot_val = cotangent.astype(jnp.float32)
    mixed_in = key_val * value_val
    gated_cot = query_val * cot_val
    conv_out, back_conv, kernel_grad = channel_local(mixed_in, gated_cot, filter_taps, devices)
    inner_sum = conv_out + skip_gain[None, :] * mixed_in
    mixed_grad = back_conv + skip_gain[None, :] * gated_cot
    output = (query_val * inner_sum).astype(jnp.bfloat16)
    query_grad = (cot_val * inner_sum).astype(jnp.bfloat16)
    key_grad = (mixed_grad * value_val).astype(jnp.bfloat16)
    value_grad = (mixed_grad * key_val).astype(jnp.bfloat16)
    time_scale = 1.0 / math.sqrt(seq_length)
    filter_grad = kernel_grad * time_scale
    filter_sq = jnp.sum(filter_grad * filter_grad)
    skip_part = jnp.sum(gated_cot * mixed_in, axis=0) * time_scale
    skip_grad = lax.psum(skip_part, "seq")
    total_sq = lax.psum(filter_sq + jnp.sum(skip_grad * skip_grad) / devices, ("seq", "ch"))
    grad_rms = jnp.sqrt(total_sq / (channels * lax.axis_size("ch") * (seq_length + 1)))
    return (output, query_grad, key_grad, value_grad, filter_grad, skip_grad, grad_rms)


def split_high_low(array):
    high = array.astype(jnp.bfloat16)
    return high, (array - high.astype(jnp.float32)).astype(jnp.bfloat16)


def half_tables(points):
    odd = 2 * np.arange(points, dtype=np.int64) + 1
    angles = math.pi / (4 * points) * (odd[:, None] * odd[None, :] % (8 * points))
    parts = []
    for table in (np.cos(angles), np.sin(angles)):
        table = table.astype(np.float32)
        high = table.astype(jnp.bfloat16)
        parts += [high, (table - high.astype(np.float32)).astype(jnp.bfloat16)]
    shift = math.pi / (4 * points) * odd[:, None] * np.ones((1, LANES))
    return np.stack(parts), np.stack([np.cos(shift), np.sin(shift)]).astype(np.float32)


def kernel(
    devices, groups, count,
    k_hbm, v_hbm, q_hbm, c_hbm, h_hbm, skip_hbm, table_hbm, twist_hbm,
    out_ref, dq_ref, dk_ref, dv_ref, dh_ref, dskip_ref, rms_ref,
    gates, skip_ref, x_buf, g_buf, wide, flat,
    send, recv, spec, prod, back, home, extra,
    part_send, part_home, half_send, half_home, sq_acc, sq_send, sq_all, table, twist,
    load_sem, in_send, in_recv, out_send, home_recv, extra_recv, small_send, small_recv, ready,
):
    me = lax.axis_index("seq")
    mine = lax.axis_index("ch")
    rows, channels = q_hbm.shape
    half = rows // 2
    points = half * devices
    low = LANES // 2
    time_scale = 1.0 / math.sqrt(2 * points)
    blocks = channels // LANES
    side = devices // 2
    pair = devices // 4
    split = 3 * pair
    base = me // side * side
    other = side - base
    early = me < side
    late = me >= side
    near_here = me < pair
    whole_here = (me >= pair) & (me < side)
    far_two = (me >= side) & (me < split)
    far_one = me >= split

    barrier = pltpu.get_barrier_semaphore()
    for k in range(1, groups):
        pl.semaphore_signal(
            barrier, inc=1, device_id={"ch": lax.rem(mine + k, groups)}, device_id_type=MESH
        )

    @pl.when(me < split)
    def _():
        for k in range(1, devices):
            pl.semaphore_signal(
                barrier, inc=1, device_id={"seq": lax.rem(me + k, devices)}, device_id_type=MESH
            )

    @pl.when(far_one)
    def _():
        for k in range(1, pair):
            peer = split + lax.rem(me - split + k, pair)
            pl.semaphore_signal(barrier, inc=1, device_id={"seq": peer}, device_id_type=MESH)

    def columns_of(j):
        return pl.ds(j * LANES, LANES)

    for index, source in enumerate((k_hbm, v_hbm, q_hbm, c_hbm)):
        pltpu.make_async_copy(source, gates.at[index], load_sem.at[index // 2]).start()
    for j in range(blocks):
        pltpu.make_async_copy(h_hbm.at[:, columns_of(j)], wide.at[j], load_sem.at[2]).start()
    loads = (
        pltpu.make_async_copy(skip_hbm, skip_ref, load_sem.at[3]),
        pltpu.make_async_copy(table_hbm, table, load_sem.at[4]),
        pltpu.make_async_copy(twist_hbm, twist, load_sem.at[5]),
    )
    for load in loads:
        load.start()

    @pl.when(far_one)
    def _():
        pl.semaphore_wait(barrier, devices + groups - 2)
        for device in range(split):
            pl.semaphore_signal(
                ready, inc=1, device_id={"seq": jnp.int32(device)}, device_id_type=MESH
            )

    def gate(index, j):
        return gates[index, :, columns_of(j)].astype(jnp.float32)

    def wait_bytes(ref, sem):
        pltpu.make_async_copy(ref, ref, sem).wait()

    def near_owner(c):
        return (c % pair, c // pair)

    def far_owner(c):
        return (side + c, 0) if c < side else (c, 1)

    def whole_owner(c):
        return (c - side, 0)

    def give(signal, c, owner, can_be_me):
        device, slot = owner
        target = recv.at[(slot * 3 + signal) * devices + me]
        sem = in_recv.at[slot * 3 + signal]

        def remote():
            pltpu.make_async_remote_copy(
                src_ref=send.at[signal, c],
                dst_ref=target,
                send_sem=in_send.at[0],
                recv_sem=sem,
                device_id={"seq": jnp.int32(device)},
                device_id_type=MESH,
            ).start()

        if not can_be_me:
            remote()
            return

        pl.when(me != device)(remote)

        @pl.when(me == device)
        def _():
            pltpu.make_async_copy(send.at[signal, c], target, sem).start()

    def give_far(signal, chunks, can_be_me=False):
        for c in chunks:
            give(signal, c, far_owner(c), can_be_me)

    def give_whole(signal, can_be_me=False):
        for c in range(split, devices):
            give(signal, c, whole_owner(c), can_be_me)

    def give_near(signal, slot, can_be_me=False):
        for c in range(slot * pair, (slot + 1) * pair):
            give(signal, c, near_owner(c), can_be_me)

    def await_input(slot, signal, start, sources):
        first_one = (slot * 3 + signal) * devices + start
        wait_bytes(recv.at[pl.ds(first_one, sources)], in_recv.at[slot * 3 + signal])

    def to_home(slot, kind, c, dest):
        pltpu.make_async_remote_copy(
            src_ref=back.at[slot, kind, dest],
            dst_ref=home.at[kind, c],
            send_sem=out_send.at[0],
            recv_sem=home_recv.at[kind],
            device_id={"seq": dest},
            device_id_type=MESH,
        ).start()

    def to_extra(slot, kind, c, dest):
        pltpu.make_async_remote_copy(
            src_ref=back.at[slot, kind, dest],
            dst_ref=extra.at[kind, c],
            send_sem=out_send.at[0],
            recv_sem=extra_recv.at[kind],
            device_id={"seq": dest},
            device_id_type=MESH,
        ).start()

    def inward(slot, kind, c):
        for k in range(1, side):
            to_home(slot, kind, c, base + lax.rem(me - base + k, side))
        pltpu.make_async_copy(back.at[slot, kind, me], home.at[kind, c], home_recv.at[kind]).start()

    def small_copy(source, target, index, device_id):
        return pltpu.make_async_remote_copy(
            src_ref=source,
            dst_ref=target,
            send_sem=small_send.at[index],
            recv_sem=small_recv.at[index],
            device_id=device_id,
            device_id_type=MESH,
        )

    def share_part():
        wait_bytes(part_home.at[pl.ds(0, side - 1)], small_recv.at[0])
        part = part_home[base]
        for k in range(1, side):
            part = part + part_home[base + k]
        half_send[...] = part
        peer = lax.rem(me + side, devices)
        small_copy(half_send, half_home, 2, {"seq": peer}).start()

    def share_squares(squares):
        row = jnp.sum(squares, axis=0, keepdims=True)
        sq_send[0] = row
        sq_all[me * groups + mine] = row
        for k in range(devices):
            for n in range(groups):
                if k or n:
                    peer = {"seq": lax.rem(me + k, devices), "ch": lax.rem(mine + n, groups)}
                    small_copy(sq_send.at[0], sq_all.at[me * groups + mine], 1, peer).start()

    first = lax.broadcasted_iota(jnp.int32, (half, LANES), 1) < low

    def pack(source, signal):
        for j in range(blocks):
            even = source[j, pl.ds(0, half, stride=2), :]
            odd = source[j, pl.ds(1, half, stride=2), :]
            send[signal, 2 * j] = jnp.where(first, even, pltpu.roll(odd, low, 1))
            send[signal, 2 * j + 1] = jnp.where(first, pltpu.roll(even, low, 1), odd)

    wait_bytes(gates.at[pl.ds(0, 2)], load_sem.at[0])
    for j in range(blocks):
        x_buf[j] = gate(0, j) * gate(1, j)
    pack(x_buf, 0)
    @pl.when(me < split)
    def _():
        pl.semaphore_wait(barrier, split + groups - 2)

    to_two = (*range(pair), *range(side, split))
    to_one = range(pair, side)

    @pl.when(early)
    def _():
        give_far(0, to_two)

    @pl.when(near_here)
    def _():
        give_whole(0)
        for slot in range(3):
            give_near(0, slot, True)

    @pl.when(whole_here)
    def _():
        give_near(0, 0)
        give_whole(0, True)

    @pl.when(far_two)
    def _():
        give_whole(0)
        give_far(0, range(pair), True)

    @pl.when(far_one)
    def _():
        give_far(0, range(pair))

    wait_bytes(gates.at[pl.ds(2, 2)], load_sem.at[1])
    for j in range(blocks):
        g_buf[j] = gate(2, j) * gate(3, j)
    pack(g_buf, 1)

    @pl.when(near_here)
    def _():
        give_whole(1)
        for slot in range(3):
            give_near(1, slot, True)

    @pl.when(whole_here)
    def _():
        give_near(1, 0)
        give_whole(1, True)

    @pl.when(far_two)
    def _():
        give_whole(1)
        give_far(1, range(pair), True)
        for signal in (0, 1):
            give_far(signal, range(side, split), True)

    @pl.when(far_one)
    def _():
        give_far(1, range(pair))
        give_whole(0)
        give_whole(1)
        for signal in (0, 1):
            give_far(signal, to_one, True)
        for signal in (0, 1):
            give_far(signal, range(side, split))

    wait_bytes(wide, load_sem.at[2])
    pack(wide, 2)

    @pl.when(whole_here)
    def _():
        give_whole(2, True)

    @pl.when(far_two)
    def _():
        give_whole(2)

    @pl.when(me < split)
    def _():
        pl.semaphore_wait(ready, pair)

    @pl.when(early)
    def _():
        give_far(0, to_one)

    @pl.when(near_here)
    def _():
        give_far(2, (*to_two, *to_one))
        give_whole(2)
        for slot in range(3):
            give_near(2, slot, True)

    @pl.when(whole_here)
    def _():
        for slot in (1, 2):
            for signal in (0, 1):
                give_near(signal, slot)
        for slot in range(3):
            give_near(2, slot)

    @pl.when(far_two)
    def _():
        for signal in (0, 1):
            give_far(signal, to_one)
        give_far(2, to_two, True)
        give_far(2, to_one)

    @pl.when(far_one)
    def _():
        give_whole(2)
        give_far(2, to_two)
        give_far(2, to_one, True)

    @pl.when(late)
    def _():
        extra[...] = jnp.zeros(extra.shape, jnp.float32)

    for j in range(blocks):
        part_send[pl.ds(j, 1), :] = jnp.sum(x_buf[j] * g_buf[j], axis=0, keepdims=True) * time_scale
    part_home[me] = part_send[...]
    for k in range(1, side):
        peer = base + lax.rem(me - base + k, side)
        small_copy(part_send, part_home.at[me], 0, {"seq": peer}).start()
    sq_acc[...] = jnp.zeros((8, LANES), jnp.float32)
    for load in loads:
        load.wait()

    def times(which, pieces, at_row, at_column):
        high, rest = pieces
        both = jnp.concatenate([high, rest], axis=1)
        main = jnp.dot(
            table[2 * which, at_row, at_column], both, preferred_element_type=jnp.float32
        )
        small = jnp.dot(
            table[2 * which + 1, at_row, at_column], high, preferred_element_type=jnp.float32
        )
        return main[:, :LANES] + (main[:, LANES:] + small)

    full = slice(0, points)
    early_part = slice(0, points // 2)
    late_part = slice(points // 2, points)

    def forward(slot, signal, part):
        start = (slot * 3 + signal) * devices + part.start // half
        sources = (part.stop - part.start) // half
        data = recv[pl.ds(start, sources)].reshape(sources * half, LANES)
        pieces = split_high_low(data)
        spec[slot, signal, 0] = times(0, pieces, full, part)
        spec[slot, signal, 1] = -times(1, pieces, full, part)

    def inverse(slot, kind, part, scale):
        series = times(0, split_high_low(prod[0]), part, full)
        series = series - times(1, split_high_low(prod[1]), part, full)
        series = series * (scale / points)
        start = part.start // half
        sources = (part.stop - part.start) // half
        back[slot, kind, start : start + sources] = series.reshape(sources, half, LANES)
        return series

    def square_sum(series):
        sq_acc[...] += jnp.sum((series * series).reshape(side * half // 8, 8, LANES), axis=0)

    step = 128

    def halves(slot, ref_row, part, at):
        value = spec[slot, ref_row, part, at, :]
        turned = pltpu.roll(value, low, 1)
        left = lax.broadcasted_iota(jnp.int32, (step, LANES), 1) < low
        return value, turned, jnp.where(left, value, turned), jnp.where(left, turned, value)

    def products(slot, signal, other_signal, conjugate):
        sign = jnp.where(lax.broadcasted_iota(jnp.int32, (step, LANES), 1) < low, 1.0, -1.0)

        @pl.loop(0, points // step)
        def _(index):
            at = pl.ds(pl.multiple_of(index * step, step), step)
            cosine = twist[0, at, :]
            sine = twist[1, at, :]
            signed = sine * sign
            _, _, even_re, odd_re = halves(slot, other_signal, 0, at)
            _, _, even_im, odd_im = halves(slot, other_signal, 1, at)
            a_re, as_re, _, _ = halves(slot, signal, 0, at)
            a_im, as_im, _, _ = halves(slot, signal, 1, at)
            p_re = even_re * cosine - even_im * sine
            p_im = even_im * cosine + even_re * sine
            if conjugate:
                r_re = odd_re * cosine - odd_im * signed
                r_im = odd_im * cosine + odd_re * signed
                prod[0, at, :] = a_re * p_re + a_im * p_im + (as_re * r_re + as_im * r_im)
                prod[1, at, :] = a_im * p_re - a_re * p_im + (as_im * r_re - as_re * r_im)
            else:
                r_re = odd_re * cosine + odd_im * signed
                r_im = odd_im * cosine - odd_re * signed
                prod[0, at, :] = a_re * p_re - a_im * p_im + (as_re * r_re - as_im * r_im)
                prod[1, at, :] = a_im * p_re + a_re * p_im + (as_im * r_re + as_re * r_im)

    @pl.when(near_here)
    def _():
        @pl.loop(0, 3)
        def _(slot):
            c = slot * pair + me
            for signal in (0, 1):
                await_input(slot, signal, 0, side)
                forward(slot, signal, early_part)
            products(slot, 1, 0, True)
            inverse(slot, 0, early_part, time_scale)
            inward(slot, 0, c)

        @pl.loop(0, 3)
        def _(slot):
            c = slot * pair + me
            await_input(slot, 2, 0, side)
            forward(slot, 2, early_part)
            products(slot, 1, 2, True)
            inverse(slot, 1, early_part, 1.0)
            inward(slot, 1, c)
            products(slot, 0, 2, False)
            inverse(slot, 2, early_part, 1.0)
            inward(slot, 2, c)

    def outward(slot, kind, c):
        @pl.when(whole_here)
        def _():
            for k in range(side):
                to_home(slot, kind, c, other + k)

        if kind < 2:
            @pl.when(late)
            def _():
                for k in range(side):
                    to_extra(slot, kind, c, other + k)

        inward(slot, kind, c)

    @pl.when(me >= pair)
    def _():
        zone = me // pair
        slots = 2 - lax.rem(zone, 2)

        @pl.when(late)
        def _():
            await_input(0, 1, side, side)

        @pl.loop(0, slots)
        def _(slot):
            c = lax.rem(me + side + side * slot, devices)

            @pl.when(late & (slot > 0))
            def _():
                await_input(slot, 1, side, side)

            @pl.when(late)
            def _():
                forward(slot, 1, late_part)

            await_input(slot, 0, 0, devices)

            forward(slot, 0, full)

            @pl.when(whole_here)
            def _():
                await_input(slot, 1, 0, devices)
                forward(slot, 1, full)
                give_far(2, (*to_two, *to_one))

            products(slot, 1, 0, True)
            series = inverse(slot, 0, full, time_scale)
            outward(slot, 0, c)
            square_sum(series[points // 2 :])

        @pl.when(late)
        def _():
            share_part()
            share_squares(sq_acc[...])

        @pl.loop(0, slots)
        def _(slot):
            c = lax.rem(me + side + side * slot, devices)
            await_input(slot, 2, 0, devices)
            forward(slot, 2, full)
            products(slot, 1, 2, True)
            inverse(slot, 1, full, 1.0)
            outward(slot, 1, c)

        @pl.loop(0, slots)
        def _(slot):
            c = lax.rem(me + side + side * slot, devices)
            products(slot, 0, 2, False)
            inverse(slot, 2, full, 1.0)
            outward(slot, 2, c)

    def await_home(kind):
        wait_bytes(home.at[kind], home_recv.at[kind])
        if kind < 2:
            @pl.when(early)
            def _():
                wait_bytes(extra.at[kind], extra_recv.at[kind])

    def unpack(kind, j):
        pieces = []
        for c in (2 * j, 2 * j + 1):
            value = home[kind, c]
            pieces.append(value + extra[kind, c] if kind < 2 and c < split else value)
        left, right = pieces
        flat[j, pl.ds(0, half, stride=2), :] = jnp.where(first, left, pltpu.roll(right, low, 1))
        flat[j, pl.ds(1, half, stride=2), :] = jnp.where(first, pltpu.roll(left, low, 1), right)
        return flat[j]

    pl.when(early)(share_part)
    wait_bytes(half_home, small_recv.at[2])
    direct = half_send[...] + half_home[...]
    for j in range(blocks):
        dskip_ref[:, columns_of(j)] = direct[j : j + 1]

    await_home(0)
    squares = sq_acc[...]
    for j in range(blocks):
        squares = squares + direct[j : j + 1] * direct[j : j + 1] * (1.0 / (8 * side))
    for j in range(blocks):
        value = unpack(0, j)
        dh_ref[:, columns_of(j)] = value
        squares = squares + jnp.sum((value * value).reshape(rows // 8, 8, LANES), axis=0)

    @pl.when(early)
    def _():
        share_squares(squares)

    def assemble_inner():
        await_home(2)
        for j in range(blocks):
            at = columns_of(j)
            inner = unpack(2, j) + skip_ref[:, at] * x_buf[j]
            out_ref[:, at] = (gate(2, j) * inner).astype(jnp.bfloat16)
            dq_ref[:, at] = (gate(3, j) * inner).astype(jnp.bfloat16)

    def assemble_grad():
        await_home(1)
        for j in range(blocks):
            at = columns_of(j)
            grad = unpack(1, j) + skip_ref[:, at] * g_buf[j]
            dk_ref[:, at] = (grad * gate(1, j)).astype(jnp.bfloat16)
            dv_ref[:, at] = (grad * gate(0, j)).astype(jnp.bfloat16)

    everyone = devices * groups

    def finish_squares():
        wait_bytes(sq_all.at[pl.ds(0, everyone - 1)], small_recv.at[1])
        total = sq_all[0]
        for k in range(1, everyone):
            total = total + sq_all[k]
        total = jnp.sum(total, axis=1, keepdims=True)
        rms_ref[...] = jnp.sqrt(total / count)

    assemble_inner()
    pl.when(early)(finish_squares)
    assemble_grad()
    pl.when(late)(finish_squares)

    for condition, sent, returned in (
        (near_here, 3 * (split - 3) + 2 * split + 3 * pair, 9 * (side - 1)),
        (whole_here, 5 * split + 3 * (pair - 1), 3 * (devices - 1)),
        (far_two, 3 * (split - 2) + 3 * pair, 2 * (2 * side + 3 * (side - 1))),
        (far_one, 3 * (split - 1) + 3 * pair, 2 * side + 3 * (side - 1)),
    ):
        @pl.when(condition)
        def _():
            wait_bytes(recv.at[pl.ds(0, sent)], in_send.at[0])
            wait_bytes(recv.at[pl.ds(0, returned)], out_send.at[0])

    wait_bytes(part_home.at[pl.ds(0, side - 1)], small_send.at[0])
    wait_bytes(half_home, small_send.at[2])
    wait_bytes(sq_all.at[pl.ds(0, everyone - 1)], small_send.at[1])


def emit(*refs):
    sources, targets, sem = refs[:7], refs[7:14], refs[14]
    copies = [
        pltpu.make_async_copy(source, target, sem.at[index])
        for index, (source, target) in enumerate(zip(sources, targets))
    ]
    for copy in copies:
        copy.start()
    for copy in copies:
        copy.wait()


def fused_body(query_input, key_input, value_input, cotangent, filter_taps, skip_gain):
    devices = lax.axis_size("seq")
    groups = lax.axis_size("ch")
    rows, channels = query_input.shape
    half = rows // 2
    points = half * devices
    tables, twists = half_tables(points)
    count = float(channels * groups * (rows * devices + 1))
    vmem = pl.BlockSpec(memory_space=pltpu.VMEM)
    hbm = pl.BlockSpec(memory_space=pltpu.HBM)
    chunks = 2 * channels // LANES
    blocks = channels // LANES
    shapes = [((rows, channels), jnp.bfloat16)] * 4 + [
        ((rows, channels), jnp.float32),
        ((1, channels), jnp.float32),
        ((1, 1), jnp.float32),
    ]
    held = pl.pallas_call(
        functools.partial(kernel, devices, groups, count),
        out_shape=tuple(pltpu.VMEM(*shape) for shape in shapes),
        in_specs=[hbm] * 8,
        out_specs=(vmem,) * 7,
        scratch_shapes=[
            pltpu.VMEM((4, rows, channels), jnp.bfloat16),
            pltpu.VMEM((1, channels), jnp.float32),
            pltpu.VMEM((blocks, rows, LANES), jnp.float32),
            pltpu.VMEM((blocks, rows, LANES), jnp.float32),
            pltpu.VMEM((blocks, rows, LANES), jnp.float32),
            pltpu.VMEM((blocks, rows, LANES), jnp.float32),
            pltpu.VMEM((3, chunks, half, LANES), jnp.float32),
            pltpu.VMEM((9 * devices, half, LANES), jnp.float32),
            pltpu.VMEM((3, 3, 2, points, LANES), jnp.float32),
            pltpu.VMEM((2, points, LANES), jnp.float32),
            pltpu.VMEM((3, 3, devices, half, LANES), jnp.float32),
            pltpu.VMEM((3, chunks, half, LANES), jnp.float32),
            pltpu.VMEM((2, 3 * (devices // 4), half, LANES), jnp.float32),
            pltpu.VMEM((blocks, LANES), jnp.float32),
            pltpu.VMEM((devices, blocks, LANES), jnp.float32),
            pltpu.VMEM((blocks, LANES), jnp.float32),
            pltpu.VMEM((blocks, LANES), jnp.float32),
            pltpu.VMEM((8, LANES), jnp.float32),
            pltpu.VMEM((1, 1, LANES), jnp.float32),
            pltpu.VMEM((devices * groups, 1, LANES), jnp.float32),
            pltpu.VMEM(tables.shape, jnp.bfloat16),
            pltpu.VMEM(twists.shape, jnp.float32),
            pltpu.SemaphoreType.DMA((6,)),
            pltpu.SemaphoreType.DMA((1,)),
            pltpu.SemaphoreType.DMA((9,)),
            pltpu.SemaphoreType.DMA((1,)),
            pltpu.SemaphoreType.DMA((3,)),
            pltpu.SemaphoreType.DMA((2,)),
            pltpu.SemaphoreType.DMA((3,)),
            pltpu.SemaphoreType.DMA((3,)),
            pltpu.SemaphoreType.REGULAR,
        ],
        compiler_params=pltpu.CompilerParams(
            collective_id=0, has_side_effects=True, vmem_limit_bytes=(64 << 20) - (960 << 10)
        ),
    )(
        key_input, value_input, query_input, cotangent, filter_taps,
        skip_gain.reshape(1, channels), jnp.asarray(tables), jnp.asarray(twists),
    )
    results = pl.pallas_call(
        emit,
        out_shape=tuple(jax.ShapeDtypeStruct(*shape) for shape in shapes),
        in_specs=[vmem] * 7,
        out_specs=(hbm,) * 7,
        scratch_shapes=[pltpu.SemaphoreType.DMA((7,))],
        compiler_params=pltpu.CompilerParams(vmem_limit_bytes=4 << 20),
    )(*held)
    return (*results[:5], results[5].reshape(channels), results[6].reshape(()))


def pick_body(query_input, *others):
    devices = lax.axis_size("seq")
    rows, channels = query_input.shape
    fits = devices == 8 and 2 * channels == LANES * devices and rows % 16 == 0
    chosen = fused_body if fits and rows * devices <= 2048 else body
    return chosen(query_input, *others)


def solution(mesh):
    return jax.shard_map(
        pick_body,
        mesh=mesh,
        in_specs=(
            P("seq", "ch"),
            P("seq", "ch"),
            P("seq", "ch"),
            P("seq", "ch"),
            P("seq", "ch"),
            P("ch"),
        ),
        out_specs=(
            P("seq", "ch"),
            P("seq", "ch"),
            P("seq", "ch"),
            P("seq", "ch"),
            P("seq", "ch"),
            P("ch"),
            P(),
        ),
        check_vma=False,
    )
```

```python
import functools
import math

import jax
import jax.numpy as jnp
import numpy as np
from jax import lax
from jax.experimental import pallas as pl
from jax.experimental.pallas import tpu as pltpu
from jax.sharding import PartitionSpec as P

LANES = 128
MESH = pl.DeviceIdType.MESH


def complex_mul(left_op, right_op):
    return jnp.stack(
        [
            left_op[0] * right_op[0] - left_op[1] * right_op[1],
            left_op[0] * right_op[1] + left_op[1] * right_op[0],
        ]
    )


def conj_of(stacked):
    return jnp.stack([stacked[0], -stacked[1]])


def dft_table(length, direction):
    counter = jnp.arange(length)
    angles = (
        2.0 * math.pi / length * (counter[:, None] * counter[None, :] % length).astype(jnp.float32)
    )
    return (jnp.cos(angles), direction * jnp.sin(angles))


def dft_along(stacked, length, direction, pattern):
    table_re, table_im = dft_table(length, direction)

    def contract(table, part_in):
        return jnp.einsum(pattern, table, part_in, precision=lax.Precision.HIGHEST)

    real_out = contract(table_re, stacked[0]) - contract(table_im, stacked[1])
    imag_out = contract(table_re, stacked[1]) + contract(table_im, stacked[0])
    return jnp.stack([real_out, imag_out])


def grid_twiddle(devices, block, direction):
    seq_length = devices * block
    counter = jnp.arange(devices)[:, None] * jnp.arange(block)[None, :] % seq_length
    angles = direction * 2.0 * math.pi / seq_length * counter.astype(jnp.float32)
    return jnp.stack([jnp.cos(angles), jnp.sin(angles)])[:, None, None]


def local_forward(stacked, devices, block):
    array_shape = stacked.shape
    stacked = stacked.reshape(array_shape[0], array_shape[1], array_shape[2], devices, block)
    stacked = dft_along(stacked, devices, -1.0, "kj,scjp->sckp")
    stacked = complex_mul(stacked, grid_twiddle(devices, block, -1.0))
    return dft_along(stacked, block, -1.0, "kp,scjp->scjk")


def local_inverse(stacked, devices, block):
    stacked = dft_along(stacked, block, 1.0, "kp,scjp->scjk")
    stacked = complex_mul(stacked, grid_twiddle(devices, block, 1.0))
    stacked = dft_along(stacked, devices, 1.0, "kj,scjp->sckp")
    array_shape = stacked.shape
    return stacked.reshape(array_shape[0], array_shape[1], array_shape[2], devices * block) / (
        devices * block
    )


def modulated(signals, cosine, sine_part):
    zero_part = jnp.zeros_like(signals)
    return jnp.stack(
        [
            jnp.concatenate([signals, signals * cosine]),
            jnp.concatenate([zero_part, -signals * sine_part]),
        ]
    )


def spectral_products(spectrum):
    mixed_spec = spectrum[:, 0::3]
    gated_spec = spectrum[:, 1::3]
    taps_spec = spectrum[:, 2::3]
    out_spec = complex_mul(mixed_spec, taps_spec)
    back_spec = complex_mul(gated_spec, conj_of(taps_spec))
    grad_spec = complex_mul(gated_spec, conj_of(mixed_spec))
    return jnp.stack(
        [
            out_spec[:, 0],
            back_spec[:, 0],
            grad_spec[:, 0],
            out_spec[:, 1],
            back_spec[:, 1],
            grad_spec[:, 1],
        ],
        axis=1,
    )


def unfold(series, cosine, sine_part):
    return tuple(
        (
            0.5
            * (
                series[0, signal_index]
                + cosine * series[0, signal_index + 3]
                - sine_part * series[1, signal_index + 3]
            )
            for signal_index in range(3)
        )
    )


def channel_local(mixed_in, gated_cot, filter_taps, devices):
    pieces = (
        lax.all_to_all(mixed_in, "seq", split_axis=1, concat_axis=0, tiled=True),
        lax.all_to_all(gated_cot, "seq", split_axis=1, concat_axis=0, tiled=True),
        lax.all_to_all(filter_taps, "seq", split_axis=1, concat_axis=0, tiled=True),
    )
    laid = jnp.transpose(jnp.stack(pieces), (0, 2, 1))
    seq_length = laid.shape[2]
    block = seq_length // devices
    angles = math.pi / seq_length * jnp.arange(seq_length).astype(jnp.float32)
    cosine = jnp.cos(angles)
    sine_row = jnp.sin(angles)
    spectrum = local_forward(modulated(laid, cosine, sine_row), devices, block)
    series = local_inverse(spectral_products(spectrum), devices, block)
    results = unfold(series, cosine, sine_row)
    return (
        lax.all_to_all(results[0].T, "seq", split_axis=0, concat_axis=1, tiled=True),
        lax.all_to_all(results[1].T, "seq", split_axis=0, concat_axis=1, tiled=True),
        lax.all_to_all(results[2].T, "seq", split_axis=0, concat_axis=1, tiled=True),
    )


def body(query_input, key_input, value_input, cotangent, filter_taps, skip_gain):
    devices = lax.axis_size("seq")
    row_count, channels = query_input.shape
    seq_length = row_count * devices
    query_val = query_input.astype(jnp.float32)
    key_val = key_input.astype(jnp.float32)
    value_val = value_input.astype(jnp.float32)
    cot_val = cotangent.astype(jnp.float32)
    mixed_in = key_val * value_val
    gated_cot = query_val * cot_val
    conv_out, back_conv, kernel_grad = channel_local(mixed_in, gated_cot, filter_taps, devices)
    inner_sum = conv_out + skip_gain[None, :] * mixed_in
    mixed_grad = back_conv + skip_gain[None, :] * gated_cot
    output = (query_val * inner_sum).astype(jnp.bfloat16)
    query_grad = (cot_val * inner_sum).astype(jnp.bfloat16)
    key_grad = (mixed_grad * value_val).astype(jnp.bfloat16)
    value_grad = (mixed_grad * key_val).astype(jnp.bfloat16)
    time_scale = 1.0 / math.sqrt(seq_length)
    filter_grad = kernel_grad * time_scale
    filter_sq = jnp.sum(filter_grad * filter_grad)
    skip_part = jnp.sum(gated_cot * mixed_in, axis=0) * time_scale
    skip_grad = lax.psum(skip_part, "seq")
    total_sq = lax.psum(filter_sq + jnp.sum(skip_grad * skip_grad) / devices, ("seq", "ch"))
    grad_rms = jnp.sqrt(total_sq / (channels * lax.axis_size("ch") * (seq_length + 1)))
    return (output, query_grad, key_grad, value_grad, filter_grad, skip_grad, grad_rms)


def split_high_low(array):
    high = array.astype(jnp.bfloat16)
    return high, (array - high.astype(jnp.float32)).astype(jnp.bfloat16)


def half_tables(points):
    odd = 2 * np.arange(points, dtype=np.int64) + 1
    angles = math.pi / (4 * points) * (odd[:, None] * odd[None, :] % (8 * points))
    parts = []
    for table in (np.cos(angles), np.sin(angles)):
        table = table.astype(np.float32)
        high = table.astype(jnp.bfloat16)
        parts += [high, (table - high.astype(np.float32)).astype(jnp.bfloat16)]
    shift = math.pi / (4 * points) * odd[:, None] * np.ones((1, LANES))
    return np.stack(parts), np.stack([np.cos(shift), np.sin(shift)]).astype(np.float32)


def kernel(
    devices, groups, count,
    k_hbm, v_hbm, q_hbm, c_hbm, h_hbm, skip_hbm, table_hbm, twist_hbm,
    out_ref, dq_ref, dk_ref, dv_ref, dh_ref, last_ref,
    gates, skip_ref, x_buf, g_buf, wide, flat,
    send, recv, spec, prod, back, home, extra,
    part_send, part_home, half_send, half_home, sq_acc, sq_send, sq_all, table, twist,
    load_sem, in_send, in_recv, out_send, home_recv, extra_recv, small_send, small_recv, ready,
):
    me = lax.axis_index("seq")
    mine = lax.axis_index("ch")
    rows, channels = q_hbm.shape
    half = rows // 2
    points = half * devices
    low = LANES // 2
    time_scale = 1.0 / math.sqrt(2 * points)
    blocks = channels // LANES
    side = devices // 2
    pair = devices // 4
    split = 3 * pair
    base = me // side * side
    other = side - base
    early = me < side
    late = me >= side
    near_here = me < pair
    whole_here = (me >= pair) & (me < side)
    far_two = (me >= side) & (me < split)
    far_one = me >= split

    barrier = pltpu.get_barrier_semaphore()
    for k in range(1, groups):
        pl.semaphore_signal(
            barrier, inc=1, device_id={"ch": lax.rem(mine + k, groups)}, device_id_type=MESH
        )

    @pl.when(me < split)
    def _():
        for k in range(1, devices):
            pl.semaphore_signal(
                barrier, inc=1, device_id={"seq": lax.rem(me + k, devices)}, device_id_type=MESH
            )

    @pl.when(far_one)
    def _():
        for k in range(1, pair):
            peer = split + lax.rem(me - split + k, pair)
            pl.semaphore_signal(barrier, inc=1, device_id={"seq": peer}, device_id_type=MESH)

    def columns_of(j):
        return pl.ds(j * LANES, LANES)

    for index, source in enumerate((k_hbm, v_hbm, q_hbm, c_hbm)):
        pltpu.make_async_copy(source, gates.at[index], load_sem.at[index // 2]).start()
    for j in range(blocks):
        pltpu.make_async_copy(h_hbm.at[:, columns_of(j)], wide.at[j], load_sem.at[2]).start()
    loads = (
        pltpu.make_async_copy(skip_hbm, skip_ref, load_sem.at[3]),
        pltpu.make_async_copy(table_hbm, table, load_sem.at[4]),
        pltpu.make_async_copy(twist_hbm, twist, load_sem.at[5]),
    )
    for load in loads:
        load.start()

    @pl.when(far_one)
    def _():
        pl.semaphore_wait(barrier, devices + groups - 2)
        for device in range(split):
            pl.semaphore_signal(
                ready, inc=1, device_id={"seq": jnp.int32(device)}, device_id_type=MESH
            )

    def gate(index, j):
        return gates[index, :, columns_of(j)].astype(jnp.float32)

    def wait_bytes(ref, sem):
        pltpu.make_async_copy(ref, ref, sem).wait()

    def near_owner(c):
        return (c % pair, c // pair)

    def far_owner(c):
        return (side + c, 0) if c < side else (c, 1)

    def whole_owner(c):
        return (c - side, 0)

    def give(signal, c, owner, can_be_me):
        device, slot = owner
        target = recv.at[(slot * 3 + signal) * devices + me]
        sem = in_recv.at[slot * 3 + signal]

        def remote():
            pltpu.make_async_remote_copy(
                src_ref=send.at[signal, c],
                dst_ref=target,
                send_sem=in_send.at[0],
                recv_sem=sem,
                device_id={"seq": jnp.int32(device)},
                device_id_type=MESH,
            ).start()

        if not can_be_me:
            remote()
            return

        pl.when(me != device)(remote)

        @pl.when(me == device)
        def _():
            pltpu.make_async_copy(send.at[signal, c], target, sem).start()

    def give_far(signal, chunks, can_be_me=False):
        for c in chunks:
            give(signal, c, far_owner(c), can_be_me)

    def give_whole(signal, can_be_me=False):
        for c in range(split, devices):
            give(signal, c, whole_owner(c), can_be_me)

    def give_near(signal, slot, can_be_me=False):
        for c in range(slot * pair, (slot + 1) * pair):
            give(signal, c, near_owner(c), can_be_me)

    def await_input(slot, signal, start, sources):
        first_one = (slot * 3 + signal) * devices + start
        wait_bytes(recv.at[pl.ds(first_one, sources)], in_recv.at[slot * 3 + signal])

    def to_home(slot, kind, c, dest):
        pltpu.make_async_remote_copy(
            src_ref=back.at[slot, kind, dest],
            dst_ref=home.at[kind, c],
            send_sem=out_send.at[0],
            recv_sem=home_recv.at[kind],
            device_id={"seq": dest},
            device_id_type=MESH,
        ).start()

    def to_extra(slot, kind, c, dest):
        pltpu.make_async_remote_copy(
            src_ref=back.at[slot, kind, dest],
            dst_ref=extra.at[kind, c],
            send_sem=out_send.at[0],
            recv_sem=extra_recv.at[kind],
            device_id={"seq": dest},
            device_id_type=MESH,
        ).start()

    def inward(slot, kind, c):
        for k in range(1, side):
            to_home(slot, kind, c, base + lax.rem(me - base + k, side))
        pltpu.make_async_copy(back.at[slot, kind, me], home.at[kind, c], home_recv.at[kind]).start()

    def small_copy(source, target, index, device_id):
        return pltpu.make_async_remote_copy(
            src_ref=source,
            dst_ref=target,
            send_sem=small_send.at[index],
            recv_sem=small_recv.at[index],
            device_id=device_id,
            device_id_type=MESH,
        )

    def share_part():
        wait_bytes(part_home.at[pl.ds(0, side - 1)], small_recv.at[0])
        part = part_home[base]
        for k in range(1, side):
            part = part + part_home[base + k]
        half_send[...] = part
        peer = lax.rem(me + side, devices)
        small_copy(half_send, half_home, 2, {"seq": peer}).start()

    def share_squares(squares):
        row = jnp.sum(squares, axis=0, keepdims=True)
        sq_send[0] = row
        sq_all[me * groups + mine] = row
        for k in range(devices):
            for n in range(groups):
                if k or n:
                    peer = {"seq": lax.rem(me + k, devices), "ch": lax.rem(mine + n, groups)}
                    small_copy(sq_send.at[0], sq_all.at[me * groups + mine], 1, peer).start()

    first = lax.broadcasted_iota(jnp.int32, (half, LANES), 1) < low

    def pack(source, signal):
        for j in range(blocks):
            even = source[j, pl.ds(0, half, stride=2), :]
            odd = source[j, pl.ds(1, half, stride=2), :]
            send[signal, 2 * j] = jnp.where(first, even, pltpu.roll(odd, low, 1))
            send[signal, 2 * j + 1] = jnp.where(first, pltpu.roll(even, low, 1), odd)

    wait_bytes(gates.at[pl.ds(0, 2)], load_sem.at[0])
    for j in range(blocks):
        x_buf[j] = gate(0, j) * gate(1, j)
    pack(x_buf, 0)
    @pl.when(me < split)
    def _():
        pl.semaphore_wait(barrier, split + groups - 2)

    to_two = (*range(pair), *range(side, split))
    to_one = range(pair, side)

    @pl.when(early)
    def _():
        give_far(0, to_two)

    @pl.when(near_here)
    def _():
        give_whole(0)
        for slot in range(3):
            give_near(0, slot, True)

    @pl.when(whole_here)
    def _():
        give_near(0, 0)
        give_whole(0, True)

    @pl.when(far_two)
    def _():
        give_whole(0)
        give_far(0, range(pair), True)

    @pl.when(far_one)
    def _():
        give_far(0, range(pair))

    wait_bytes(gates.at[pl.ds(2, 2)], load_sem.at[1])
    for j in range(blocks):
        g_buf[j] = gate(2, j) * gate(3, j)
    pack(g_buf, 1)

    @pl.when(near_here)
    def _():
        give_whole(1)
        for slot in range(3):
            give_near(1, slot, True)

    @pl.when(whole_here)
    def _():
        give_near(1, 0)
        give_whole(1, True)

    @pl.when(far_two)
    def _():
        give_whole(1)
        give_far(1, range(pair), True)
        for signal in (0, 1):
            give_far(signal, range(side, split), True)

    @pl.when(far_one)
    def _():
        give_far(1, range(pair))
        give_whole(0)
        give_whole(1)
        for signal in (0, 1):
            give_far(signal, to_one, True)
        for signal in (0, 1):
            give_far(signal, range(side, split))

    wait_bytes(wide, load_sem.at[2])
    pack(wide, 2)

    @pl.when(whole_here)
    def _():
        give_whole(2, True)

    @pl.when(far_two)
    def _():
        give_whole(2)

    @pl.when(me < split)
    def _():
        pl.semaphore_wait(ready, pair)

    @pl.when(early)
    def _():
        give_far(0, to_one)

    @pl.when(near_here)
    def _():
        give_far(2, (*to_two, *to_one))
        give_whole(2)
        for slot in range(3):
            give_near(2, slot, True)

    @pl.when(whole_here)
    def _():
        for slot in (1, 2):
            for signal in (0, 1):
                give_near(signal, slot)
        for slot in range(3):
            give_near(2, slot)

    @pl.when(far_two)
    def _():
        for signal in (0, 1):
            give_far(signal, to_one)
        give_far(2, to_two, True)
        give_far(2, to_one)

    @pl.when(far_one)
    def _():
        give_whole(2)
        give_far(2, to_two)
        give_far(2, to_one, True)

    @pl.when(late)
    def _():
        extra[...] = jnp.zeros(extra.shape, jnp.float32)

    for j in range(blocks):
        part_send[pl.ds(j, 1), :] = jnp.sum(x_buf[j] * g_buf[j], axis=0, keepdims=True) * time_scale
    part_home[me] = part_send[...]
    for k in range(1, side):
        peer = base + lax.rem(me - base + k, side)
        small_copy(part_send, part_home.at[me], 0, {"seq": peer}).start()
    sq_acc[...] = jnp.zeros((8, LANES), jnp.float32)
    for load in loads:
        load.wait()

    def times(which, pieces, at_row, at_column):
        high, rest = pieces
        both = jnp.concatenate([high, rest], axis=1)
        main = jnp.dot(
            table[2 * which, at_row, at_column], both, preferred_element_type=jnp.float32
        )
        small = jnp.dot(
            table[2 * which + 1, at_row, at_column], high, preferred_element_type=jnp.float32
        )
        return main[:, :LANES] + (main[:, LANES:] + small)

    full = slice(0, points)
    early_part = slice(0, points // 2)
    late_part = slice(points // 2, points)

    def forward(slot, signal, part):
        start = (slot * 3 + signal) * devices + part.start // half
        sources = (part.stop - part.start) // half
        data = recv[pl.ds(start, sources)].reshape(sources * half, LANES)
        pieces = split_high_low(data)
        spec[slot, signal, 0] = times(0, pieces, full, part)
        spec[slot, signal, 1] = -times(1, pieces, full, part)

    def inverse(slot, kind, part, scale):
        series = times(0, split_high_low(prod[0]), part, full)
        series = series - times(1, split_high_low(prod[1]), part, full)
        series = series * (scale / points)
        start = part.start // half
        sources = (part.stop - part.start) // half
        back[slot, kind, start : start + sources] = series.reshape(sources, half, LANES)
        return series

    def square_sum(series):
        sq_acc[...] += jnp.sum((series * series).reshape(side * half // 8, 8, LANES), axis=0)

    step = 128

    def halves(slot, ref_row, part, at):
        value = spec[slot, ref_row, part, at, :]
        turned = pltpu.roll(value, low, 1)
        left = lax.broadcasted_iota(jnp.int32, (step, LANES), 1) < low
        return value, turned, jnp.where(left, value, turned), jnp.where(left, turned, value)

    def products(slot, signal, other_signal, conjugate):
        sign = jnp.where(lax.broadcasted_iota(jnp.int32, (step, LANES), 1) < low, 1.0, -1.0)

        @pl.loop(0, points // step)
        def _(index):
            at = pl.ds(pl.multiple_of(index * step, step), step)
            cosine = twist[0, at, :]
            sine = twist[1, at, :]
            signed = sine * sign
            _, _, even_re, odd_re = halves(slot, other_signal, 0, at)
            _, _, even_im, odd_im = halves(slot, other_signal, 1, at)
            a_re, as_re, _, _ = halves(slot, signal, 0, at)
            a_im, as_im, _, _ = halves(slot, signal, 1, at)
            p_re = even_re * cosine - even_im * sine
            p_im = even_im * cosine + even_re * sine
            if conjugate:
                r_re = odd_re * cosine - odd_im * signed
                r_im = odd_im * cosine + odd_re * signed
                prod[0, at, :] = a_re * p_re + a_im * p_im + (as_re * r_re + as_im * r_im)
                prod[1, at, :] = a_im * p_re - a_re * p_im + (as_im * r_re - as_re * r_im)
            else:
                r_re = odd_re * cosine + odd_im * signed
                r_im = odd_im * cosine - odd_re * signed
                prod[0, at, :] = a_re * p_re - a_im * p_im + (as_re * r_re - as_im * r_im)
                prod[1, at, :] = a_im * p_re + a_re * p_im + (as_im * r_re + as_re * r_im)

    @pl.when(near_here)
    def _():
        @pl.loop(0, 3)
        def _(slot):
            c = slot * pair + me
            for signal in (0, 1):
                await_input(slot, signal, 0, side)
                forward(slot, signal, early_part)
            products(slot, 1, 0, True)
            inverse(slot, 0, early_part, time_scale)
            inward(slot, 0, c)

        @pl.loop(0, 3)
        def _(slot):
            c = slot * pair + me
            await_input(slot, 2, 0, side)
            forward(slot, 2, early_part)
            products(slot, 1, 2, True)
            inverse(slot, 1, early_part, 1.0)
            inward(slot, 1, c)
            products(slot, 0, 2, False)
            inverse(slot, 2, early_part, 1.0)
            inward(slot, 2, c)

    def outward(slot, kind, c):
        @pl.when(whole_here)
        def _():
            for k in range(side):
                to_home(slot, kind, c, other + k)

        if kind < 2:
            @pl.when(late)
            def _():
                for k in range(side):
                    to_extra(slot, kind, c, other + k)

        inward(slot, kind, c)

    @pl.when(me >= pair)
    def _():
        zone = me // pair
        slots = 2 - lax.rem(zone, 2)

        @pl.when(late)
        def _():
            await_input(0, 1, side, side)

        @pl.loop(0, slots)
        def _(slot):
            c = lax.rem(me + side + side * slot, devices)

            @pl.when(late & (slot > 0))
            def _():
                await_input(slot, 1, side, side)

            @pl.when(late)
            def _():
                forward(slot, 1, late_part)

            await_input(slot, 0, 0, devices)

            forward(slot, 0, full)

            @pl.when(whole_here)
            def _():
                await_input(slot, 1, 0, devices)
                forward(slot, 1, full)
                give_far(2, (*to_two, *to_one))

            products(slot, 1, 0, True)
            series = inverse(slot, 0, full, time_scale)
            outward(slot, 0, c)
            square_sum(series[points // 2 :])

        @pl.when(late)
        def _():
            share_part()
            share_squares(sq_acc[...])

        @pl.loop(0, slots)
        def _(slot):
            c = lax.rem(me + side + side * slot, devices)
            await_input(slot, 2, 0, devices)
            forward(slot, 2, full)
            products(slot, 1, 2, True)
            inverse(slot, 1, full, 1.0)
            outward(slot, 1, c)

        @pl.loop(0, slots)
        def _(slot):
            c = lax.rem(me + side + side * slot, devices)
            products(slot, 0, 2, False)
            inverse(slot, 2, full, 1.0)
            outward(slot, 2, c)

    def await_home(kind):
        wait_bytes(home.at[kind], home_recv.at[kind])
        if kind < 2:
            @pl.when(early)
            def _():
                wait_bytes(extra.at[kind], extra_recv.at[kind])

    def unpack(kind, j):
        pieces = []
        for c in (2 * j, 2 * j + 1):
            value = home[kind, c]
            pieces.append(value + extra[kind, c] if kind < 2 and c < split else value)
        left, right = pieces
        flat[j, pl.ds(0, half, stride=2), :] = jnp.where(first, left, pltpu.roll(right, low, 1))
        flat[j, pl.ds(1, half, stride=2), :] = jnp.where(first, pltpu.roll(left, low, 1), right)
        return flat[j]

    pl.when(early)(share_part)
    wait_bytes(half_home, small_recv.at[2])
    direct = half_send[...] + half_home[...]
    for j in range(blocks):
        last_ref[0:1, columns_of(j)] = direct[j : j + 1]

    await_home(0)
    squares = sq_acc[...]
    for j in range(blocks):
        squares = squares + direct[j : j + 1] * direct[j : j + 1] * (1.0 / (8 * side))
    for j in range(blocks):
        value = unpack(0, j)
        dh_ref[:, columns_of(j)] = value
        squares = squares + jnp.sum((value * value).reshape(rows // 8, 8, LANES), axis=0)

    @pl.when(early)
    def _():
        share_squares(squares)

    def assemble_inner():
        await_home(2)
        for j in range(blocks):
            at = columns_of(j)
            inner = unpack(2, j) + skip_ref[:, at] * x_buf[j]
            out_ref[:, at] = (gate(2, j) * inner).astype(jnp.bfloat16)
            dq_ref[:, at] = (gate(3, j) * inner).astype(jnp.bfloat16)

    def assemble_grad():
        await_home(1)
        for j in range(blocks):
            at = columns_of(j)
            grad = unpack(1, j) + skip_ref[:, at] * g_buf[j]
            dk_ref[:, at] = (grad * gate(1, j)).astype(jnp.bfloat16)
            dv_ref[:, at] = (grad * gate(0, j)).astype(jnp.bfloat16)

    everyone = devices * groups

    def finish_squares():
        wait_bytes(sq_all.at[pl.ds(0, everyone - 1)], small_recv.at[1])
        total = sq_all[0]
        for k in range(1, everyone):
            total = total + sq_all[k]
        total = jnp.sum(total, axis=1, keepdims=True)
        last_ref[1:2, :] = jnp.broadcast_to(jnp.sqrt(total / count), (1, channels))

    assemble_inner()
    pl.when(early)(finish_squares)
    assemble_grad()
    pl.when(late)(finish_squares)

    for condition, sent, returned in (
        (near_here, 3 * (split - 3) + 2 * split + 3 * pair, 9 * (side - 1)),
        (whole_here, 5 * split + 3 * (pair - 1), 3 * (devices - 1)),
        (far_two, 3 * (split - 2) + 3 * pair, 2 * (2 * side + 3 * (side - 1))),
        (far_one, 3 * (split - 1) + 3 * pair, 2 * side + 3 * (side - 1)),
    ):
        @pl.when(condition)
        def _():
            wait_bytes(recv.at[pl.ds(0, sent)], in_send.at[0])
            wait_bytes(recv.at[pl.ds(0, returned)], out_send.at[0])

    wait_bytes(part_home.at[pl.ds(0, side - 1)], small_send.at[0])
    wait_bytes(half_home, small_send.at[2])
    wait_bytes(sq_all.at[pl.ds(0, everyone - 1)], small_send.at[1])


def emit(*refs):
    sources, last_ref, targets = refs[:5], refs[5], refs[6:13]
    skip_row, rms_value, sem = refs[13:]
    sources = (*sources, skip_row, rms_value)
    copies = [
        pltpu.make_async_copy(source, target, sem.at[index])
        for index, (source, target) in enumerate(zip(sources, targets))
    ]
    for copy in copies[:5]:
        copy.start()
    skip_row[...] = last_ref[0:1, :]
    rms_value[...] = last_ref[1:2, 0:1]
    for copy in copies[5:]:
        copy.start()
    for copy in copies:
        copy.wait()


def fused_body(query_input, key_input, value_input, cotangent, filter_taps, skip_gain):
    devices = lax.axis_size("seq")
    groups = lax.axis_size("ch")
    rows, channels = query_input.shape
    half = rows // 2
    points = half * devices
    tables, twists = half_tables(points)
    count = float(channels * groups * (rows * devices + 1))
    vmem = pl.BlockSpec(memory_space=pltpu.VMEM)
    hbm = pl.BlockSpec(memory_space=pltpu.HBM)
    chunks = 2 * channels // LANES
    blocks = channels // LANES
    shapes = [((rows, channels), jnp.bfloat16)] * 4 + [
        ((rows, channels), jnp.float32),
        ((1, channels), jnp.float32),
        ((1, 1), jnp.float32),
    ]
    held = pl.pallas_call(
        functools.partial(kernel, devices, groups, count),
        out_shape=tuple(
            pltpu.VMEM(*shape) for shape in (*shapes[:5], ((2, channels), jnp.float32))
        ),
        in_specs=[hbm] * 8,
        out_specs=(vmem,) * 6,
        scratch_shapes=[
            pltpu.VMEM((4, rows, channels), jnp.bfloat16),
            pltpu.VMEM((1, channels), jnp.float32),
            pltpu.VMEM((blocks, rows, LANES), jnp.float32),
            pltpu.VMEM((blocks, rows, LANES), jnp.float32),
            pltpu.VMEM((blocks, rows, LANES), jnp.float32),
            pltpu.VMEM((blocks, rows, LANES), jnp.float32),
            pltpu.VMEM((3, chunks, half, LANES), jnp.float32),
            pltpu.VMEM((9 * devices, half, LANES), jnp.float32),
            pltpu.VMEM((3, 3, 2, points, LANES), jnp.float32),
            pltpu.VMEM((2, points, LANES), jnp.float32),
            pltpu.VMEM((3, 3, devices, half, LANES), jnp.float32),
            pltpu.VMEM((3, chunks, half, LANES), jnp.float32),
            pltpu.VMEM((2, 3 * (devices // 4), half, LANES), jnp.float32),
            pltpu.VMEM((blocks, LANES), jnp.float32),
            pltpu.VMEM((devices, blocks, LANES), jnp.float32),
            pltpu.VMEM((blocks, LANES), jnp.float32),
            pltpu.VMEM((blocks, LANES), jnp.float32),
            pltpu.VMEM((8, LANES), jnp.float32),
            pltpu.VMEM((1, 1, LANES), jnp.float32),
            pltpu.VMEM((devices * groups, 1, LANES), jnp.float32),
            pltpu.VMEM(tables.shape, jnp.bfloat16),
            pltpu.VMEM(twists.shape, jnp.float32),
            pltpu.SemaphoreType.DMA((6,)),
            pltpu.SemaphoreType.DMA((1,)),
            pltpu.SemaphoreType.DMA((9,)),
            pltpu.SemaphoreType.DMA((1,)),
            pltpu.SemaphoreType.DMA((3,)),
            pltpu.SemaphoreType.DMA((2,)),
            pltpu.SemaphoreType.DMA((3,)),
            pltpu.SemaphoreType.DMA((3,)),
            pltpu.SemaphoreType.REGULAR,
        ],
        compiler_params=pltpu.CompilerParams(
            collective_id=0, has_side_effects=True, vmem_limit_bytes=(64 << 20) - (960 << 10)
        ),
    )(
        key_input, value_input, query_input, cotangent, filter_taps,
        skip_gain.reshape(1, channels), jnp.asarray(tables), jnp.asarray(twists),
    )
    results = pl.pallas_call(
        emit,
        out_shape=tuple(jax.ShapeDtypeStruct(*shape) for shape in shapes),
        in_specs=[vmem] * 6,
        out_specs=(hbm,) * 7,
        scratch_shapes=[
            pltpu.VMEM((1, channels), jnp.float32),
            pltpu.VMEM((1, 1), jnp.float32),
            pltpu.SemaphoreType.DMA((7,)),
        ],
        compiler_params=pltpu.CompilerParams(vmem_limit_bytes=4 << 20),
    )(*held)
    return (*results[:5], results[5].reshape(channels), results[6].reshape(()))


def pick_body(query_input, *others):
    devices = lax.axis_size("seq")
    rows, channels = query_input.shape
    fits = devices == 8 and 2 * channels == LANES * devices and rows % 16 == 0
    chosen = fused_body if fits and rows * devices <= 2048 else body
    return chosen(query_input, *others)


def solution(mesh):
    return jax.shard_map(
        pick_body,
        mesh=mesh,
        in_specs=(
            P("seq", "ch"),
            P("seq", "ch"),
            P("seq", "ch"),
            P("seq", "ch"),
            P("seq", "ch"),
            P("ch"),
        ),
        out_specs=(
            P("seq", "ch"),
            P("seq", "ch"),
            P("seq", "ch"),
            P("seq", "ch"),
            P("seq", "ch"),
            P("ch"),
            P(),
        ),
        check_vma=False,
    )
```

```python
import functools
import math

import jax
import jax.numpy as jnp
import numpy as np
from jax import lax
from jax.experimental import pallas as pl
from jax.experimental.pallas import tpu as pltpu
from jax.sharding import PartitionSpec as P

LANES = 128
MESH = pl.DeviceIdType.MESH


def complex_mul(left_op, right_op):
    return jnp.stack(
        [
            left_op[0] * right_op[0] - left_op[1] * right_op[1],
            left_op[0] * right_op[1] + left_op[1] * right_op[0],
        ]
    )


def conj_of(stacked):
    return jnp.stack([stacked[0], -stacked[1]])


def dft_table(length, direction):
    counter = jnp.arange(length)
    angles = (
        2.0 * math.pi / length * (counter[:, None] * counter[None, :] % length).astype(jnp.float32)
    )
    return (jnp.cos(angles), direction * jnp.sin(angles))


def dft_along(stacked, length, direction, pattern):
    table_re, table_im = dft_table(length, direction)

    def contract(table, part_in):
        return jnp.einsum(pattern, table, part_in, precision=lax.Precision.HIGHEST)

    real_out = contract(table_re, stacked[0]) - contract(table_im, stacked[1])
    imag_out = contract(table_re, stacked[1]) + contract(table_im, stacked[0])
    return jnp.stack([real_out, imag_out])


def grid_twiddle(devices, block, direction):
    seq_length = devices * block
    counter = jnp.arange(devices)[:, None] * jnp.arange(block)[None, :] % seq_length
    angles = direction * 2.0 * math.pi / seq_length * counter.astype(jnp.float32)
    return jnp.stack([jnp.cos(angles), jnp.sin(angles)])[:, None, None]


def local_forward(stacked, devices, block):
    array_shape = stacked.shape
    stacked = stacked.reshape(array_shape[0], array_shape[1], array_shape[2], devices, block)
    stacked = dft_along(stacked, devices, -1.0, "kj,scjp->sckp")
    stacked = complex_mul(stacked, grid_twiddle(devices, block, -1.0))
    return dft_along(stacked, block, -1.0, "kp,scjp->scjk")


def local_inverse(stacked, devices, block):
    stacked = dft_along(stacked, block, 1.0, "kp,scjp->scjk")
    stacked = complex_mul(stacked, grid_twiddle(devices, block, 1.0))
    stacked = dft_along(stacked, devices, 1.0, "kj,scjp->sckp")
    array_shape = stacked.shape
    return stacked.reshape(array_shape[0], array_shape[1], array_shape[2], devices * block) / (
        devices * block
    )


def modulated(signals, cosine, sine_part):
    zero_part = jnp.zeros_like(signals)
    return jnp.stack(
        [
            jnp.concatenate([signals, signals * cosine]),
            jnp.concatenate([zero_part, -signals * sine_part]),
        ]
    )


def spectral_products(spectrum):
    mixed_spec = spectrum[:, 0::3]
    gated_spec = spectrum[:, 1::3]
    taps_spec = spectrum[:, 2::3]
    out_spec = complex_mul(mixed_spec, taps_spec)
    back_spec = complex_mul(gated_spec, conj_of(taps_spec))
    grad_spec = complex_mul(gated_spec, conj_of(mixed_spec))
    return jnp.stack(
        [
            out_spec[:, 0],
            back_spec[:, 0],
            grad_spec[:, 0],
            out_spec[:, 1],
            back_spec[:, 1],
            grad_spec[:, 1],
        ],
        axis=1,
    )


def unfold(series, cosine, sine_part):
    return tuple(
        (
            0.5
            * (
                series[0, signal_index]
                + cosine * series[0, signal_index + 3]
                - sine_part * series[1, signal_index + 3]
            )
            for signal_index in range(3)
        )
    )


def channel_local(mixed_in, gated_cot, filter_taps, devices):
    pieces = (
        lax.all_to_all(mixed_in, "seq", split_axis=1, concat_axis=0, tiled=True),
        lax.all_to_all(gated_cot, "seq", split_axis=1, concat_axis=0, tiled=True),
        lax.all_to_all(filter_taps, "seq", split_axis=1, concat_axis=0, tiled=True),
    )
    laid = jnp.transpose(jnp.stack(pieces), (0, 2, 1))
    seq_length = laid.shape[2]
    block = seq_length // devices
    angles = math.pi / seq_length * jnp.arange(seq_length).astype(jnp.float32)
    cosine = jnp.cos(angles)
    sine_row = jnp.sin(angles)
    spectrum = local_forward(modulated(laid, cosine, sine_row), devices, block)
    series = local_inverse(spectral_products(spectrum), devices, block)
    results = unfold(series, cosine, sine_row)
    return (
        lax.all_to_all(results[0].T, "seq", split_axis=0, concat_axis=1, tiled=True),
        lax.all_to_all(results[1].T, "seq", split_axis=0, concat_axis=1, tiled=True),
        lax.all_to_all(results[2].T, "seq", split_axis=0, concat_axis=1, tiled=True),
    )


def body(query_input, key_input, value_input, cotangent, filter_taps, skip_gain):
    devices = lax.axis_size("seq")
    row_count, channels = query_input.shape
    seq_length = row_count * devices
    query_val = query_input.astype(jnp.float32)
    key_val = key_input.astype(jnp.float32)
    value_val = value_input.astype(jnp.float32)
    cot_val = cotangent.astype(jnp.float32)
    mixed_in = key_val * value_val
    gated_cot = query_val * cot_val
    conv_out, back_conv, kernel_grad = channel_local(mixed_in, gated_cot, filter_taps, devices)
    inner_sum = conv_out + skip_gain[None, :] * mixed_in
    mixed_grad = back_conv + skip_gain[None, :] * gated_cot
    output = (query_val * inner_sum).astype(jnp.bfloat16)
    query_grad = (cot_val * inner_sum).astype(jnp.bfloat16)
    key_grad = (mixed_grad * value_val).astype(jnp.bfloat16)
    value_grad = (mixed_grad * key_val).astype(jnp.bfloat16)
    time_scale = 1.0 / math.sqrt(seq_length)
    filter_grad = kernel_grad * time_scale
    filter_sq = jnp.sum(filter_grad * filter_grad)
    skip_part = jnp.sum(gated_cot * mixed_in, axis=0) * time_scale
    skip_grad = lax.psum(skip_part, "seq")
    total_sq = lax.psum(filter_sq + jnp.sum(skip_grad * skip_grad) / devices, ("seq", "ch"))
    grad_rms = jnp.sqrt(total_sq / (channels * lax.axis_size("ch") * (seq_length + 1)))
    return (output, query_grad, key_grad, value_grad, filter_grad, skip_grad, grad_rms)


def split_high_low(array):
    high = array.astype(jnp.bfloat16)
    return high, (array - high.astype(jnp.float32)).astype(jnp.bfloat16)


def half_tables(points):
    odd = 2 * np.arange(points, dtype=np.int64) + 1
    angles = math.pi / (4 * points) * (odd[:, None] * odd[None, :] % (8 * points))
    parts = []
    for table in (np.cos(angles), np.sin(angles)):
        table = table.astype(np.float32)
        high = table.astype(jnp.bfloat16)
        parts += [high, (table - high.astype(np.float32)).astype(jnp.bfloat16)]
    shift = math.pi / (4 * points) * odd[:, None] * np.ones((1, LANES))
    return np.stack(parts), np.stack([np.cos(shift), np.sin(shift)]).astype(np.float32)


def kernel(
    devices, groups, count,
    k_hbm, v_hbm, q_hbm, c_hbm, h_hbm, skip_hbm, table_hbm, twist_hbm,
    out_ref, dq_ref, dk_ref, dv_ref, dh_ref, last_ref,
    gates, skip_ref, x_buf, g_buf, wide, flat,
    send, recv, spec, prod, back, home, extra,
    part_send, part_home, half_send, half_home, sq_acc, sq_send, sq_all, table, twist,
    load_sem, in_send, in_recv, out_send, home_recv, extra_recv, small_send, small_recv, ready,
):
    me = lax.axis_index("seq")
    mine = lax.axis_index("ch")
    rows, channels = q_hbm.shape
    half = rows // 2
    points = half * devices
    low = LANES // 2
    time_scale = 1.0 / math.sqrt(2 * points)
    blocks = channels // LANES
    side = devices // 2
    pair = devices // 4
    split = 3 * pair
    base = me // side * side
    other = side - base
    early = me < side
    late = me >= side
    near_here = me < pair
    whole_here = (me >= pair) & (me < side)
    far_two = (me >= side) & (me < split)
    far_one = me >= split

    barrier = pltpu.get_barrier_semaphore()
    for k in range(1, groups):
        pl.semaphore_signal(
            barrier, inc=1, device_id={"ch": lax.rem(mine + k, groups)}, device_id_type=MESH
        )

    @pl.when(me < split)
    def _():
        for k in range(1, devices):
            pl.semaphore_signal(
                barrier, inc=1, device_id={"seq": lax.rem(me + k, devices)}, device_id_type=MESH
            )

    @pl.when(far_one)
    def _():
        for k in range(1, pair):
            peer = split + lax.rem(me - split + k, pair)
            pl.semaphore_signal(barrier, inc=1, device_id={"seq": peer}, device_id_type=MESH)

    def columns_of(j):
        return pl.ds(j * LANES, LANES)

    for index, source in enumerate((k_hbm, v_hbm, q_hbm, c_hbm)):
        pltpu.make_async_copy(source, gates.at[index], load_sem.at[index // 2]).start()
    for j in range(blocks):
        pltpu.make_async_copy(h_hbm.at[:, columns_of(j)], wide.at[j], load_sem.at[2]).start()
    loads = (
        pltpu.make_async_copy(skip_hbm, skip_ref, load_sem.at[3]),
        pltpu.make_async_copy(table_hbm, table, load_sem.at[4]),
        pltpu.make_async_copy(twist_hbm, twist, load_sem.at[5]),
    )
    for load in loads:
        load.start()

    @pl.when(far_one)
    def _():
        pl.semaphore_wait(barrier, devices + groups - 2)
        for device in range(split):
            pl.semaphore_signal(
                ready, inc=1, device_id={"seq": jnp.int32(device)}, device_id_type=MESH
            )

    def gate(index, j):
        return gates[index, :, columns_of(j)].astype(jnp.float32)

    def wait_bytes(ref, sem):
        pltpu.make_async_copy(ref, ref, sem).wait()

    def near_owner(c):
        return (c % pair, c // pair)

    def far_owner(c):
        return (side + c, 0) if c < side else (c, 1)

    def whole_owner(c):
        return (c - side, 0)

    def give(signal, c, owner, can_be_me):
        device, slot = owner
        target = recv.at[(slot * 3 + signal) * devices + me]
        sem = in_recv.at[slot * 3 + signal]

        def remote():
            pltpu.make_async_remote_copy(
                src_ref=send.at[signal, c],
                dst_ref=target,
                send_sem=in_send.at[0],
                recv_sem=sem,
                device_id={"seq": jnp.int32(device)},
                device_id_type=MESH,
            ).start()

        if not can_be_me:
            remote()
            return

        pl.when(me != device)(remote)

        @pl.when(me == device)
        def _():
            pltpu.make_async_copy(send.at[signal, c], target, sem).start()

    def give_far(signal, chunks, can_be_me=False):
        for c in chunks:
            give(signal, c, far_owner(c), can_be_me)

    def give_whole(signal, can_be_me=False):
        for c in range(split, devices):
            give(signal, c, whole_owner(c), can_be_me)

    def give_near(signal, slot, can_be_me=False):
        for c in range(slot * pair, (slot + 1) * pair):
            give(signal, c, near_owner(c), can_be_me)

    def await_input(slot, signal, start, sources):
        first_one = (slot * 3 + signal) * devices + start
        wait_bytes(recv.at[pl.ds(first_one, sources)], in_recv.at[slot * 3 + signal])

    def to_home(slot, kind, c, dest):
        pltpu.make_async_remote_copy(
            src_ref=back.at[slot, kind, dest],
            dst_ref=home.at[kind, c],
            send_sem=out_send.at[0],
            recv_sem=home_recv.at[kind],
            device_id={"seq": dest},
            device_id_type=MESH,
        ).start()

    def to_extra(slot, kind, c, dest):
        pltpu.make_async_remote_copy(
            src_ref=back.at[slot, kind, dest],
            dst_ref=extra.at[kind, c],
            send_sem=out_send.at[0],
            recv_sem=extra_recv.at[kind],
            device_id={"seq": dest},
            device_id_type=MESH,
        ).start()

    def inward(slot, kind, c):
        for k in range(1, side):
            to_home(slot, kind, c, base + lax.rem(me - base + k, side))
        pltpu.make_async_copy(back.at[slot, kind, me], home.at[kind, c], home_recv.at[kind]).start()

    def small_copy(source, target, index, device_id):
        return pltpu.make_async_remote_copy(
            src_ref=source,
            dst_ref=target,
            send_sem=small_send.at[index],
            recv_sem=small_recv.at[index],
            device_id=device_id,
            device_id_type=MESH,
        )

    def share_part():
        wait_bytes(part_home.at[pl.ds(0, side - 1)], small_recv.at[0])
        part = part_home[base]
        for k in range(1, side):
            part = part + part_home[base + k]
        half_send[...] = part
        peer = lax.rem(me + side, devices)
        small_copy(half_send, half_home, 2, {"seq": peer}).start()

    def share_squares(squares):
        row = jnp.sum(squares, axis=0, keepdims=True)
        sq_send[0] = row
        sq_all[me * groups + mine] = row
        for k in range(devices):
            for n in range(groups):
                if k or n:
                    peer = {"seq": lax.rem(me + k, devices), "ch": lax.rem(mine + n, groups)}
                    small_copy(sq_send.at[0], sq_all.at[me * groups + mine], 1, peer).start()

    first = lax.broadcasted_iota(jnp.int32, (half, LANES), 1) < low

    def pack(source, signal):
        for j in range(blocks):
            even = source[j, pl.ds(0, half, stride=2), :]
            odd = source[j, pl.ds(1, half, stride=2), :]
            send[signal, 2 * j] = jnp.where(first, even, pltpu.roll(odd, low, 1))
            send[signal, 2 * j + 1] = jnp.where(first, pltpu.roll(even, low, 1), odd)

    wait_bytes(gates.at[pl.ds(0, 2)], load_sem.at[0])
    for j in range(blocks):
        x_buf[j] = gate(0, j) * gate(1, j)
    pack(x_buf, 0)
    @pl.when(me < split)
    def _():
        pl.semaphore_wait(barrier, split + groups - 2)

    to_two = (*range(pair), *range(side, split))
    to_one = range(pair, side)

    @pl.when(early)
    def _():
        give_far(0, to_two)

    @pl.when(near_here)
    def _():
        give_whole(0)
        for slot in range(3):
            give_near(0, slot, True)

    @pl.when(whole_here)
    def _():
        give_near(0, 0)
        give_whole(0, True)

    @pl.when(far_two)
    def _():
        give_whole(0)
        give_far(0, range(pair), True)

    @pl.when(far_one)
    def _():
        give_far(0, range(pair))

    wait_bytes(gates.at[pl.ds(2, 2)], load_sem.at[1])
    for j in range(blocks):
        g_buf[j] = gate(2, j) * gate(3, j)
    pack(g_buf, 1)

    @pl.when(near_here)
    def _():
        give_whole(1)
        for slot in range(3):
            give_near(1, slot, True)

    @pl.when(whole_here)
    def _():
        give_near(1, 0)
        give_whole(1, True)

    @pl.when(far_two)
    def _():
        give_whole(1)
        give_far(1, range(pair), True)
        for signal in (0, 1):
            give_far(signal, range(side, split), True)

    @pl.when(far_one)
    def _():
        give_far(1, range(pair))
        give_whole(0)
        give_whole(1)
        for signal in (0, 1):
            give_far(signal, to_one, True)
        for signal in (0, 1):
            give_far(signal, range(side, split))

    wait_bytes(wide, load_sem.at[2])
    pack(wide, 2)

    @pl.when(whole_here)
    def _():
        give_whole(2, True)

    @pl.when(far_two)
    def _():
        give_whole(2)

    @pl.when(me < split)
    def _():
        pl.semaphore_wait(ready, pair)

    @pl.when(early)
    def _():
        give_far(0, to_one)

    @pl.when(near_here)
    def _():
        give_far(2, range(split))
        give_whole(2)
        for slot in range(3):
            give_near(2, slot, True)

    @pl.when(whole_here)
    def _():
        for slot in (1, 2):
            for signal in (0, 1):
                give_near(signal, slot)
        for slot in range(3):
            give_near(2, slot)

    @pl.when(far_two)
    def _():
        for signal in (0, 1):
            give_far(signal, to_one)
        give_far(2, range(split), True)

    @pl.when(far_one)
    def _():
        give_whole(2)
        give_far(2, range(split), True)

    @pl.when(late)
    def _():
        extra[...] = jnp.zeros(extra.shape, jnp.float32)

    for j in range(blocks):
        part_send[pl.ds(j, 1), :] = jnp.sum(x_buf[j] * g_buf[j], axis=0, keepdims=True) * time_scale
    part_home[me] = part_send[...]
    for k in range(1, side):
        peer = base + lax.rem(me - base + k, side)
        small_copy(part_send, part_home.at[me], 0, {"seq": peer}).start()
    sq_acc[...] = jnp.zeros((8, LANES), jnp.float32)
    for load in loads:
        load.wait()

    def times(which, pieces, at_row, at_column):
        high, rest = pieces
        both = jnp.concatenate([high, rest], axis=1)
        main = jnp.dot(
            table[2 * which, at_row, at_column], both, preferred_element_type=jnp.float32
        )
        small = jnp.dot(
            table[2 * which + 1, at_row, at_column], high, preferred_element_type=jnp.float32
        )
        return main[:, :LANES] + (main[:, LANES:] + small)

    full = slice(0, points)
    early_part = slice(0, points // 2)
    late_part = slice(points // 2, points)

    def forward(slot, signal, part):
        start = (slot * 3 + signal) * devices + part.start // half
        sources = (part.stop - part.start) // half
        data = recv[pl.ds(start, sources)].reshape(sources * half, LANES)
        pieces = split_high_low(data)
        spec[slot, signal, 0] = times(0, pieces, full, part)
        spec[slot, signal, 1] = -times(1, pieces, full, part)

    def inverse(slot, kind, part, scale):
        series = times(0, split_high_low(prod[0]), part, full)
        series = series - times(1, split_high_low(prod[1]), part, full)
        series = series * (scale / points)
        start = part.start // half
        sources = (part.stop - part.start) // half
        back[slot, kind, start : start + sources] = series.reshape(sources, half, LANES)
        return series

    def square_sum(series):
        sq_acc[...] += jnp.sum((series * series).reshape(side * half // 8, 8, LANES), axis=0)

    step = 128

    def halves(slot, ref_row, part, at):
        value = spec[slot, ref_row, part, at, :]
        turned = pltpu.roll(value, low, 1)
        left = lax.broadcasted_iota(jnp.int32, (step, LANES), 1) < low
        return value, turned, jnp.where(left, value, turned), jnp.where(left, turned, value)

    def products(slot, signal, other_signal, conjugate):
        sign = jnp.where(lax.broadcasted_iota(jnp.int32, (step, LANES), 1) < low, 1.0, -1.0)

        @pl.loop(0, points // step)
        def _(index):
            at = pl.ds(pl.multiple_of(index * step, step), step)
            cosine = twist[0, at, :]
            sine = twist[1, at, :]
            signed = sine * sign
            _, _, even_re, odd_re = halves(slot, other_signal, 0, at)
            _, _, even_im, odd_im = halves(slot, other_signal, 1, at)
            a_re, as_re, _, _ = halves(slot, signal, 0, at)
            a_im, as_im, _, _ = halves(slot, signal, 1, at)
            p_re = even_re * cosine - even_im * sine
            p_im = even_im * cosine + even_re * sine
            if conjugate:
                r_re = odd_re * cosine - odd_im * signed
                r_im = odd_im * cosine + odd_re * signed
                prod[0, at, :] = a_re * p_re + a_im * p_im + (as_re * r_re + as_im * r_im)
                prod[1, at, :] = a_im * p_re - a_re * p_im + (as_im * r_re - as_re * r_im)
            else:
                r_re = odd_re * cosine + odd_im * signed
                r_im = odd_im * cosine - odd_re * signed
                prod[0, at, :] = a_re * p_re - a_im * p_im + (as_re * r_re - as_im * r_im)
                prod[1, at, :] = a_im * p_re + a_re * p_im + (as_im * r_re + as_re * r_im)

    @pl.when(near_here)
    def _():
        @pl.loop(0, 3)
        def _(slot):
            c = slot * pair + me
            for signal in (0, 1):
                await_input(slot, signal, 0, side)
                forward(slot, signal, early_part)
            products(slot, 1, 0, True)
            inverse(slot, 0, early_part, time_scale)
            inward(slot, 0, c)

        @pl.loop(0, 3)
        def _(slot):
            c = slot * pair + me
            await_input(slot, 2, 0, side)
            forward(slot, 2, early_part)
            products(slot, 1, 2, True)
            inverse(slot, 1, early_part, 1.0)
            inward(slot, 1, c)
            products(slot, 0, 2, False)
            inverse(slot, 2, early_part, 1.0)
            inward(slot, 2, c)

    def outward(slot, kind, c):
        @pl.when(whole_here)
        def _():
            for k in range(side):
                to_home(slot, kind, c, other + k)

        if kind < 2:
            @pl.when(late)
            def _():
                for k in range(side if kind == 0 else 1):
                    to_extra(slot, kind, c, other + k)

        inward(slot, kind, c)

    @pl.when(me >= pair)
    def _():
        zone = me // pair
        slots = 2 - lax.rem(zone, 2)

        @pl.when(late)
        def _():
            await_input(0, 1, side, side)

        @pl.loop(0, slots)
        def _(slot):
            c = lax.rem(me + side + side * slot, devices)

            @pl.when(late & (slot > 0))
            def _():
                await_input(slot, 1, side, side)

            @pl.when(late)
            def _():
                forward(slot, 1, late_part)

            await_input(slot, 0, 0, devices)

            forward(slot, 0, full)

            @pl.when(whole_here)
            def _():
                await_input(slot, 1, 0, devices)
                forward(slot, 1, full)
                give_far(2, range(split))

            products(slot, 1, 0, True)
            series = inverse(slot, 0, full, time_scale)
            outward(slot, 0, c)
            square_sum(series[points // 2 :])

        @pl.when(late)
        def _():
            share_part()
            share_squares(sq_acc[...])

        @pl.loop(0, slots)
        def _(slot):
            c = lax.rem(me + side + side * slot, devices)
            await_input(slot, 2, 0, devices)
            forward(slot, 2, full)
            products(slot, 1, 2, True)
            inverse(slot, 1, full, 1.0)
            outward(slot, 1, c)

        @pl.when(late)
        def _():
            @pl.loop(0, slots)
            def _(slot):
                c = lax.rem(me + side + side * slot, devices)
                for k in range(1, side):
                    to_extra(slot, 1, c, other + k)

        @pl.loop(0, slots)
        def _(slot):
            c = lax.rem(me + side + side * slot, devices)
            products(slot, 0, 2, False)
            inverse(slot, 2, full, 1.0)
            outward(slot, 2, c)

    def await_home(kind):
        wait_bytes(home.at[kind], home_recv.at[kind])
        if kind < 2:
            @pl.when(early)
            def _():
                wait_bytes(extra.at[kind], extra_recv.at[kind])

    def unpack(kind, j):
        pieces = []
        for c in (2 * j, 2 * j + 1):
            value = home[kind, c]
            pieces.append(value + extra[kind, c] if kind < 2 and c < split else value)
        left, right = pieces
        flat[j, pl.ds(0, half, stride=2), :] = jnp.where(first, left, pltpu.roll(right, low, 1))
        flat[j, pl.ds(1, half, stride=2), :] = jnp.where(first, pltpu.roll(left, low, 1), right)
        return flat[j]

    pl.when(early)(share_part)
    wait_bytes(half_home, small_recv.at[2])
    direct = half_send[...] + half_home[...]
    for j in range(blocks):
        last_ref[0:1, columns_of(j)] = direct[j : j + 1]

    await_home(0)
    squares = sq_acc[...]
    for j in range(blocks):
        squares = squares + direct[j : j + 1] * direct[j : j + 1] * (1.0 / (8 * side))
    for j in range(blocks):
        value = unpack(0, j)
        dh_ref[:, columns_of(j)] = value
        squares = squares + jnp.sum((value * value).reshape(rows // 8, 8, LANES), axis=0)

    @pl.when(early)
    def _():
        share_squares(squares)

    def assemble_inner():
        await_home(2)
        for j in range(blocks):
            at = columns_of(j)
            inner = unpack(2, j) + skip_ref[:, at] * x_buf[j]
            out_ref[:, at] = (gate(2, j) * inner).astype(jnp.bfloat16)
            dq_ref[:, at] = (gate(3, j) * inner).astype(jnp.bfloat16)

    def assemble_grad():
        await_home(1)
        for j in range(blocks):
            at = columns_of(j)
            grad = unpack(1, j) + skip_ref[:, at] * g_buf[j]
            dk_ref[:, at] = (grad * gate(1, j)).astype(jnp.bfloat16)
            dv_ref[:, at] = (grad * gate(0, j)).astype(jnp.bfloat16)

    everyone = devices * groups

    def finish_squares():
        wait_bytes(sq_all.at[pl.ds(0, everyone - 1)], small_recv.at[1])
        total = sq_all[0]
        for k in range(1, everyone):
            total = total + sq_all[k]
        total = jnp.sum(total, axis=1, keepdims=True)
        last_ref[1:2, :] = jnp.broadcast_to(jnp.sqrt(total / count), (1, channels))

    assemble_inner()
    pl.when(early)(finish_squares)
    assemble_grad()
    pl.when(late)(finish_squares)

    for condition, sent, returned in (
        (near_here, 3 * (split - 3) + 2 * split + 3 * pair, 9 * (side - 1)),
        (whole_here, 5 * split + 3 * (pair - 1), 3 * (devices - 1)),
        (far_two, 3 * (split - 2) + 3 * pair, 2 * (2 * side + 3 * (side - 1))),
        (far_one, 3 * (split - 1) + 3 * pair, 2 * side + 3 * (side - 1)),
    ):
        @pl.when(condition)
        def _():
            wait_bytes(recv.at[pl.ds(0, sent)], in_send.at[0])
            wait_bytes(recv.at[pl.ds(0, returned)], out_send.at[0])

    wait_bytes(part_home.at[pl.ds(0, side - 1)], small_send.at[0])
    wait_bytes(half_home, small_send.at[2])
    wait_bytes(sq_all.at[pl.ds(0, everyone - 1)], small_send.at[1])


def emit(*refs):
    sources, last_ref, targets = refs[:5], refs[5], refs[6:13]
    skip_row, rms_value, sem = refs[13:]
    sources = (*sources, skip_row, rms_value)
    copies = [
        pltpu.make_async_copy(source, target, sem.at[index])
        for index, (source, target) in enumerate(zip(sources, targets))
    ]
    for copy in copies[:5]:
        copy.start()
    skip_row[...] = last_ref[0:1, :]
    rms_value[...] = last_ref[1:2, 0:1]
    for copy in copies[5:]:
        copy.start()
    for copy in copies:
        copy.wait()


def fused_body(query_input, key_input, value_input, cotangent, filter_taps, skip_gain):
    devices = lax.axis_size("seq")
    groups = lax.axis_size("ch")
    rows, channels = query_input.shape
    half = rows // 2
    points = half * devices
    tables, twists = half_tables(points)
    count = float(channels * groups * (rows * devices + 1))
    vmem = pl.BlockSpec(memory_space=pltpu.VMEM)
    hbm = pl.BlockSpec(memory_space=pltpu.HBM)
    chunks = 2 * channels // LANES
    blocks = channels // LANES
    shapes = [((rows, channels), jnp.bfloat16)] * 4 + [
        ((rows, channels), jnp.float32),
        ((1, channels), jnp.float32),
        ((1, 1), jnp.float32),
    ]
    held = pl.pallas_call(
        functools.partial(kernel, devices, groups, count),
        out_shape=tuple(
            pltpu.VMEM(*shape) for shape in (*shapes[:5], ((2, channels), jnp.float32))
        ),
        in_specs=[hbm] * 8,
        out_specs=(vmem,) * 6,
        scratch_shapes=[
            pltpu.VMEM((4, rows, channels), jnp.bfloat16),
            pltpu.VMEM((1, channels), jnp.float32),
            pltpu.VMEM((blocks, rows, LANES), jnp.float32),
            pltpu.VMEM((blocks, rows, LANES), jnp.float32),
            pltpu.VMEM((blocks, rows, LANES), jnp.float32),
            pltpu.VMEM((blocks, rows, LANES), jnp.float32),
            pltpu.VMEM((3, chunks, half, LANES), jnp.float32),
            pltpu.VMEM((9 * devices, half, LANES), jnp.float32),
            pltpu.VMEM((3, 3, 2, points, LANES), jnp.float32),
            pltpu.VMEM((2, points, LANES), jnp.float32),
            pltpu.VMEM((3, 3, devices, half, LANES), jnp.float32),
            pltpu.VMEM((3, chunks, half, LANES), jnp.float32),
            pltpu.VMEM((2, 3 * (devices // 4), half, LANES), jnp.float32),
            pltpu.VMEM((blocks, LANES), jnp.float32),
            pltpu.VMEM((devices, blocks, LANES), jnp.float32),
            pltpu.VMEM((blocks, LANES), jnp.float32),
            pltpu.VMEM((blocks, LANES), jnp.float32),
            pltpu.VMEM((8, LANES), jnp.float32),
            pltpu.VMEM((1, 1, LANES), jnp.float32),
            pltpu.VMEM((devices * groups, 1, LANES), jnp.float32),
            pltpu.VMEM(tables.shape, jnp.bfloat16),
            pltpu.VMEM(twists.shape, jnp.float32),
            pltpu.SemaphoreType.DMA((6,)),
            pltpu.SemaphoreType.DMA((1,)),
            pltpu.SemaphoreType.DMA((9,)),
            pltpu.SemaphoreType.DMA((1,)),
            pltpu.SemaphoreType.DMA((3,)),
            pltpu.SemaphoreType.DMA((2,)),
            pltpu.SemaphoreType.DMA((3,)),
            pltpu.SemaphoreType.DMA((3,)),
            pltpu.SemaphoreType.REGULAR,
        ],
        compiler_params=pltpu.CompilerParams(
            collective_id=0, has_side_effects=True, vmem_limit_bytes=(64 << 20) - (960 << 10)
        ),
    )(
        key_input, value_input, query_input, cotangent, filter_taps,
        skip_gain.reshape(1, channels), jnp.asarray(tables), jnp.asarray(twists),
    )
    results = pl.pallas_call(
        emit,
        out_shape=tuple(jax.ShapeDtypeStruct(*shape) for shape in shapes),
        in_specs=[vmem] * 6,
        out_specs=(hbm,) * 7,
        scratch_shapes=[
            pltpu.VMEM((1, channels), jnp.float32),
            pltpu.VMEM((1, 1), jnp.float32),
            pltpu.SemaphoreType.DMA((7,)),
        ],
        compiler_params=pltpu.CompilerParams(vmem_limit_bytes=4 << 20),
    )(*held)
    return (*results[:5], results[5].reshape(channels), results[6].reshape(()))


def pick_body(query_input, *others):
    devices = lax.axis_size("seq")
    rows, channels = query_input.shape
    fits = devices == 8 and 2 * channels == LANES * devices and rows % 16 == 0
    chosen = fused_body if fits and rows * devices <= 2048 else body
    return chosen(query_input, *others)


def solution(mesh):
    return jax.shard_map(
        pick_body,
        mesh=mesh,
        in_specs=(
            P("seq", "ch"),
            P("seq", "ch"),
            P("seq", "ch"),
            P("seq", "ch"),
            P("seq", "ch"),
            P("ch"),
        ),
        out_specs=(
            P("seq", "ch"),
            P("seq", "ch"),
            P("seq", "ch"),
            P("seq", "ch"),
            P("seq", "ch"),
            P("ch"),
            P(),
        ),
        check_vma=False,
    )
```

```python
import functools
import math

import jax
import jax.numpy as jnp
import numpy as np
from jax import lax
from jax.experimental import pallas as pl
from jax.experimental.pallas import tpu as pltpu
from jax.sharding import PartitionSpec as P

LANES = 128
MESH = pl.DeviceIdType.MESH


def complex_mul(left_op, right_op):
    return jnp.stack(
        [
            left_op[0] * right_op[0] - left_op[1] * right_op[1],
            left_op[0] * right_op[1] + left_op[1] * right_op[0],
        ]
    )


def conj_of(stacked):
    return jnp.stack([stacked[0], -stacked[1]])


def dft_table(length, direction):
    counter = jnp.arange(length)
    angles = (
        2.0 * math.pi / length * (counter[:, None] * counter[None, :] % length).astype(jnp.float32)
    )
    return (jnp.cos(angles), direction * jnp.sin(angles))


def dft_along(stacked, length, direction, pattern):
    table_re, table_im = dft_table(length, direction)

    def contract(table, part_in):
        return jnp.einsum(pattern, table, part_in, precision=lax.Precision.HIGHEST)

    real_out = contract(table_re, stacked[0]) - contract(table_im, stacked[1])
    imag_out = contract(table_re, stacked[1]) + contract(table_im, stacked[0])
    return jnp.stack([real_out, imag_out])


def grid_twiddle(devices, block, direction):
    seq_length = devices * block
    counter = jnp.arange(devices)[:, None] * jnp.arange(block)[None, :] % seq_length
    angles = direction * 2.0 * math.pi / seq_length * counter.astype(jnp.float32)
    return jnp.stack([jnp.cos(angles), jnp.sin(angles)])[:, None, None]


def local_forward(stacked, devices, block):
    array_shape = stacked.shape
    stacked = stacked.reshape(array_shape[0], array_shape[1], array_shape[2], devices, block)
    stacked = dft_along(stacked, devices, -1.0, "kj,scjp->sckp")
    stacked = complex_mul(stacked, grid_twiddle(devices, block, -1.0))
    return dft_along(stacked, block, -1.0, "kp,scjp->scjk")


def local_inverse(stacked, devices, block):
    stacked = dft_along(stacked, block, 1.0, "kp,scjp->scjk")
    stacked = complex_mul(stacked, grid_twiddle(devices, block, 1.0))
    stacked = dft_along(stacked, devices, 1.0, "kj,scjp->sckp")
    array_shape = stacked.shape
    return stacked.reshape(array_shape[0], array_shape[1], array_shape[2], devices * block) / (
        devices * block
    )


def modulated(signals, cosine, sine_part):
    zero_part = jnp.zeros_like(signals)
    return jnp.stack(
        [
            jnp.concatenate([signals, signals * cosine]),
            jnp.concatenate([zero_part, -signals * sine_part]),
        ]
    )


def spectral_products(spectrum):
    mixed_spec = spectrum[:, 0::3]
    gated_spec = spectrum[:, 1::3]
    taps_spec = spectrum[:, 2::3]
    out_spec = complex_mul(mixed_spec, taps_spec)
    back_spec = complex_mul(gated_spec, conj_of(taps_spec))
    grad_spec = complex_mul(gated_spec, conj_of(mixed_spec))
    return jnp.stack(
        [
            out_spec[:, 0],
            back_spec[:, 0],
            grad_spec[:, 0],
            out_spec[:, 1],
            back_spec[:, 1],
            grad_spec[:, 1],
        ],
        axis=1,
    )


def unfold(series, cosine, sine_part):
    return tuple(
        (
            0.5
            * (
                series[0, signal_index]
                + cosine * series[0, signal_index + 3]
                - sine_part * series[1, signal_index + 3]
            )
            for signal_index in range(3)
        )
    )


def channel_local(mixed_in, gated_cot, filter_taps, devices):
    pieces = (
        lax.all_to_all(mixed_in, "seq", split_axis=1, concat_axis=0, tiled=True),
        lax.all_to_all(gated_cot, "seq", split_axis=1, concat_axis=0, tiled=True),
        lax.all_to_all(filter_taps, "seq", split_axis=1, concat_axis=0, tiled=True),
    )
    laid = jnp.transpose(jnp.stack(pieces), (0, 2, 1))
    seq_length = laid.shape[2]
    block = seq_length // devices
    angles = math.pi / seq_length * jnp.arange(seq_length).astype(jnp.float32)
    cosine = jnp.cos(angles)
    sine_row = jnp.sin(angles)
    spectrum = local_forward(modulated(laid, cosine, sine_row), devices, block)
    series = local_inverse(spectral_products(spectrum), devices, block)
    results = unfold(series, cosine, sine_row)
    return (
        lax.all_to_all(results[0].T, "seq", split_axis=0, concat_axis=1, tiled=True),
        lax.all_to_all(results[1].T, "seq", split_axis=0, concat_axis=1, tiled=True),
        lax.all_to_all(results[2].T, "seq", split_axis=0, concat_axis=1, tiled=True),
    )


def body(query_input, key_input, value_input, cotangent, filter_taps, skip_gain):
    devices = lax.axis_size("seq")
    row_count, channels = query_input.shape
    seq_length = row_count * devices
    query_val = query_input.astype(jnp.float32)
    key_val = key_input.astype(jnp.float32)
    value_val = value_input.astype(jnp.float32)
    cot_val = cotangent.astype(jnp.float32)
    mixed_in = key_val * value_val
    gated_cot = query_val * cot_val
    conv_out, back_conv, kernel_grad = channel_local(mixed_in, gated_cot, filter_taps, devices)
    inner_sum = conv_out + skip_gain[None, :] * mixed_in
    mixed_grad = back_conv + skip_gain[None, :] * gated_cot
    output = (query_val * inner_sum).astype(jnp.bfloat16)
    query_grad = (cot_val * inner_sum).astype(jnp.bfloat16)
    key_grad = (mixed_grad * value_val).astype(jnp.bfloat16)
    value_grad = (mixed_grad * key_val).astype(jnp.bfloat16)
    time_scale = 1.0 / math.sqrt(seq_length)
    filter_grad = kernel_grad * time_scale
    filter_sq = jnp.sum(filter_grad * filter_grad)
    skip_part = jnp.sum(gated_cot * mixed_in, axis=0) * time_scale
    skip_grad = lax.psum(skip_part, "seq")
    total_sq = lax.psum(filter_sq + jnp.sum(skip_grad * skip_grad) / devices, ("seq", "ch"))
    grad_rms = jnp.sqrt(total_sq / (channels * lax.axis_size("ch") * (seq_length + 1)))
    return (output, query_grad, key_grad, value_grad, filter_grad, skip_grad, grad_rms)


def split_high_low(array):
    high = array.astype(jnp.bfloat16)
    return high, (array - high.astype(jnp.float32)).astype(jnp.bfloat16)


def half_tables(points):
    odd = 2 * np.arange(points, dtype=np.int64) + 1
    angles = math.pi / (4 * points) * (odd[:, None] * odd[None, :] % (8 * points))
    parts = []
    for table in (np.cos(angles), np.sin(angles)):
        table = table.astype(np.float32)
        high = table.astype(jnp.bfloat16)
        parts += [high, (table - high.astype(np.float32)).astype(jnp.bfloat16)]
    shift = math.pi / (4 * points) * odd[:, None] * np.ones((1, LANES))
    return np.stack(parts), np.stack([np.cos(shift), np.sin(shift)]).astype(np.float32)


def kernel(
    devices, groups, count,
    k_hbm, v_hbm, q_hbm, c_hbm, h_hbm, skip_hbm, table_hbm, twist_hbm,
    out_ref, dq_ref, dk_ref, dv_ref, dh_ref, last_ref,
    gates, skip_ref, x_buf, g_buf, wide, flat,
    send, recv, spec, prod, back, home, extra,
    part_send, part_home, half_send, half_home, sq_acc, sq_send, sq_all, table, twist,
    load_sem, in_send, in_recv, out_send, home_recv, extra_recv, small_send, small_recv, ready,
):
    me = lax.axis_index("seq")
    mine = lax.axis_index("ch")
    rows, channels = q_hbm.shape
    half = rows // 2
    points = half * devices
    low = LANES // 2
    time_scale = 1.0 / math.sqrt(2 * points)
    blocks = channels // LANES
    side = devices // 2
    pair = devices // 4
    split = 3 * pair
    base = me // side * side
    other = side - base
    early = me < side
    late = me >= side
    near_here = me < pair
    whole_here = (me >= pair) & (me < side)
    far_two = (me >= side) & (me < split)
    far_one = me >= split

    barrier = pltpu.get_barrier_semaphore()
    for k in range(1, groups):
        pl.semaphore_signal(
            barrier, inc=1, device_id={"ch": lax.rem(mine + k, groups)}, device_id_type=MESH
        )

    @pl.when(me < split)
    def _():
        for k in range(1, devices):
            pl.semaphore_signal(
                barrier, inc=1, device_id={"seq": lax.rem(me + k, devices)}, device_id_type=MESH
            )

    @pl.when(far_one)
    def _():
        for k in range(1, pair):
            peer = split + lax.rem(me - split + k, pair)
            pl.semaphore_signal(barrier, inc=1, device_id={"seq": peer}, device_id_type=MESH)

    def columns_of(j):
        return pl.ds(j * LANES, LANES)

    for index, source in enumerate((k_hbm, v_hbm, q_hbm, c_hbm)):
        pltpu.make_async_copy(source, gates.at[index], load_sem.at[index // 2]).start()
    for j in range(blocks):
        pltpu.make_async_copy(h_hbm.at[:, columns_of(j)], wide.at[j], load_sem.at[2]).start()
    loads = (
        pltpu.make_async_copy(skip_hbm, skip_ref, load_sem.at[3]),
        pltpu.make_async_copy(table_hbm, table, load_sem.at[4]),
        pltpu.make_async_copy(twist_hbm, twist, load_sem.at[5]),
    )
    for load in loads:
        load.start()

    @pl.when(far_one)
    def _():
        pl.semaphore_wait(barrier, devices + groups - 2)
        for device in range(split):
            pl.semaphore_signal(
                ready, inc=1, device_id={"seq": jnp.int32(device)}, device_id_type=MESH
            )

    def gate(index, j):
        return gates[index, :, columns_of(j)].astype(jnp.float32)

    def wait_bytes(ref, sem):
        pltpu.make_async_copy(ref, ref, sem).wait()

    def near_owner(c):
        return (c % pair, c // pair)

    def far_owner(c):
        return (side + c, 0) if c < side else (c, 1)

    def whole_owner(c):
        return (c - side, 0)

    def give(signal, c, owner, can_be_me):
        device, slot = owner
        target = recv.at[(slot * 3 + signal) * devices + me]
        sem = in_recv.at[slot * 3 + signal]

        def remote():
            pltpu.make_async_remote_copy(
                src_ref=send.at[signal, c],
                dst_ref=target,
                send_sem=in_send.at[0],
                recv_sem=sem,
                device_id={"seq": jnp.int32(device)},
                device_id_type=MESH,
            ).start()

        if not can_be_me:
            remote()
            return

        pl.when(me != device)(remote)

        @pl.when(me == device)
        def _():
            pltpu.make_async_copy(send.at[signal, c], target, sem).start()

    def give_far(signal, chunks, can_be_me=False):
        for c in chunks:
            give(signal, c, far_owner(c), can_be_me)

    def give_whole(signal, can_be_me=False):
        for c in range(split, devices):
            give(signal, c, whole_owner(c), can_be_me)

    def give_near(signal, slot, can_be_me=False):
        for c in range(slot * pair, (slot + 1) * pair):
            give(signal, c, near_owner(c), can_be_me)

    def await_input(slot, signal, start, sources):
        first_one = (slot * 3 + signal) * devices + start
        wait_bytes(recv.at[pl.ds(first_one, sources)], in_recv.at[slot * 3 + signal])

    def to_home(slot, kind, c, dest):
        pltpu.make_async_remote_copy(
            src_ref=back.at[slot, kind, dest],
            dst_ref=home.at[kind, c],
            send_sem=out_send.at[0],
            recv_sem=home_recv.at[kind],
            device_id={"seq": dest},
            device_id_type=MESH,
        ).start()

    def to_extra(slot, kind, c, dest):
        pltpu.make_async_remote_copy(
            src_ref=back.at[slot, kind, dest],
            dst_ref=extra.at[kind, c],
            send_sem=out_send.at[0],
            recv_sem=extra_recv.at[kind],
            device_id={"seq": dest},
            device_id_type=MESH,
        ).start()

    def inward(slot, kind, c):
        for k in range(1, side):
            to_home(slot, kind, c, base + lax.rem(me - base + k, side))
        pltpu.make_async_copy(back.at[slot, kind, me], home.at[kind, c], home_recv.at[kind]).start()

    def small_copy(source, target, index, device_id):
        return pltpu.make_async_remote_copy(
            src_ref=source,
            dst_ref=target,
            send_sem=small_send.at[index],
            recv_sem=small_recv.at[index],
            device_id=device_id,
            device_id_type=MESH,
        )

    def share_part():
        wait_bytes(part_home.at[pl.ds(0, side - 1)], small_recv.at[0])
        part = part_home[base]
        for k in range(1, side):
            part = part + part_home[base + k]
        half_send[...] = part
        peer = lax.rem(me + side, devices)
        small_copy(half_send, half_home, 2, {"seq": peer}).start()

    def share_squares(squares):
        row = jnp.sum(squares, axis=0, keepdims=True)
        sq_send[0] = row
        sq_all[me * groups + mine] = row
        for k in range(devices):
            for n in range(groups):
                if k or n:
                    peer = {"seq": lax.rem(me + k, devices), "ch": lax.rem(mine + n, groups)}
                    small_copy(sq_send.at[0], sq_all.at[me * groups + mine], 1, peer).start()

    first = lax.broadcasted_iota(jnp.int32, (half, LANES), 1) < low

    def pack(source, signal):
        for j in range(blocks):
            even = source[j, pl.ds(0, half, stride=2), :]
            odd = source[j, pl.ds(1, half, stride=2), :]
            send[signal, 2 * j] = jnp.where(first, even, pltpu.roll(odd, low, 1))
            send[signal, 2 * j + 1] = jnp.where(first, pltpu.roll(even, low, 1), odd)

    wait_bytes(gates.at[pl.ds(0, 2)], load_sem.at[0])
    for j in range(blocks):
        x_buf[j] = gate(0, j) * gate(1, j)
    pack(x_buf, 0)
    @pl.when(me < split)
    def _():
        pl.semaphore_wait(barrier, split + groups - 2)

    to_two = (*range(pair), *range(side, split))
    to_one = range(pair, side)

    @pl.when(early)
    def _():
        give_far(0, to_two)

    @pl.when(near_here)
    def _():
        give_whole(0)
        for slot in range(3):
            give_near(0, slot, True)

    @pl.when(whole_here)
    def _():
        give_near(0, 0)
        give_whole(0, True)

    @pl.when(far_two)
    def _():
        give_whole(0)
        give_far(0, range(pair), True)

    @pl.when(far_one)
    def _():
        give_far(0, range(pair))

    wait_bytes(gates.at[pl.ds(2, 2)], load_sem.at[1])
    for j in range(blocks):
        g_buf[j] = gate(2, j) * gate(3, j)
    pack(g_buf, 1)

    @pl.when(near_here)
    def _():
        give_whole(1)
        for slot in range(3):
            give_near(1, slot, True)

    @pl.when(whole_here)
    def _():
        give_near(1, 0)
        give_whole(1, True)

    @pl.when(far_two)
    def _():
        give_whole(1)
        give_far(1, range(pair), True)
        for signal in (0, 1):
            give_far(signal, range(side, split), True)

    @pl.when(far_one)
    def _():
        give_far(1, range(pair))
        give_whole(0)
        give_whole(1)
        for signal in (0, 1):
            give_far(signal, to_one, True)
        for signal in (0, 1):
            give_far(signal, range(side, split))

    wait_bytes(wide, load_sem.at[2])
    pack(wide, 2)

    @pl.when(whole_here)
    def _():
        give_whole(2, True)

    @pl.when(far_two)
    def _():
        give_whole(2)

    @pl.when(me < split)
    def _():
        pl.semaphore_wait(ready, pair)

    @pl.when(early)
    def _():
        give_far(0, to_one)

    @pl.when(near_here)
    def _():
        give_far(2, range(split))
        give_whole(2)
        for slot in range(3):
            give_near(2, slot, True)

    @pl.when(whole_here)
    def _():
        for slot in (1, 2):
            for signal in (0, 1):
                give_near(signal, slot)
        for slot in range(3):
            give_near(2, slot)

    @pl.when(far_two)
    def _():
        for signal in (0, 1):
            give_far(signal, to_one)
        give_far(2, range(split), True)

    @pl.when(far_one)
    def _():
        give_whole(2)
        give_far(2, range(split), True)

    @pl.when(late)
    def _():
        extra[...] = jnp.zeros(extra.shape, jnp.float32)

    for j in range(blocks):
        part_send[pl.ds(j, 1), :] = jnp.sum(x_buf[j] * g_buf[j], axis=0, keepdims=True) * time_scale
    part_home[me] = part_send[...]
    for k in range(1, side):
        peer = base + lax.rem(me - base + k, side)
        small_copy(part_send, part_home.at[me], 0, {"seq": peer}).start()
    sq_acc[...] = jnp.zeros((8, LANES), jnp.float32)
    for load in loads:
        load.wait()

    def times(which, pieces, at_row, at_column):
        high, rest = pieces
        both = jnp.concatenate([high, rest], axis=1)
        main = jnp.dot(
            table[2 * which, at_row, at_column], both, preferred_element_type=jnp.float32
        )
        small = jnp.dot(
            table[2 * which + 1, at_row, at_column], high, preferred_element_type=jnp.float32
        )
        return main[:, :LANES] + (main[:, LANES:] + small)

    full = slice(0, points)
    early_part = slice(0, points // 2)
    late_part = slice(points // 2, points)

    def forward(slot, signal, part):
        start = (slot * 3 + signal) * devices + part.start // half
        sources = (part.stop - part.start) // half
        data = recv[pl.ds(start, sources)].reshape(sources * half, LANES)
        pieces = split_high_low(data)
        spec[slot, signal, 0] = times(0, pieces, full, part)
        spec[slot, signal, 1] = -times(1, pieces, full, part)

    def inverse(slot, kind, part, scale):
        series = times(0, split_high_low(prod[0]), part, full)
        series = series - times(1, split_high_low(prod[1]), part, full)
        series = series * (scale / points)
        start = part.start // half
        sources = (part.stop - part.start) // half
        back[slot, kind, start : start + sources] = series.reshape(sources, half, LANES)
        return series

    def square_sum(series):
        sq_acc[...] += jnp.sum((series * series).reshape(side * half // 8, 8, LANES), axis=0)

    step = 128

    def halves(slot, ref_row, part, at):
        value = spec[slot, ref_row, part, at, :]
        turned = pltpu.roll(value, low, 1)
        left = lax.broadcasted_iota(jnp.int32, (step, LANES), 1) < low
        return value, turned, jnp.where(left, value, turned), jnp.where(left, turned, value)

    def products(slot, signal, other_signal, conjugate):
        sign = jnp.where(lax.broadcasted_iota(jnp.int32, (step, LANES), 1) < low, 1.0, -1.0)

        @pl.loop(0, points // step)
        def _(index):
            at = pl.ds(pl.multiple_of(index * step, step), step)
            cosine = twist[0, at, :]
            sine = twist[1, at, :]
            signed = sine * sign
            _, _, even_re, odd_re = halves(slot, other_signal, 0, at)
            _, _, even_im, odd_im = halves(slot, other_signal, 1, at)
            a_re, as_re, _, _ = halves(slot, signal, 0, at)
            a_im, as_im, _, _ = halves(slot, signal, 1, at)
            p_re = even_re * cosine - even_im * sine
            p_im = even_im * cosine + even_re * sine
            if conjugate:
                r_re = odd_re * cosine - odd_im * signed
                r_im = odd_im * cosine + odd_re * signed
                prod[0, at, :] = a_re * p_re + a_im * p_im + (as_re * r_re + as_im * r_im)
                prod[1, at, :] = a_im * p_re - a_re * p_im + (as_im * r_re - as_re * r_im)
            else:
                r_re = odd_re * cosine + odd_im * signed
                r_im = odd_im * cosine - odd_re * signed
                prod[0, at, :] = a_re * p_re - a_im * p_im + (as_re * r_re - as_im * r_im)
                prod[1, at, :] = a_im * p_re + a_re * p_im + (as_im * r_re + as_re * r_im)

    @pl.when(near_here)
    def _():
        @pl.loop(0, 3)
        def _(slot):
            c = slot * pair + me
            for signal in (0, 1):
                await_input(slot, signal, 0, side)
                forward(slot, signal, early_part)
            products(slot, 1, 0, True)
            inverse(slot, 0, early_part, time_scale)
            inward(slot, 0, c)

        @pl.loop(0, 3)
        def _(slot):
            c = slot * pair + me
            await_input(slot, 2, 0, side)
            forward(slot, 2, early_part)
            products(slot, 1, 2, True)
            inverse(slot, 1, early_part, 1.0)
            inward(slot, 1, c)
            products(slot, 0, 2, False)
            inverse(slot, 2, early_part, 1.0)
            inward(slot, 2, c)

    def outward(slot, kind, c):
        if kind < 2:
            @pl.when(late)
            def _():
                for k in range(side if kind == 0 else 1):
                    to_extra(slot, kind, c, other + k)

        inward(slot, kind, c)

        @pl.when(whole_here)
        def _():
            for k in range(side):
                to_home(slot, kind, c, other + k)

    @pl.when(me >= pair)
    def _():
        zone = me // pair
        slots = 2 - lax.rem(zone, 2)

        @pl.when(late)
        def _():
            await_input(0, 1, side, side)

        @pl.loop(0, slots)
        def _(slot):
            c = lax.rem(me + side + side * slot, devices)

            @pl.when(late & (slot > 0))
            def _():
                await_input(slot, 1, side, side)

            @pl.when(late)
            def _():
                forward(slot, 1, late_part)

            await_input(slot, 0, 0, devices)

            forward(slot, 0, full)

            @pl.when(whole_here)
            def _():
                await_input(slot, 1, 0, devices)
                forward(slot, 1, full)
                give_far(2, range(split))

            products(slot, 1, 0, True)
            series = inverse(slot, 0, full, time_scale)
            outward(slot, 0, c)
            square_sum(series[points // 2 :])

        @pl.when(late)
        def _():
            share_part()
            share_squares(sq_acc[...])

        @pl.loop(0, slots)
        def _(slot):
            c = lax.rem(me + side + side * slot, devices)
            await_input(slot, 2, 0, devices)
            forward(slot, 2, full)
            products(slot, 1, 2, True)
            inverse(slot, 1, full, 1.0)
            outward(slot, 1, c)

        @pl.when(late)
        def _():
            @pl.loop(0, slots)
            def _(slot):
                c = lax.rem(me + side + side * slot, devices)
                for k in range(1, side):
                    to_extra(slot, 1, c, other + k)

        @pl.loop(0, slots)
        def _(slot):
            c = lax.rem(me + side + side * slot, devices)
            products(slot, 0, 2, False)
            inverse(slot, 2, full, 1.0)
            outward(slot, 2, c)

    def await_home(kind):
        wait_bytes(home.at[kind], home_recv.at[kind])
        if kind < 2:
            @pl.when(early)
            def _():
                wait_bytes(extra.at[kind], extra_recv.at[kind])

    def unpack(kind, j):
        pieces = []
        for c in (2 * j, 2 * j + 1):
            value = home[kind, c]
            pieces.append(value + extra[kind, c] if kind < 2 and c < split else value)
        left, right = pieces
        flat[j, pl.ds(0, half, stride=2), :] = jnp.where(first, left, pltpu.roll(right, low, 1))
        flat[j, pl.ds(1, half, stride=2), :] = jnp.where(first, pltpu.roll(left, low, 1), right)
        return flat[j]

    pl.when(early)(share_part)
    wait_bytes(half_home, small_recv.at[2])
    direct = half_send[...] + half_home[...]
    for j in range(blocks):
        last_ref[0:1, columns_of(j)] = direct[j : j + 1]

    await_home(0)
    squares = sq_acc[...]
    for j in range(blocks):
        squares = squares + direct[j : j + 1] * direct[j : j + 1] * (1.0 / (8 * side))
    for j in range(blocks):
        value = unpack(0, j)
        dh_ref[:, columns_of(j)] = value
        squares = squares + jnp.sum((value * value).reshape(rows // 8, 8, LANES), axis=0)

    @pl.when(early)
    def _():
        share_squares(squares)

    def assemble_inner():
        await_home(2)
        for j in range(blocks):
            at = columns_of(j)
            inner = unpack(2, j) + skip_ref[:, at] * x_buf[j]
            out_ref[:, at] = (gate(2, j) * inner).astype(jnp.bfloat16)
            dq_ref[:, at] = (gate(3, j) * inner).astype(jnp.bfloat16)

    def assemble_grad():
        await_home(1)
        for j in range(blocks):
            at = columns_of(j)
            grad = unpack(1, j) + skip_ref[:, at] * g_buf[j]
            dk_ref[:, at] = (grad * gate(1, j)).astype(jnp.bfloat16)
            dv_ref[:, at] = (grad * gate(0, j)).astype(jnp.bfloat16)

    everyone = devices * groups

    def finish_squares():
        wait_bytes(sq_all.at[pl.ds(0, everyone - 1)], small_recv.at[1])
        total = sq_all[0]
        for k in range(1, everyone):
            total = total + sq_all[k]
        total = jnp.sum(total, axis=1, keepdims=True)
        last_ref[1:2, :] = jnp.broadcast_to(jnp.sqrt(total / count), (1, channels))

    assemble_inner()
    pl.when(early)(finish_squares)
    assemble_grad()
    pl.when(late)(finish_squares)

    for condition, sent, returned in (
        (near_here, 3 * (split - 3) + 2 * split + 3 * pair, 9 * (side - 1)),
        (whole_here, 5 * split + 3 * (pair - 1), 3 * (devices - 1)),
        (far_two, 3 * (split - 2) + 3 * pair, 2 * (2 * side + 3 * (side - 1))),
        (far_one, 3 * (split - 1) + 3 * pair, 2 * side + 3 * (side - 1)),
    ):
        @pl.when(condition)
        def _():
            wait_bytes(recv.at[pl.ds(0, sent)], in_send.at[0])
            wait_bytes(recv.at[pl.ds(0, returned)], out_send.at[0])

    wait_bytes(part_home.at[pl.ds(0, side - 1)], small_send.at[0])
    wait_bytes(half_home, small_send.at[2])
    wait_bytes(sq_all.at[pl.ds(0, everyone - 1)], small_send.at[1])


def emit(*refs):
    sources, last_ref, targets = refs[:5], refs[5], refs[6:13]
    skip_row, rms_value, sem = refs[13:]
    sources = (*sources, skip_row, rms_value)
    copies = [
        pltpu.make_async_copy(source, target, sem.at[index])
        for index, (source, target) in enumerate(zip(sources, targets))
    ]
    for copy in copies[:5]:
        copy.start()
    skip_row[...] = last_ref[0:1, :]
    rms_value[...] = last_ref[1:2, 0:1]
    for copy in copies[5:]:
        copy.start()
    for copy in copies:
        copy.wait()


def fused_body(query_input, key_input, value_input, cotangent, filter_taps, skip_gain):
    devices = lax.axis_size("seq")
    groups = lax.axis_size("ch")
    rows, channels = query_input.shape
    half = rows // 2
    points = half * devices
    tables, twists = half_tables(points)
    count = float(channels * groups * (rows * devices + 1))
    vmem = pl.BlockSpec(memory_space=pltpu.VMEM)
    hbm = pl.BlockSpec(memory_space=pltpu.HBM)
    chunks = 2 * channels // LANES
    blocks = channels // LANES
    shapes = [((rows, channels), jnp.bfloat16)] * 4 + [
        ((rows, channels), jnp.float32),
        ((1, channels), jnp.float32),
        ((1, 1), jnp.float32),
    ]
    held = pl.pallas_call(
        functools.partial(kernel, devices, groups, count),
        out_shape=tuple(
            pltpu.VMEM(*shape) for shape in (*shapes[:5], ((2, channels), jnp.float32))
        ),
        in_specs=[hbm] * 8,
        out_specs=(vmem,) * 6,
        scratch_shapes=[
            pltpu.VMEM((4, rows, channels), jnp.bfloat16),
            pltpu.VMEM((1, channels), jnp.float32),
            pltpu.VMEM((blocks, rows, LANES), jnp.float32),
            pltpu.VMEM((blocks, rows, LANES), jnp.float32),
            pltpu.VMEM((blocks, rows, LANES), jnp.float32),
            pltpu.VMEM((blocks, rows, LANES), jnp.float32),
            pltpu.VMEM((3, chunks, half, LANES), jnp.float32),
            pltpu.VMEM((9 * devices, half, LANES), jnp.float32),
            pltpu.VMEM((3, 3, 2, points, LANES), jnp.float32),
            pltpu.VMEM((2, points, LANES), jnp.float32),
            pltpu.VMEM((3, 3, devices, half, LANES), jnp.float32),
            pltpu.VMEM((3, chunks, half, LANES), jnp.float32),
            pltpu.VMEM((2, 3 * (devices // 4), half, LANES), jnp.float32),
            pltpu.VMEM((blocks, LANES), jnp.float32),
            pltpu.VMEM((devices, blocks, LANES), jnp.float32),
            pltpu.VMEM((blocks, LANES), jnp.float32),
            pltpu.VMEM((blocks, LANES), jnp.float32),
            pltpu.VMEM((8, LANES), jnp.float32),
            pltpu.VMEM((1, 1, LANES), jnp.float32),
            pltpu.VMEM((devices * groups, 1, LANES), jnp.float32),
            pltpu.VMEM(tables.shape, jnp.bfloat16),
            pltpu.VMEM(twists.shape, jnp.float32),
            pltpu.SemaphoreType.DMA((6,)),
            pltpu.SemaphoreType.DMA((1,)),
            pltpu.SemaphoreType.DMA((9,)),
            pltpu.SemaphoreType.DMA((1,)),
            pltpu.SemaphoreType.DMA((3,)),
            pltpu.SemaphoreType.DMA((2,)),
            pltpu.SemaphoreType.DMA((3,)),
            pltpu.SemaphoreType.DMA((3,)),
            pltpu.SemaphoreType.REGULAR,
        ],
        compiler_params=pltpu.CompilerParams(
            collective_id=0, has_side_effects=True, vmem_limit_bytes=(64 << 20) - (960 << 10)
        ),
    )(
        key_input, value_input, query_input, cotangent, filter_taps,
        skip_gain.reshape(1, channels), jnp.asarray(tables), jnp.asarray(twists),
    )
    results = pl.pallas_call(
        emit,
        out_shape=tuple(jax.ShapeDtypeStruct(*shape) for shape in shapes),
        in_specs=[vmem] * 6,
        out_specs=(hbm,) * 7,
        scratch_shapes=[
            pltpu.VMEM((1, channels), jnp.float32),
            pltpu.VMEM((1, 1), jnp.float32),
            pltpu.SemaphoreType.DMA((7,)),
        ],
        compiler_params=pltpu.CompilerParams(vmem_limit_bytes=4 << 20),
    )(*held)
    return (*results[:5], results[5].reshape(channels), results[6].reshape(()))


def pick_body(query_input, *others):
    devices = lax.axis_size("seq")
    rows, channels = query_input.shape
    fits = devices == 8 and 2 * channels == LANES * devices and rows % 16 == 0
    chosen = fused_body if fits and rows * devices <= 2048 else body
    return chosen(query_input, *others)


def solution(mesh):
    return jax.shard_map(
        pick_body,
        mesh=mesh,
        in_specs=(
            P("seq", "ch"),
            P("seq", "ch"),
            P("seq", "ch"),
            P("seq", "ch"),
            P("seq", "ch"),
            P("ch"),
        ),
        out_specs=(
            P("seq", "ch"),
            P("seq", "ch"),
            P("seq", "ch"),
            P("seq", "ch"),
            P("seq", "ch"),
            P("ch"),
            P(),
        ),
        check_vma=False,
    )
```

```python
import functools
import math

import jax
import jax.numpy as jnp
import numpy as np
from jax import lax
from jax.experimental import pallas as pl
from jax.experimental.pallas import tpu as pltpu
from jax.sharding import PartitionSpec as P

LANES = 128
MESH = pl.DeviceIdType.MESH


def complex_mul(left_op, right_op):
    return jnp.stack(
        [
            left_op[0] * right_op[0] - left_op[1] * right_op[1],
            left_op[0] * right_op[1] + left_op[1] * right_op[0],
        ]
    )


def conj_of(stacked):
    return jnp.stack([stacked[0], -stacked[1]])


def dft_table(length, direction):
    counter = jnp.arange(length)
    angles = (
        2.0 * math.pi / length * (counter[:, None] * counter[None, :] % length).astype(jnp.float32)
    )
    return (jnp.cos(angles), direction * jnp.sin(angles))


def dft_along(stacked, length, direction, pattern):
    table_re, table_im = dft_table(length, direction)

    def contract(table, part_in):
        return jnp.einsum(pattern, table, part_in, precision=lax.Precision.HIGHEST)

    real_out = contract(table_re, stacked[0]) - contract(table_im, stacked[1])
    imag_out = contract(table_re, stacked[1]) + contract(table_im, stacked[0])
    return jnp.stack([real_out, imag_out])


def grid_twiddle(devices, block, direction):
    seq_length = devices * block
    counter = jnp.arange(devices)[:, None] * jnp.arange(block)[None, :] % seq_length
    angles = direction * 2.0 * math.pi / seq_length * counter.astype(jnp.float32)
    return jnp.stack([jnp.cos(angles), jnp.sin(angles)])[:, None, None]


def local_forward(stacked, devices, block):
    array_shape = stacked.shape
    stacked = stacked.reshape(array_shape[0], array_shape[1], array_shape[2], devices, block)
    stacked = dft_along(stacked, devices, -1.0, "kj,scjp->sckp")
    stacked = complex_mul(stacked, grid_twiddle(devices, block, -1.0))
    return dft_along(stacked, block, -1.0, "kp,scjp->scjk")


def local_inverse(stacked, devices, block):
    stacked = dft_along(stacked, block, 1.0, "kp,scjp->scjk")
    stacked = complex_mul(stacked, grid_twiddle(devices, block, 1.0))
    stacked = dft_along(stacked, devices, 1.0, "kj,scjp->sckp")
    array_shape = stacked.shape
    return stacked.reshape(array_shape[0], array_shape[1], array_shape[2], devices * block) / (
        devices * block
    )


def modulated(signals, cosine, sine_part):
    zero_part = jnp.zeros_like(signals)
    return jnp.stack(
        [
            jnp.concatenate([signals, signals * cosine]),
            jnp.concatenate([zero_part, -signals * sine_part]),
        ]
    )


def spectral_products(spectrum):
    mixed_spec = spectrum[:, 0::3]
    gated_spec = spectrum[:, 1::3]
    taps_spec = spectrum[:, 2::3]
    out_spec = complex_mul(mixed_spec, taps_spec)
    back_spec = complex_mul(gated_spec, conj_of(taps_spec))
    grad_spec = complex_mul(gated_spec, conj_of(mixed_spec))
    return jnp.stack(
        [
            out_spec[:, 0],
            back_spec[:, 0],
            grad_spec[:, 0],
            out_spec[:, 1],
            back_spec[:, 1],
            grad_spec[:, 1],
        ],
        axis=1,
    )


def unfold(series, cosine, sine_part):
    return tuple(
        (
            0.5
            * (
                series[0, signal_index]
                + cosine * series[0, signal_index + 3]
                - sine_part * series[1, signal_index + 3]
            )
            for signal_index in range(3)
        )
    )


def channel_local(mixed_in, gated_cot, filter_taps, devices):
    pieces = (
        lax.all_to_all(mixed_in, "seq", split_axis=1, concat_axis=0, tiled=True),
        lax.all_to_all(gated_cot, "seq", split_axis=1, concat_axis=0, tiled=True),
        lax.all_to_all(filter_taps, "seq", split_axis=1, concat_axis=0, tiled=True),
    )
    laid = jnp.transpose(jnp.stack(pieces), (0, 2, 1))
    seq_length = laid.shape[2]
    block = seq_length // devices
    angles = math.pi / seq_length * jnp.arange(seq_length).astype(jnp.float32)
    cosine = jnp.cos(angles)
    sine_row = jnp.sin(angles)
    spectrum = local_forward(modulated(laid, cosine, sine_row), devices, block)
    series = local_inverse(spectral_products(spectrum), devices, block)
    results = unfold(series, cosine, sine_row)
    return (
        lax.all_to_all(results[0].T, "seq", split_axis=0, concat_axis=1, tiled=True),
        lax.all_to_all(results[1].T, "seq", split_axis=0, concat_axis=1, tiled=True),
        lax.all_to_all(results[2].T, "seq", split_axis=0, concat_axis=1, tiled=True),
    )


def body(query_input, key_input, value_input, cotangent, filter_taps, skip_gain):
    devices = lax.axis_size("seq")
    row_count, channels = query_input.shape
    seq_length = row_count * devices
    query_val = query_input.astype(jnp.float32)
    key_val = key_input.astype(jnp.float32)
    value_val = value_input.astype(jnp.float32)
    cot_val = cotangent.astype(jnp.float32)
    mixed_in = key_val * value_val
    gated_cot = query_val * cot_val
    conv_out, back_conv, kernel_grad = channel_local(mixed_in, gated_cot, filter_taps, devices)
    inner_sum = conv_out + skip_gain[None, :] * mixed_in
    mixed_grad = back_conv + skip_gain[None, :] * gated_cot
    output = (query_val * inner_sum).astype(jnp.bfloat16)
    query_grad = (cot_val * inner_sum).astype(jnp.bfloat16)
    key_grad = (mixed_grad * value_val).astype(jnp.bfloat16)
    value_grad = (mixed_grad * key_val).astype(jnp.bfloat16)
    time_scale = 1.0 / math.sqrt(seq_length)
    filter_grad = kernel_grad * time_scale
    filter_sq = jnp.sum(filter_grad * filter_grad)
    skip_part = jnp.sum(gated_cot * mixed_in, axis=0) * time_scale
    skip_grad = lax.psum(skip_part, "seq")
    total_sq = lax.psum(filter_sq + jnp.sum(skip_grad * skip_grad) / devices, ("seq", "ch"))
    grad_rms = jnp.sqrt(total_sq / (channels * lax.axis_size("ch") * (seq_length + 1)))
    return (output, query_grad, key_grad, value_grad, filter_grad, skip_grad, grad_rms)


def split_high_low(array):
    high = array.astype(jnp.bfloat16)
    return high, (array - high.astype(jnp.float32)).astype(jnp.bfloat16)


def half_tables(points):
    odd = 2 * np.arange(points, dtype=np.int64) + 1
    angles = math.pi / (4 * points) * (odd[:, None] * odd[None, :] % (8 * points))
    parts = []
    for table in (np.cos(angles), np.sin(angles)):
        table = table.astype(np.float32)
        high = table.astype(jnp.bfloat16)
        parts += [high, (table - high.astype(np.float32)).astype(jnp.bfloat16)]
    shift = math.pi / (4 * points) * odd[:, None] * np.ones((1, LANES))
    return np.stack(parts), np.stack([np.cos(shift), np.sin(shift)]).astype(np.float32)


def kernel(
    devices, groups, count,
    k_hbm, v_hbm, q_hbm, c_hbm, h_hbm, skip_hbm, table_hbm, twist_hbm,
    out_ref, dq_ref, dk_ref, dv_ref, dh_ref, last_ref,
    gates, skip_ref, x_buf, g_buf, wide, flat,
    send, recv, spec, prod, back, home, extra,
    part_send, part_home, half_send, half_home, sq_acc, sq_send, sq_all, table, twist,
    load_sem, in_send, in_recv, out_send, home_recv, extra_recv, small_send, small_recv, ready,
):
    me = lax.axis_index("seq")
    mine = lax.axis_index("ch")
    rows, channels = q_hbm.shape
    half = rows // 2
    points = half * devices
    low = LANES // 2
    time_scale = 1.0 / math.sqrt(2 * points)
    blocks = channels // LANES
    side = devices // 2
    pair = devices // 4
    split = 3 * pair
    base = me // side * side
    other = side - base
    early = me < side
    late = me >= side
    near_here = me < pair
    whole_here = (me >= pair) & (me < side)
    far_two = (me >= side) & (me < split)
    far_one = me >= split

    barrier = pltpu.get_barrier_semaphore()
    for k in range(1, groups):
        pl.semaphore_signal(
            barrier, inc=1, device_id={"ch": lax.rem(mine + k, groups)}, device_id_type=MESH
        )

    @pl.when(me < split)
    def _():
        for k in range(1, devices):
            pl.semaphore_signal(
                barrier, inc=1, device_id={"seq": lax.rem(me + k, devices)}, device_id_type=MESH
            )

    @pl.when(far_one)
    def _():
        for k in range(1, pair):
            peer = split + lax.rem(me - split + k, pair)
            pl.semaphore_signal(barrier, inc=1, device_id={"seq": peer}, device_id_type=MESH)

    def columns_of(j):
        return pl.ds(j * LANES, LANES)

    for index, source in enumerate((k_hbm, v_hbm, q_hbm, c_hbm)):
        pltpu.make_async_copy(source, gates.at[index], load_sem.at[index // 2]).start()
    for j in range(blocks):
        pltpu.make_async_copy(h_hbm.at[:, columns_of(j)], wide.at[j], load_sem.at[2]).start()
    loads = (
        pltpu.make_async_copy(skip_hbm, skip_ref, load_sem.at[3]),
        pltpu.make_async_copy(table_hbm, table, load_sem.at[4]),
        pltpu.make_async_copy(twist_hbm, twist, load_sem.at[5]),
    )
    for load in loads:
        load.start()

    @pl.when(far_one)
    def _():
        pl.semaphore_wait(barrier, devices + groups - 2)
        for device in range(split):
            pl.semaphore_signal(
                ready, inc=1, device_id={"seq": jnp.int32(device)}, device_id_type=MESH
            )

    def gate(index, j):
        return gates[index, :, columns_of(j)].astype(jnp.float32)

    def wait_bytes(ref, sem):
        pltpu.make_async_copy(ref, ref, sem).wait()

    def near_owner(c):
        return (c % pair, c // pair)

    def far_owner(c):
        return (side + c, 0) if c < side else (c, 1)

    def whole_owner(c):
        return (c - side, 0)

    def give(signal, c, owner, can_be_me):
        device, slot = owner
        target = recv.at[(slot * 3 + signal) * devices + me]
        sem = in_recv.at[slot * 3 + signal]

        def remote():
            pltpu.make_async_remote_copy(
                src_ref=send.at[signal, c],
                dst_ref=target,
                send_sem=in_send.at[0],
                recv_sem=sem,
                device_id={"seq": jnp.int32(device)},
                device_id_type=MESH,
            ).start()

        if not can_be_me:
            remote()
            return

        pl.when(me != device)(remote)

        @pl.when(me == device)
        def _():
            pltpu.make_async_copy(send.at[signal, c], target, sem).start()

    def give_far(signal, chunks, can_be_me=False):
        for c in chunks:
            give(signal, c, far_owner(c), can_be_me)

    def give_whole(signal, can_be_me=False):
        for c in range(split, devices):
            give(signal, c, whole_owner(c), can_be_me)

    def give_near(signal, slot, can_be_me=False):
        for c in range(slot * pair, (slot + 1) * pair):
            give(signal, c, near_owner(c), can_be_me)

    def await_input(slot, signal, start, sources):
        first_one = (slot * 3 + signal) * devices + start
        wait_bytes(recv.at[pl.ds(first_one, sources)], in_recv.at[slot * 3 + signal])

    def to_home(slot, kind, c, dest):
        pltpu.make_async_remote_copy(
            src_ref=back.at[slot, kind, dest],
            dst_ref=home.at[kind, c],
            send_sem=out_send.at[0],
            recv_sem=home_recv.at[kind],
            device_id={"seq": dest},
            device_id_type=MESH,
        ).start()

    def to_extra(slot, kind, c, dest):
        pltpu.make_async_remote_copy(
            src_ref=back.at[slot, kind, dest],
            dst_ref=extra.at[kind, c],
            send_sem=out_send.at[0],
            recv_sem=extra_recv.at[kind],
            device_id={"seq": dest},
            device_id_type=MESH,
        ).start()

    def inward(slot, kind, c):
        for k in range(1, side):
            to_home(slot, kind, c, base + lax.rem(me - base + k, side))
        pltpu.make_async_copy(back.at[slot, kind, me], home.at[kind, c], home_recv.at[kind]).start()

    def small_copy(source, target, index, device_id):
        return pltpu.make_async_remote_copy(
            src_ref=source,
            dst_ref=target,
            send_sem=small_send.at[index],
            recv_sem=small_recv.at[index],
            device_id=device_id,
            device_id_type=MESH,
        )

    def share_part():
        wait_bytes(part_home.at[pl.ds(0, side - 1)], small_recv.at[0])
        part = part_home[base]
        for k in range(1, side):
            part = part + part_home[base + k]
        half_send[...] = part
        peer = lax.rem(me + side, devices)
        small_copy(half_send, half_home, 2, {"seq": peer}).start()

    def share_squares(squares):
        row = jnp.sum(squares, axis=0, keepdims=True)
        sq_send[0] = row
        sq_all[me * groups + mine] = row
        for k in range(devices):
            for n in range(groups):
                if k or n:
                    peer = {"seq": lax.rem(me + k, devices), "ch": lax.rem(mine + n, groups)}
                    small_copy(sq_send.at[0], sq_all.at[me * groups + mine], 1, peer).start()

    first = lax.broadcasted_iota(jnp.int32, (half, LANES), 1) < low

    def pack(source, signal):
        for j in range(blocks):
            even = source[j, pl.ds(0, half, stride=2), :]
            odd = source[j, pl.ds(1, half, stride=2), :]
            send[signal, 2 * j] = jnp.where(first, even, pltpu.roll(odd, low, 1))
            send[signal, 2 * j + 1] = jnp.where(first, pltpu.roll(even, low, 1), odd)

    wait_bytes(gates.at[pl.ds(0, 2)], load_sem.at[0])
    for j in range(blocks):
        x_buf[j] = gate(0, j) * gate(1, j)
    pack(x_buf, 0)
    @pl.when(me < split)
    def _():
        pl.semaphore_wait(barrier, split + groups - 2)

    to_two = (*range(pair), *range(side, split))
    to_one = range(pair, side)

    @pl.when(early)
    def _():
        give_far(0, to_two)

    @pl.when(near_here)
    def _():
        give_whole(0)
        for slot in range(3):
            give_near(0, slot, True)

    @pl.when(whole_here)
    def _():
        give_near(0, 0)
        give_whole(0, True)

    @pl.when(far_two)
    def _():
        give_whole(0)
        give_far(0, range(pair), True)

    @pl.when(far_one)
    def _():
        give_far(0, range(pair))

    wait_bytes(gates.at[pl.ds(2, 2)], load_sem.at[1])
    for j in range(blocks):
        g_buf[j] = gate(2, j) * gate(3, j)
    pack(g_buf, 1)

    @pl.when(near_here)
    def _():
        give_whole(1)
        for slot in range(3):
            give_near(1, slot, True)

    @pl.when(whole_here)
    def _():
        give_near(1, 0)
        give_whole(1, True)
        for slot in (1, 2):
            for signal in (0, 1):
                give_near(signal, slot)

    @pl.when(far_two)
    def _():
        give_whole(1)
        give_far(1, range(pair), True)
        for signal in (0, 1):
            give_far(signal, range(side, split), True)

    @pl.when(far_one)
    def _():
        give_far(1, range(pair))
        give_whole(0)
        give_whole(1)
        for signal in (0, 1):
            give_far(signal, to_one, True)
        for signal in (0, 1):
            give_far(signal, range(side, split))

    wait_bytes(wide, load_sem.at[2])
    pack(wide, 2)

    @pl.when(whole_here)
    def _():
        give_whole(2, True)

    @pl.when(far_two)
    def _():
        give_whole(2)

    @pl.when(me < split)
    def _():
        pl.semaphore_wait(ready, pair)

    @pl.when(early)
    def _():
        give_far(0, to_one)

    @pl.when(near_here)
    def _():
        give_far(2, range(split))
        give_whole(2)
        for slot in range(3):
            give_near(2, slot, True)

    @pl.when(whole_here)
    def _():
        for slot in range(3):
            give_near(2, slot)

    @pl.when(far_two)
    def _():
        for signal in (0, 1):
            give_far(signal, to_one)
        give_far(2, range(split), True)

    @pl.when(far_one)
    def _():
        give_whole(2)
        give_far(2, range(split), True)

    @pl.when(late)
    def _():
        extra[...] = jnp.zeros(extra.shape, jnp.float32)

    for j in range(blocks):
        part_send[pl.ds(j, 1), :] = jnp.sum(x_buf[j] * g_buf[j], axis=0, keepdims=True) * time_scale
    part_home[me] = part_send[...]
    for k in range(1, side):
        peer = base + lax.rem(me - base + k, side)
        small_copy(part_send, part_home.at[me], 0, {"seq": peer}).start()
    sq_acc[...] = jnp.zeros((8, LANES), jnp.float32)
    for load in loads:
        load.wait()

    def times(which, pieces, at_row, at_column):
        high, rest = pieces
        both = jnp.concatenate([high, rest], axis=1)
        main = jnp.dot(
            table[2 * which, at_row, at_column], both, preferred_element_type=jnp.float32
        )
        small = jnp.dot(
            table[2 * which + 1, at_row, at_column], high, preferred_element_type=jnp.float32
        )
        return main[:, :LANES] + (main[:, LANES:] + small)

    full = slice(0, points)
    early_part = slice(0, points // 2)
    late_part = slice(points // 2, points)

    def forward(slot, signal, part):
        start = (slot * 3 + signal) * devices + part.start // half
        sources = (part.stop - part.start) // half
        data = recv[pl.ds(start, sources)].reshape(sources * half, LANES)
        pieces = split_high_low(data)
        spec[slot, signal, 0] = times(0, pieces, full, part)
        spec[slot, signal, 1] = -times(1, pieces, full, part)

    def inverse(slot, kind, part, scale):
        series = times(0, split_high_low(prod[0]), part, full)
        series = series - times(1, split_high_low(prod[1]), part, full)
        series = series * (scale / points)
        start = part.start // half
        sources = (part.stop - part.start) // half
        back[slot, kind, start : start + sources] = series.reshape(sources, half, LANES)
        return series

    def square_sum(series):
        sq_acc[...] += jnp.sum((series * series).reshape(side * half // 8, 8, LANES), axis=0)

    step = 128

    def halves(slot, ref_row, part, at):
        value = spec[slot, ref_row, part, at, :]
        turned = pltpu.roll(value, low, 1)
        left = lax.broadcasted_iota(jnp.int32, (step, LANES), 1) < low
        return value, turned, jnp.where(left, value, turned), jnp.where(left, turned, value)

    def products(slot, signal, other_signal, conjugate):
        sign = jnp.where(lax.broadcasted_iota(jnp.int32, (step, LANES), 1) < low, 1.0, -1.0)

        @pl.loop(0, points // step)
        def _(index):
            at = pl.ds(pl.multiple_of(index * step, step), step)
            cosine = twist[0, at, :]
            sine = twist[1, at, :]
            signed = sine * sign
            _, _, even_re, odd_re = halves(slot, other_signal, 0, at)
            _, _, even_im, odd_im = halves(slot, other_signal, 1, at)
            a_re, as_re, _, _ = halves(slot, signal, 0, at)
            a_im, as_im, _, _ = halves(slot, signal, 1, at)
            p_re = even_re * cosine - even_im * sine
            p_im = even_im * cosine + even_re * sine
            if conjugate:
                r_re = odd_re * cosine - odd_im * signed
                r_im = odd_im * cosine + odd_re * signed
                prod[0, at, :] = a_re * p_re + a_im * p_im + (as_re * r_re + as_im * r_im)
                prod[1, at, :] = a_im * p_re - a_re * p_im + (as_im * r_re - as_re * r_im)
            else:
                r_re = odd_re * cosine + odd_im * signed
                r_im = odd_im * cosine - odd_re * signed
                prod[0, at, :] = a_re * p_re - a_im * p_im + (as_re * r_re - as_im * r_im)
                prod[1, at, :] = a_im * p_re + a_re * p_im + (as_im * r_re + as_re * r_im)

    @pl.when(near_here)
    def _():
        @pl.loop(0, 3)
        def _(slot):
            c = slot * pair + me
            for signal in (0, 1):
                await_input(slot, signal, 0, side)
                forward(slot, signal, early_part)
            products(slot, 1, 0, True)
            inverse(slot, 0, early_part, time_scale)
            inward(slot, 0, c)

        @pl.loop(0, 3)
        def _(slot):
            c = slot * pair + me
            await_input(slot, 2, 0, side)
            forward(slot, 2, early_part)
            products(slot, 1, 2, True)
            inverse(slot, 1, early_part, 1.0)
            inward(slot, 1, c)
            products(slot, 0, 2, False)
            inverse(slot, 2, early_part, 1.0)
            inward(slot, 2, c)

    def outward(slot, kind, c):
        @pl.when(whole_here)
        def _():
            for k in range(side):
                to_home(slot, kind, c, other + k)

        if kind < 2:
            @pl.when(late)
            def _():
                for k in range(side if kind == 0 else 1):
                    to_extra(slot, kind, c, other + k)

        inward(slot, kind, c)

    @pl.when(me >= pair)
    def _():
        zone = me // pair
        slots = 2 - lax.rem(zone, 2)

        @pl.when(late)
        def _():
            await_input(0, 1, side, side)

        @pl.loop(0, slots)
        def _(slot):
            c = lax.rem(me + side + side * slot, devices)

            @pl.when(late & (slot > 0))
            def _():
                await_input(slot, 1, side, side)

            @pl.when(late)
            def _():
                forward(slot, 1, late_part)

            await_input(slot, 0, 0, devices)

            forward(slot, 0, full)

            @pl.when(whole_here)
            def _():
                await_input(slot, 1, 0, devices)
                forward(slot, 1, full)
                give_far(2, range(split))

            products(slot, 1, 0, True)
            series = inverse(slot, 0, full, time_scale)
            outward(slot, 0, c)
            square_sum(series[points // 2 :])

        @pl.when(late)
        def _():
            share_part()
            share_squares(sq_acc[...])

        @pl.loop(0, slots)
        def _(slot):
            c = lax.rem(me + side + side * slot, devices)
            await_input(slot, 2, 0, devices)
            forward(slot, 2, full)
            products(slot, 1, 2, True)
            inverse(slot, 1, full, 1.0)
            outward(slot, 1, c)

        @pl.when(late)
        def _():
            @pl.loop(0, slots)
            def _(slot):
                c = lax.rem(me + side + side * slot, devices)
                for k in range(1, side):
                    to_extra(slot, 1, c, other + k)

        @pl.loop(0, slots)
        def _(slot):
            c = lax.rem(me + side + side * slot, devices)
            products(slot, 0, 2, False)
            inverse(slot, 2, full, 1.0)
            outward(slot, 2, c)

    def await_home(kind):
        wait_bytes(home.at[kind], home_recv.at[kind])
        if kind < 2:
            @pl.when(early)
            def _():
                wait_bytes(extra.at[kind], extra_recv.at[kind])

    def unpack(kind, j):
        pieces = []
        for c in (2 * j, 2 * j + 1):
            value = home[kind, c]
            pieces.append(value + extra[kind, c] if kind < 2 and c < split else value)
        left, right = pieces
        flat[j, pl.ds(0, half, stride=2), :] = jnp.where(first, left, pltpu.roll(right, low, 1))
        flat[j, pl.ds(1, half, stride=2), :] = jnp.where(first, pltpu.roll(left, low, 1), right)
        return flat[j]

    pl.when(early)(share_part)
    wait_bytes(half_home, small_recv.at[2])
    direct = half_send[...] + half_home[...]
    for j in range(blocks):
        last_ref[0:1, columns_of(j)] = direct[j : j + 1]

    await_home(0)
    squares = sq_acc[...]
    for j in range(blocks):
        squares = squares + direct[j : j + 1] * direct[j : j + 1] * (1.0 / (8 * side))
    for j in range(blocks):
        value = unpack(0, j)
        dh_ref[:, columns_of(j)] = value
        squares = squares + jnp.sum((value * value).reshape(rows // 8, 8, LANES), axis=0)

    @pl.when(early)
    def _():
        share_squares(squares)

    def assemble_inner():
        await_home(2)
        for j in range(blocks):
            at = columns_of(j)
            inner = unpack(2, j) + skip_ref[:, at] * x_buf[j]
            out_ref[:, at] = (gate(2, j) * inner).astype(jnp.bfloat16)
            dq_ref[:, at] = (gate(3, j) * inner).astype(jnp.bfloat16)

    def assemble_grad():
        await_home(1)
        for j in range(blocks):
            at = columns_of(j)
            grad = unpack(1, j) + skip_ref[:, at] * g_buf[j]
            dk_ref[:, at] = (grad * gate(1, j)).astype(jnp.bfloat16)
            dv_ref[:, at] = (grad * gate(0, j)).astype(jnp.bfloat16)

    everyone = devices * groups

    def finish_squares():
        wait_bytes(sq_all.at[pl.ds(0, everyone - 1)], small_recv.at[1])
        total = sq_all[0]
        for k in range(1, everyone):
            total = total + sq_all[k]
        total = jnp.sum(total, axis=1, keepdims=True)
        last_ref[1:2, :] = jnp.broadcast_to(jnp.sqrt(total / count), (1, channels))

    assemble_inner()
    pl.when(early)(finish_squares)
    assemble_grad()
    pl.when(late)(finish_squares)

    for condition, sent, returned in (
        (near_here, 3 * (split - 3) + 2 * split + 3 * pair, 9 * (side - 1)),
        (whole_here, 5 * split + 3 * (pair - 1), 3 * (devices - 1)),
        (far_two, 3 * (split - 2) + 3 * pair, 2 * (2 * side + 3 * (side - 1))),
        (far_one, 3 * (split - 1) + 3 * pair, 2 * side + 3 * (side - 1)),
    ):
        @pl.when(condition)
        def _():
            wait_bytes(recv.at[pl.ds(0, sent)], in_send.at[0])
            wait_bytes(recv.at[pl.ds(0, returned)], out_send.at[0])

    wait_bytes(part_home.at[pl.ds(0, side - 1)], small_send.at[0])
    wait_bytes(half_home, small_send.at[2])
    wait_bytes(sq_all.at[pl.ds(0, everyone - 1)], small_send.at[1])


def emit(*refs):
    sources, last_ref, targets = refs[:5], refs[5], refs[6:13]
    skip_row, rms_value, sem = refs[13:]
    sources = (*sources, skip_row, rms_value)
    copies = [
        pltpu.make_async_copy(source, target, sem.at[index])
        for index, (source, target) in enumerate(zip(sources, targets))
    ]
    for copy in copies[:5]:
        copy.start()
    skip_row[...] = last_ref[0:1, :]
    rms_value[...] = last_ref[1:2, 0:1]
    for copy in copies[5:]:
        copy.start()
    for copy in copies:
        copy.wait()


def fused_body(query_input, key_input, value_input, cotangent, filter_taps, skip_gain):
    devices = lax.axis_size("seq")
    groups = lax.axis_size("ch")
    rows, channels = query_input.shape
    half = rows // 2
    points = half * devices
    tables, twists = half_tables(points)
    count = float(channels * groups * (rows * devices + 1))
    vmem = pl.BlockSpec(memory_space=pltpu.VMEM)
    hbm = pl.BlockSpec(memory_space=pltpu.HBM)
    chunks = 2 * channels // LANES
    blocks = channels // LANES
    shapes = [((rows, channels), jnp.bfloat16)] * 4 + [
        ((rows, channels), jnp.float32),
        ((1, channels), jnp.float32),
        ((1, 1), jnp.float32),
    ]
    held = pl.pallas_call(
        functools.partial(kernel, devices, groups, count),
        out_shape=tuple(
            pltpu.VMEM(*shape) for shape in (*shapes[:5], ((2, channels), jnp.float32))
        ),
        in_specs=[hbm] * 8,
        out_specs=(vmem,) * 6,
        scratch_shapes=[
            pltpu.VMEM((4, rows, channels), jnp.bfloat16),
            pltpu.VMEM((1, channels), jnp.float32),
            pltpu.VMEM((blocks, rows, LANES), jnp.float32),
            pltpu.VMEM((blocks, rows, LANES), jnp.float32),
            pltpu.VMEM((blocks, rows, LANES), jnp.float32),
            pltpu.VMEM((blocks, rows, LANES), jnp.float32),
            pltpu.VMEM((3, chunks, half, LANES), jnp.float32),
            pltpu.VMEM((9 * devices, half, LANES), jnp.float32),
            pltpu.VMEM((3, 3, 2, points, LANES), jnp.float32),
            pltpu.VMEM((2, points, LANES), jnp.float32),
            pltpu.VMEM((3, 3, devices, half, LANES), jnp.float32),
            pltpu.VMEM((3, chunks, half, LANES), jnp.float32),
            pltpu.VMEM((2, 3 * (devices // 4), half, LANES), jnp.float32),
            pltpu.VMEM((blocks, LANES), jnp.float32),
            pltpu.VMEM((devices, blocks, LANES), jnp.float32),
            pltpu.VMEM((blocks, LANES), jnp.float32),
            pltpu.VMEM((blocks, LANES), jnp.float32),
            pltpu.VMEM((8, LANES), jnp.float32),
            pltpu.VMEM((1, 1, LANES), jnp.float32),
            pltpu.VMEM((devices * groups, 1, LANES), jnp.float32),
            pltpu.VMEM(tables.shape, jnp.bfloat16),
            pltpu.VMEM(twists.shape, jnp.float32),
            pltpu.SemaphoreType.DMA((6,)),
            pltpu.SemaphoreType.DMA((1,)),
            pltpu.SemaphoreType.DMA((9,)),
            pltpu.SemaphoreType.DMA((1,)),
            pltpu.SemaphoreType.DMA((3,)),
            pltpu.SemaphoreType.DMA((2,)),
            pltpu.SemaphoreType.DMA((3,)),
            pltpu.SemaphoreType.DMA((3,)),
            pltpu.SemaphoreType.REGULAR,
        ],
        compiler_params=pltpu.CompilerParams(
            collective_id=0, has_side_effects=True, vmem_limit_bytes=(64 << 20) - (960 << 10)
        ),
    )(
        key_input, value_input, query_input, cotangent, filter_taps,
        skip_gain.reshape(1, channels), jnp.asarray(tables), jnp.asarray(twists),
    )
    results = pl.pallas_call(
        emit,
        out_shape=tuple(jax.ShapeDtypeStruct(*shape) for shape in shapes),
        in_specs=[vmem] * 6,
        out_specs=(hbm,) * 7,
        scratch_shapes=[
            pltpu.VMEM((1, channels), jnp.float32),
            pltpu.VMEM((1, 1), jnp.float32),
            pltpu.SemaphoreType.DMA((7,)),
        ],
        compiler_params=pltpu.CompilerParams(vmem_limit_bytes=4 << 20),
    )(*held)
    return (*results[:5], results[5].reshape(channels), results[6].reshape(()))


def pick_body(query_input, *others):
    devices = lax.axis_size("seq")
    rows, channels = query_input.shape
    fits = devices == 8 and 2 * channels == LANES * devices and rows % 16 == 0
    chosen = fused_body if fits and rows * devices <= 2048 else body
    return chosen(query_input, *others)


def solution(mesh):
    return jax.shard_map(
        pick_body,
        mesh=mesh,
        in_specs=(
            P("seq", "ch"),
            P("seq", "ch"),
            P("seq", "ch"),
            P("seq", "ch"),
            P("seq", "ch"),
            P("ch"),
        ),
        out_specs=(
            P("seq", "ch"),
            P("seq", "ch"),
            P("seq", "ch"),
            P("seq", "ch"),
            P("seq", "ch"),
            P("ch"),
            P(),
        ),
        check_vma=False,
    )
```
